128 devices in a mesh: gx: 4 (over x), gy: 4 (over z), gz: 8 (over y, core).
Axes of the slice: x: 4, y: 4, z: 4, core: 2. Of those that a mesh axis runs over, the one named last changes fastest.
Arguments:
- force: float32 [3, 128, 64, 1024], P(None, 'gx', 'gy', 'gz'), may hold values from -6 to 6
- phase: int32 [128, 64, 1024], P('gx', 'gy', 'gz'), may hold values from 0 to 7
- viscosity_table: float32 [8], replicated, may hold values from 0.1 to 10
- boundary_flags: int32 [6], replicated, may hold values from 0 to 1
Outputs:
- pressure: float32 [128, 64, 1024], P('gx', 'gy', 'gz')
- residual: float32 [128, 64, 1024], P('gx', 'gy', 'gz')
- res_norms: float32 [3], replicated
The draws below stay inside these ranges and needn't reach their ends.
Inputs may be any that keep to these rules, and one draw needn't show every extreme that they name: phase ids index viscosity_table. `boundary_flags`: 0 marks a no-slip face, 1 a free-slip face.
All inputs are finite; a program needn't handle non-finite values.
Results may differ from the reference program's by a relative error of at most 0.0003.
Values sent between devices are 32-bit elements; how exact they have to be, the bound alone decides.
A program may use at most 192 MiB of HBM per device.

```python
import math
import jax
import jax.numpy as jnp
from jax import lax

ITERS = 3
SWEEPS = 4
PHASES = 8
NX = 128
NY = 64
NZ = 1024


def touch_ends(values, stream_key, low, high):
    dims = values.shape
    spot = [jax.random.randint(jax.random.fold_in(stream_key, axis), (), 0, dims[axis]) for axis in range(len(dims))]
    values = values.at[tuple(spot)].set(low)
    longest = dims.index(max(dims))
    spot[longest] = (spot[longest] + 1) % dims[longest]
    return values.at[tuple(spot)].set(high)


def level_of(own_key, shape, pieces, low, largest):
    gain, own = 1.0, jax.random.fold_in(own_key, 6)
    for axis_at, blocks in pieces:
        heights = jnp.exp(jax.random.uniform(jax.random.fold_in(own, axis_at), (blocks,), jnp.float32, low / len(pieces), largest / len(pieces)))
        gain = gain * jnp.repeat(heights, shape[axis_at] // blocks).reshape([-1 if axis == axis_at else 1 for axis in range(len(shape))])
    return gain


def normal_values(stream_key, dims, spread, reach, shards=(), kind=jnp.bfloat16):
    values = jax.random.normal(stream_key, dims, jnp.float32) * spread
    if len(shards) > 0:
        values = level_of(stream_key, dims, shards, -0.22, 0.18) * values
    return jnp.clip(values, min=-reach, max=reach).astype(kind)


def setup_inputs(seed: int = 0) -> dict:
    splits = jax.random.split(jax.random.key(seed), 5)
    force = normal_values(splits[0], (3, NX, NY, NZ), 1.0, 6.0, ((1, 4), (2, 4), (3, 8)), jnp.float32)
    phase = touch_ends(jax.random.randint(splits[1], (NX, NY, NZ), 0, PHASES), jax.random.fold_in(splits[1], 1), 0, PHASES - 1).astype(jnp.int32)
    viscosity_table = jnp.clip(jnp.exp(jax.random.uniform(splits[2], (PHASES,), jnp.float32, math.log(0.1), math.log(10.0))), 0.1, 10.0)
    boundary_flags = touch_ends(jax.random.randint(splits[3], (6,), 0, 2), jax.random.fold_in(splits[3], 1), 0, 1).astype(jnp.int32)
    return dict(force=force, phase=phase, viscosity_table=viscosity_table, boundary_flags=boundary_flags)


OMEGA = 0.8


def lookup(phase, table):
    eta = jnp.zeros(phase.shape, jnp.float32)
    for level in range(table.shape[0]):
        eta = eta + jnp.where(phase == level, table[level], jnp.float32(0.0))
    return eta


def trim(array, keep):
    for dim in range(3):
        if dim != keep:
            array = lax.slice_in_dim(array, 1, array.shape[dim] - 1, axis=dim)
    return array


def coefficients(eta_wide, flags, starts, totals):
    walls = (flags == 0).astype(jnp.float32)
    inner = eta_wide[1:-1, 1:-1, 1:-1]
    faces = []
    diag = [jnp.zeros_like(inner) for comp in range(3)]
    for axis in range(3):
        length = eta_wide.shape[axis]
        spots = starts[axis] + jnp.arange(length, dtype=jnp.int32)
        inside = (spots >= 0) & (spots < totals[axis])
        shape = [1, 1, 1]
        shape[axis] = length - 2
        upper_in = inside[2:].reshape(shape)
        lower_in = inside[:-2].reshape(shape)
        sides = trim(eta_wide, axis)
        middle = lax.slice_in_dim(sides, 1, length - 1, axis=axis)
        upper = 0.5 * (middle + lax.slice_in_dim(sides, 2, length, axis=axis))
        lower = 0.5 * (middle + lax.slice_in_dim(sides, 0, length - 2, axis=axis))
        faces.append((jnp.where(upper_in, upper, 0.0), jnp.where(lower_in, lower, 0.0)))
        for comp in range(3):
            normal = 1.0 if comp == axis else 0.0
            wall_low = jnp.maximum(walls[2 * axis], normal)
            wall_high = jnp.maximum(walls[2 * axis + 1], normal)
            diag[comp] = diag[comp] + jnp.where(upper_in, upper, wall_high * inner) + jnp.where(lower_in, lower, wall_low * inner)
    return faces, jnp.stack(diag)


def viscous(wide, faces, diag):
    result = diag * wide[:, 1:-1, 1:-1, 1:-1]
    for axis in range(3):
        dim = axis + 1
        sides = wide
        for other in range(1, 4):
            if other != dim:
                sides = lax.slice_in_dim(sides, 1, sides.shape[other] - 1, axis=other)
        length = wide.shape[dim]
        result = result - faces[axis][0] * lax.slice_in_dim(sides, 2, length, axis=dim)
        result = result - faces[axis][1] * lax.slice_in_dim(sides, 0, length - 2, axis=dim)
    return result


def smooth(source, faces, diag, inverse):
    state = OMEGA * inverse * source
    for sweep in range(SWEEPS - 1):
        wide = jnp.pad(state, ((0, 0), (1, 1), (1, 1), (1, 1)))
        state = state + OMEGA * inverse * (source - viscous(wide, faces, diag))
    return state


def gradient(field):
    padded = jnp.pad(field, ((0, 1), (0, 1), (0, 1)))
    return jnp.stack([padded[1:, :-1, :-1] - field, padded[:-1, 1:, :-1] - field, padded[:-1, :-1, 1:] - field])


def divergence(velocity):
    total = jnp.zeros(velocity.shape[1:], jnp.float32)
    for axis in range(3):
        comp = velocity[axis]
        widths = [(0, 0), (0, 0), (0, 0)]
        widths[axis] = (1, 0)
        before = lax.slice_in_dim(jnp.pad(comp, widths), 0, comp.shape[axis], axis=axis)
        total = total + before - comp
    return total


def reference(force, phase, viscosity_table, boundary_flags):
    eta = lookup(phase, viscosity_table)
    faces, diag = coefficients(jnp.pad(eta, 1), boundary_flags, (-1, -1, -1), (NX, NY, NZ))
    inverse = 1.0 / diag

    def schur(field):
        return divergence(smooth(gradient(field), faces, diag, inverse))

    rhs = divergence(smooth(force, faces, diag, inverse))
    cells = float(NX * NY * NZ)
    pressure = jnp.zeros_like(rhs)
    residual = rhs
    scaled = eta * residual
    search = scaled
    gamma = jnp.sum(residual * scaled)
    squares = jnp.sum(residual * residual)
    norms = []
    for step in range(ITERS):
        norms.append(squares / cells)
        image = schur(search)
        alpha = gamma / jnp.sum(search * image)
        pressure = pressure + alpha * search
        residual = residual - alpha * image
        if step + 1 < ITERS:
            scaled = eta * residual
            gamma_new = jnp.sum(residual * scaled)
            squares = jnp.sum(residual * residual)
            search = scaled + (gamma_new / gamma) * search
            gamma = gamma_new
    return pressure, residual, jnp.stack(norms)
```

```python
import functools

import jax
import jax.numpy as jnp
from jax import lax
from jax.experimental import pallas as pl
from jax.experimental.pallas import tpu as pltpu
from jax.sharding import PartitionSpec as P

ITERS = 3
OMEGA = 0.8
F32 = jnp.float32
MESH = pl.DeviceIdType.MESH

BX, BY, BZ = 32, 16, 128
ROWS = BX * BY
G = 24
EROWS = 2 * G + 40 * 24
SROWS = 2 * G + 5 * 24
NSETS = 7

DIRS = [(dx, dy, dz) for dz in (0, 1, -1) for dy in (1, -1, 0) for dx in (0, 1, -1) if (dx, dy, dz) != (0, 0, 0)]
DIRS.sort(key=lambda d: (d[1] == 0 or d[0] != 0 or d[2] != 0, sum(map(abs, d))))
DIR_AT = {d: i for i, d in enumerate(DIRS)}


def piece_rows(d):
    dx, dy, dz = d
    if dz == 0:
        if dx and dy:
            return 16
        return 128 if dy else 80
    if dx and dy:
        return 8
    if dy:
        return 32
    return 16 if dx else 64


OFFSETS = {}
RECV_ROWS = 0
for _d in DIRS:
    OFFSETS[_d] = RECV_ROWS
    RECV_ROWS += piece_rows(_d)


def iota(shape, dim):
    return lax.broadcasted_iota(jnp.int32, shape, dim)


def roll_lanes(v, by):
    by = by % 128
    return v if by == 0 else pltpu.roll(v, by, 1)


def roll_rows(v, by):
    return pltpu.roll(v, by % v.shape[0], 0)


def kernel(
    sizes,
    force_hbm, phase_hbm, table, flags,
    press_out, resid_out, norms_out,
    phase, field, ystage, cstage, dstage, y5, recv, r5,
    ext, slab, kmain, kslab, wmain, wslab, smain, sslab, va, vb, sa, sb, inj,
    res, sch, wap, sim, tim, nap, pre,
    red, red1, red2,
    in_sem, out_sem, send_sem, recv_sem, send5_sem, recv5_sem, rs1, rr1, rs2, rr2,
):
    nx, ny, nz = sizes
    at = (lax.axis_index("gx"), lax.axis_index("gy"), lax.axis_index("gz"))

    def neighbour(d):
        ok = None
        for dim in range(3):
            if d[dim] == 0:
                continue
            here = at[dim] < sizes[dim] - 1 if d[dim] > 0 else at[dim] > 0
            ok = here if ok is None else jnp.logical_and(ok, here)
        return ok, tuple(at[dim] + d[dim] for dim in range(3))

    def recv_at(k, d, start=0, rows=None):
        return recv.at[k, pl.ds(OFFSETS[d] + start, piece_rows(d) if rows is None else rows)]

    def pieces(k, d):
        dx, dy, dz = d
        to = tuple(-a for a in d)
        if dz == 0:
            if dx and dy:
                side = 0 if dy < 0 else 1
                src = ystage.at[k, side, pl.ds(0 if dx < 0 else 112, 16)]
                return src, recv_at(k, to)
            if dy:
                return ystage.at[k, 0 if dy < 0 else 1], recv_at(k, to)
            if dx < 0:
                return field.at[k, pl.ds(0, 64)], recv_at(k, to, 0, 64)
            if isinstance(k, int) and k == 0:
                return field.at[k, pl.ds(ROWS - 80, 80)], recv_at(k, to)
            return field.at[k, pl.ds(ROWS - 64, 64)], recv_at(k, to, 16, 64)
        if dx and dy:
            return dstage.at[k, pl.ds(0 if dx < 0 else 24, 8)], recv_at(k, to)
        if dy:
            return dstage.at[k], recv_at(k, to)
        if dx:
            return cstage.at[k, pl.ds(0 if dx < 0 else 48, 16)], recv_at(k, to)
        return cstage.at[k], recv_at(k, to)

    def copy_of(k, d):
        src, dst = pieces(k, d)
        _, device = neighbour(d)
        to = tuple(-a for a in d)
        return pltpu.make_async_remote_copy(
            src_ref=src, dst_ref=dst,
            send_sem=send_sem.at[k, DIR_AT[d]], recv_sem=recv_sem.at[k, DIR_AT[to]],
            device_id=device, device_id_type=MESH,
        )

    def incoming(k, d):
        to = tuple(-a for a in d)
        src, dst = pieces(k, to)
        return pltpu.make_async_remote_copy(
            src_ref=src, dst_ref=dst,
            send_sem=send_sem.at[k, DIR_AT[to]], recv_sem=recv_sem.at[k, DIR_AT[d]],
            device_id=at, device_id_type=MESH,
        )

    sub8 = iota((8, 128), 0)
    lane8 = iota((8, 128), 1)
    group8, slot8 = lane8 // 16, lane8 % 16
    lane24 = iota((24, 128), 1)
    sub24 = iota((24, 128), 0)
    group24, slot24 = lane24 // 16, lane24 % 16


    def pack(k):
        def pair(xp, _):
            base = pl.multiple_of(xp * 32, 32)
            a0, a1 = field[k, pl.ds(base, 8), :], field[k, pl.ds(base + 8, 8), :]
            b0, b1 = field[k, pl.ds(base + 16, 8), :], field[k, pl.ds(base + 24, 8), :]
            to = pl.multiple_of(xp * 8, 8)
            ystage[k, 0, pl.ds(to, 8), :] = jnp.where(sub8 < 4, a0, roll_rows(b0, 4))
            ystage[k, 1, pl.ds(to, 8), :] = jnp.where(sub8 < 4, roll_rows(a1, 4), b1)
            return 0
        lax.fori_loop(0, BX // 2, pair, 0, unroll=8)

        def block(xb, _):
            acc = [[jnp.zeros((8, 128), F32) for _ in range(2)] for _ in range(3)]
            for g in range(8):
                base = pl.multiple_of(xb * 128, 128) + g * 16
                a, b = field[k, pl.ds(base, 8), :], field[k, pl.ds(base + 8, 8), :]
                for i, v in enumerate((a, b, jnp.where(sub8 < 4, a, b))):
                    acc[i][0] = jnp.where(group8 == g, roll_lanes(v, 5 + 16 * g), acc[i][0])
                    acc[i][1] = jnp.where(group8 == g, roll_lanes(v, 12 + 16 * g), acc[i][1])
            a, b, c = (jnp.where(slot8 < 9, u, v) for u, v in acc)
            to = pl.multiple_of(xb * 16, 16)
            cstage[k, pl.ds(to, 8), :] = a
            cstage[k, pl.ds(to + 8, 8), :] = b
            dstage[k, pl.ds(pl.multiple_of(xb * 8, 8), 8), :] = c
            return 0
        lax.fori_loop(0, 4, block, 0, unroll=2)

    def send(k):
        for d in DIRS:
            ok, _ = neighbour(d)

            @pl.when(ok)
            def _():
                copy_of(k, d).start()

    def receive(k):
        for d in DIRS:
            ok, _ = neighbour(d)

            @pl.when(ok)
            def _():
                incoming(k, d).wait_recv()

    def finish_sends(k):
        for d in DIRS:
            ok, _ = neighbour(d)

            @pl.when(ok)
            def _():
                copy_of(k, d).wait_send()

    def unpack(k):
        def planes(own, low, high, first, pairs):
            def pair(xp, _):
                src = pl.multiple_of(xp * 32, 32)
                side = pl.multiple_of(xp * 8, 8)
                lo, hi = low(side), high(side)
                los, his = roll_rows(lo, 4), roll_rows(hi, 4)
                for half in range(2):
                    ra, rb = roll_rows(own(src + 16 * half), 4), roll_rows(own(src + 16 * half + 8), 4)
                    to = pl.multiple_of(xp * 48, 8) + (G + (first + half) * 24)
                    ext[pl.ds(to, 8), :] = jnp.where(sub8 < 4, (lo, los)[half], ra)
                    ext[pl.ds(to + 8, 8), :] = jnp.where(sub8 < 4, ra, rb)
                    ext[pl.ds(to + 16, 8), :] = jnp.where(sub8 < 4, rb, (his, hi)[half])
                return 0
            lax.fori_loop(0, pairs, pair, 0, unroll=min(pairs, 4))

        def of(d, start=0):
            return lambda at_row: recv[k, pl.ds(at_row + (OFFSETS[d] + start), 8), :]

        planes(lambda r: field[k, pl.ds(r, 8), :], of((0, -1, 0)), of((0, 1, 0)), 4, 16)
        planes(of((-1, 0, 0), 16), of((-1, -1, 0)), of((-1, 1, 0)), 0, 2)
        planes(of((1, 0, 0)), of((1, -1, 0)), of((1, 1, 0)), 36, 2)

        def merged(d, row):
            low = recv[k, pl.ds(OFFSETS[(d[0], d[1], -1)] + row, 8), :]
            high = recv[k, pl.ds(OFFSETS[(d[0], d[1], 1)] + row, 8), :]
            return jnp.where(slot8 < 8, low, high)

        inner = []
        for t in range(2):
            inner.append([merged((-1, 0), 8 * t)] + [merged((0, 0), xb * 16 + 8 * t) for xb in range(4)] + [merged((1, 0), 8 * t)])
        sides = []
        for xb in range(6):
            dx, row = (-1, 0) if xb == 0 else (1, 0) if xb == 5 else (0, (xb - 1) * 8)
            sides.append(roll_rows(jnp.where(sub8 < 4, merged((dx, 1), row), merged((dx, -1), row)), 4))

        def shifted(parts, i):
            return roll_lanes(jnp.where(group8 < 4, parts[i + 1], parts[i]), 64)

        for i in range(5):
            a, b = roll_rows(shifted(inner[0], i), 4), roll_rows(shifted(inner[1], i), 4)
            c = shifted(sides, i)
            tiles = (jnp.where(sub8 < 4, c, a), jnp.where(sub8 < 4, a, b), jnp.where(sub8 < 4, b, c))
            for t in range(3):
                slab[pl.ds(G + i * 24 + 8 * t, 8), :] = tiles[t]

        def own(i, _):
            base = pl.multiple_of(i * 192, 8) + G
            to = pl.multiple_of(i * 24, 8) + G
            for t in range(3):
                lo, hi = jnp.zeros((8, 128), F32), jnp.zeros((8, 128), F32)
                for j in range(8):
                    v = ext[pl.ds(base + j * 24 + 8 * t, 8), :]
                    lo = jnp.where(group8 == j, roll_lanes(v, 5 + 16 * j), lo)
                    hi = jnp.where(group8 == j, roll_lanes(v, 12 + 16 * j), hi)
                mine = jnp.where(slot8 < 9, lo, hi)
                old = slab[pl.ds(to + 8 * t, 8), :]
                slab[pl.ds(to + 8 * t, 8), :] = jnp.where((slot8 >= 5) & (slot8 < 12), mine, old)
            return 0
        lax.fori_loop(0, 5, own, 0)


    def make_injection(source, c, rows0, out):
        v = source[c, pl.ds(rows0, 24), :]
        out[c, pl.ds(rows0, 24), :] = jnp.where(slot24 == 5, roll_lanes(v, -7), v)

    def main_z(v, c, i, j):
        edge = roll_lanes(inj[c, pl.ds(pl.multiple_of(i * 24, 8) + G, 24), :], 123 - 16 * j)
        up = roll_lanes(jnp.where(lane24 == 0, edge, v), 127)
        down = roll_lanes(jnp.where(lane24 == 127, edge, v), 1)
        return up, down

    def slab_x(v, below, above):
        up = roll_lanes(jnp.where(lane24 < 16, above, v), -16)
        down = roll_lanes(jnp.where(lane24 >= 112, below, v), 16)
        return up, down

    def for_planes(first, last, body):
        for p in range(first, 8):
            body(0, p)

        def block(i, _):
            for j in range(8):
                body(i, j)
            return 0
        lax.fori_loop(1, 4, block, 0)
        for p in range(32, last + 1):
            body(4, p - 32)

    def row_of(i, j):
        return pl.multiple_of(i * 192, 8) + (G + j * 24)

    def shift_rows(ref, c, base, by):
        return ref[c, pl.ds(base + by, 24), :]


    walls = [jnp.where(flags[f] == 0, F32(1.0), F32(0.0)) for f in range(6)]
    totals = (nx * BX, ny * BY, nz * BZ)

    def coefficients(e, nbrs, spots):
        faces = []
        inside = None
        diag = jnp.zeros_like(e)
        extra = [jnp.zeros_like(e) for _ in range(3)]
        for axis in range(3):
            for side in range(2):
                spot = spots[axis] + (1 if side else -1)
                here = (spot >= 0) & (spot < totals[axis])
                face = 0.5 * (e + nbrs[axis][side])
                wall = walls[2 * axis + side]
                outer = jnp.where(here, F32(0.0), e)
                diag = diag + jnp.where(here, face, e * wall)
                extra[axis] = extra[axis] + outer * (1.0 - wall)
                faces.append(face)
            here = (spots[axis] >= 0) & (spots[axis] < totals[axis])
            inside = here if inside is None else inside & here
        weights = []
        for c in range(3):
            d = diag + extra[c]
            good = inside & (d > 0)
            weights.append(jnp.where(good, OMEGA / jnp.where(good, d, F32(1.0)), F32(0.0)))
        return faces, weights

    def setup():
        for t in range(2):
            v = roll_rows(recv[0, pl.ds(OFFSETS[(-1, 0, 0)] + 8 * t, 8), :], 4)
            if t == 0:
                ext[pl.ds(0, 8), :] = jnp.where(sub8 < 4, F32(0.0), v)
                keep = v
            else:
                ext[pl.ds(8, 8), :] = jnp.where(sub8 < 4, keep, v)
                ext[pl.ds(16, 8), :] = jnp.where(sub8 < 4, v, F32(0.0))

        def injection(i, _):
            base = pl.multiple_of(i * 24, 8) + G
            v = slab[pl.ds(base, 24), :]
            inj[0, pl.ds(base, 24), :] = jnp.where(slot24 == 5, roll_lanes(v, -7), v)
            return 0
        lax.fori_loop(0, 5, injection, 0)

        def main_block(i, _):
            fives = roll_rows(jnp.where(sub8 < 4, r5[pl.ds(pl.multiple_of(i * 8, 8) + 8, 8), :], r5[pl.ds(pl.multiple_of(i * 8, 8), 8), :]), 4)
            for j in range(8):
                b = row_of(i, j)
                e = ext[pl.ds(b, 24), :]
                up, down = main_z(e, 0, i, j)
                five = jnp.broadcast_to(fives[j:j + 1, :], (24, 128))
                below = jnp.where(sub24 == 0, five, ext[pl.ds(b - 1, 24), :])
                nbrs = (
                    (ext[pl.ds(b - 24, 24), :], ext[pl.ds(b + 24, 24), :]),
                    (below, ext[pl.ds(b + 1, 24), :]),
                    (down, up),
                )
                spots = (
                    jnp.broadcast_to(at[0] * BX + (i * 8 + j - 4), (24, 128)),
                    sub24 + (at[1] * BY - 4),
                    lane24 + at[2] * BZ,
                )
                faces, weights = coefficients(e, nbrs, spots)
                for f in range(6):
                    kmain[f, pl.ds(b, 24), :] = faces[f]
                for c in range(3):
                    wmain[c, pl.ds(b, 24), :] = weights[c]
            return 0
        lax.fori_loop(0, 5, main_block, 0)

        def slab_block(i, _):
            b = pl.multiple_of(i * 24, 8) + G
            e = slab[pl.ds(b, 24), :]
            xu, xd = slab_x(e, slab[pl.ds(b - 24, 24), :], slab[pl.ds(b + 24, 24), :])
            nbrs = (
                (xd, xu),
                (slab[pl.ds(b - 1, 24), :], slab[pl.ds(b + 1, 24), :]),
                (roll_lanes(e, 1), roll_lanes(e, 127)),
            )
            spots = (
                group24 + (at[0] * BX - 4 + i * 8),
                sub24 + (at[1] * BY - 4),
                jnp.where(slot24 < 9, slot24 - 5, slot24 + 116) + at[2] * BZ,
            )
            faces, weights = coefficients(e, nbrs, spots)
            for f in range(6):
                kslab[f, pl.ds(b, 24), :] = faces[f]
            for c in range(3):
                wslab[c, pl.ds(b, 24), :] = weights[c]
            return 0
        lax.fori_loop(0, 5, slab_block, 0)


    def gradient():
        def slab_block(i, _):
            b = pl.multiple_of(i * 24, 8) + G
            p = slab[pl.ds(b, 24), :]
            above = slab[pl.ds(b + 24, 24), :]
            xu = roll_lanes(jnp.where(lane24 < 16, above, p), -16)
            nbrs = (xu, slab[pl.ds(b + 1, 24), :], roll_lanes(p, 127))
            for c in range(3):
                sslab[c, pl.ds(b, 24), :] = wslab[c, pl.ds(b, 24), :] * (nbrs[c] - p)
            inj[0, pl.ds(b, 24), :] = jnp.where(slot24 == 5, roll_lanes(p, -7), p)
            return 0
        lax.fori_loop(0, 5, slab_block, 0)

        def plane(i, j):
            b = row_of(i, j)
            p = ext[pl.ds(b, 24), :]
            edge = roll_lanes(inj[0, pl.ds(pl.multiple_of(i * 24, 8) + G, 24), :], 123 - 16 * j)
            zu = roll_lanes(jnp.where(lane24 == 0, edge, p), 127)
            nbrs = (ext[pl.ds(b + 24, 24), :], ext[pl.ds(b + 1, 24), :], zu)
            for c in range(3):
                smain[c, pl.ds(b, 24), :] = wmain[c, pl.ds(b, 24), :] * (nbrs[c] - p)
        for_planes(0, 38, plane)

    def scaled_force(c):
        def slab_block(i, _):
            b = pl.multiple_of(i * 24, 8) + G
            sslab[c, pl.ds(b, 24), :] = wslab[c, pl.ds(b, 24), :] * slab[pl.ds(b, 24), :]
            return 0
        lax.fori_loop(0, 5, slab_block, 0)

        def block(i, _):
            for j in range(8):
                b = row_of(i, j)
                smain[c, pl.ds(b, 24), :] = wmain[c, pl.ds(b, 24), :] * ext[pl.ds(b, 24), :]
            return 0
        lax.fori_loop(0, 5, block, 0)

    def injections(source):
        def block(i, _):
            b = pl.multiple_of(i * 24, 8) + G
            for c in range(3):
                make_injection(source, c, b, inj)
            return 0
        lax.fori_loop(0, 5, block, 0, unroll=True)

    def sweep(src, dst, ssrc, sdst, first, last, with_slab):
        injections(ssrc)

        def plane(i, j):
            b = row_of(i, j)
            k = [kmain[f, pl.ds(b, 24), :] for f in range(6)]
            for c in range(3):
                v = src[c, pl.ds(b, 24), :]
                zu, zd = main_z(v, c, i, j)
                total = k[0] * src[c, pl.ds(b - 24, 24), :] + k[1] * src[c, pl.ds(b + 24, 24), :]
                total = total + (k[2] * shift_rows(src, c, b, -1) + k[3] * shift_rows(src, c, b, 1))
                total = total + (k[4] * zd + k[5] * zu)
                dst[c, pl.ds(b, 24), :] = (
                    (1.0 - OMEGA) * v + smain[c, pl.ds(b, 24), :] + wmain[c, pl.ds(b, 24), :] * total
                )
        for_planes(first, last, plane)

        def block(i, _):
            b = pl.multiple_of(i * 24, 8) + G
            k = [kslab[f, pl.ds(b, 24), :] for f in range(6)]
            for c in range(3):
                v = ssrc[c, pl.ds(b, 24), :]
                xu, xd = slab_x(v, ssrc[c, pl.ds(b - 24, 24), :], ssrc[c, pl.ds(b + 24, 24), :])
                total = k[0] * xd + k[1] * xu
                total = total + (k[2] * shift_rows(ssrc, c, b, -1) + k[3] * shift_rows(ssrc, c, b, 1))
                total = total + (k[4] * roll_lanes(v, 1) + k[5] * roll_lanes(v, 127))
                sdst[c, pl.ds(b, 24), :] = (
                    (1.0 - OMEGA) * v + sslab[c, pl.ds(b, 24), :] + wslab[c, pl.ds(b, 24), :] * total
                )
            return 0
        lax.fori_loop(0, 5, block, 0, unroll=True)

    def divergence(src, ssrc, out):
        def block(i, _):
            b = pl.multiple_of(i * 24, 8) + G
            make_injection(ssrc, 2, b, inj)
            return 0
        lax.fori_loop(0, 5, block, 0, unroll=True)

        def plane(i, j):
            b = row_of(i, j) + 4
            x, y, z = (src[c, pl.ds(b, 16), :] for c in range(3))
            edge = roll_lanes(inj[2, pl.ds(pl.multiple_of(i * 24, 8) + (G + 4), 16), :], 123 - 16 * j)
            zd = roll_lanes(jnp.where(iota((16, 128), 1) == 127, edge, z), 1)
            total = (src[0, pl.ds(b - 24, 16), :] - x) + (src[1, pl.ds(b - 1, 16), :] - y) + (zd - z)
            to = pl.multiple_of(i * 128, 16) + (j * 16 - 64)
            out[pl.ds(to, 16), :] = total
        for_planes(4, 35, plane)

    def apply(out):
        sweep(smain, va, sslab, sa, 1, 37, True)
        sweep(va, vb, sa, sb, 2, 36, True)
        sweep(vb, va, sb, sa, 3, 35, True)
        divergence(va, sa, out)


    me_z = at[2]
    me_xy = at[0] * ny + at[1]
    nxy = nx * ny

    def z_copy(k, off):
        other = lax.rem(me_z + off, nz)
        return pltpu.make_async_remote_copy(
            src_ref=red.at[k], dst_ref=red1.at[k, me_z], send_sem=rs1.at[k, off], recv_sem=rr1.at[k, off],
            device_id=(at[0], at[1], other), device_id_type=MESH,
        )

    def xy_copy(k, ox, oy):
        off = ox * ny + oy
        return pltpu.make_async_remote_copy(
            src_ref=red.at[k], dst_ref=red2.at[k, me_xy], send_sem=rs2.at[k, off], recv_sem=rr2.at[k, off],
            device_id=(lax.rem(at[0] + ox, nx), lax.rem(at[1] + oy, ny), at[2]), device_id_type=MESH,
        )

    offsets_xy = [(ox, oy) for ox in range(nx) for oy in range(ny) if (ox, oy) != (0, 0)]

    def reduce_start(k, value):
        red[k] = value
        red1[k, me_z] = value
        for off in range(1, nz):
            z_copy(k, off).start()

    def reduce_middle(k):
        for off in range(1, nz):
            z_copy(k, off).wait_recv()
        for off in range(1, nz):
            z_copy(k, off).wait_send()
        value = red1[k, 0]
        for i in range(1, nz):
            value = value + red1[k, i]
        red[k] = value
        red2[k, me_xy] = value
        for ox, oy in offsets_xy:
            xy_copy(k, ox, oy).start()

    def reduce_end(k):
        for ox, oy in offsets_xy:
            xy_copy(k, ox, oy).wait_recv()
        for ox, oy in offsets_xy:
            xy_copy(k, ox, oy).wait_send()
        value = red2[k, 0]
        for i in range(1, nxy):
            value = value + red2[k, i]
        value = jnp.broadcast_to(jnp.sum(value, axis=1, keepdims=True), (8, 128))
        return [jnp.broadcast_to(value[i:i + 1, :], (8, 128)) for i in range(3)]


    load_phase = pltpu.make_async_copy(phase_hbm, phase, in_sem.at[0])
    load_force = pltpu.make_async_copy(force_hbm, field.at[pl.ds(1, 3)], in_sem.at[1])
    load_phase.start()
    load_force.start()

    def clear_recv(i, _):
        for k in range(NSETS):
            recv[k, pl.ds(pl.multiple_of(i * 8, 8), 8), :] = jnp.zeros((8, 128), F32)
        return 0
    lax.fori_loop(0, RECV_ROWS // 8, clear_recv, 0, unroll=2)

    for t in range(0, 48, 8):
        r5[pl.ds(t, 8), :] = jnp.zeros((8, 128), F32)

    barrier = pltpu.get_barrier_semaphore()
    count = jnp.int32(0)
    for d in DIRS:
        ok, device = neighbour(d)

        @pl.when(ok)
        def _():
            pl.semaphore_signal(barrier, inc=1, device_id=device, device_id_type=MESH)
        count = count + ok.astype(jnp.int32)
    for off in range(1, nz):
        pl.semaphore_signal(barrier, inc=1, device_id=(at[0], at[1], lax.rem(me_z + off, nz)), device_id_type=MESH)
    for ox, oy in offsets_xy:
        pl.semaphore_signal(
            barrier, inc=1, device_id=(lax.rem(at[0] + ox, nx), lax.rem(at[1] + oy, ny), at[2]), device_id_type=MESH
        )
    count = count + (nz - 1 + nxy - 1)

    zero24 = jnp.zeros((24, 128), F32)
    for ref, rows in ((ext, EROWS), (slab, SROWS)):
        ref[pl.ds(0, 24), :] = zero24
        ref[pl.ds(rows - 24, 24), :] = zero24
    for ref, rows in ((smain, EROWS), (va, EROWS), (vb, EROWS), (sslab, SROWS), (sa, SROWS), (sb, SROWS)):
        for c in range(3):
            ref[c, pl.ds(0, 24), :] = zero24
            ref[c, pl.ds(rows - 24, 24), :] = zero24
    for ref in (smain, va, vb):
        for c in range(3):
            for xx in (0, 1, 2, 37, 38, 39):
                ref[c, pl.ds(G + xx * 24, 24), :] = zero24

    load_phase.wait()

    def lookup(i, _):
        for u in range(4):
            r = pl.multiple_of(i * 32, 32) + 8 * u
            ids = phase[pl.ds(r, 8), :]
            eta = jnp.zeros((8, 128), F32)
            for level in range(8):
                eta = eta + jnp.where(ids == level, table[level], F32(0.0))
            field[0, pl.ds(r, 8), :] = eta
        return 0
    lax.fori_loop(0, ROWS // 32, lookup, 0)
    pack(0)
    for x in range(BX):
        y5[pl.ds(x, 1), :] = field[0, pl.ds(x * 16 + 11, 1), :]
    pl.semaphore_wait(barrier, count)
    send(0)
    has_y_up, _ = neighbour((0, 1, 0))
    has_y_down, _ = neighbour((0, -1, 0))
    copy5_out = pltpu.make_async_remote_copy(
        src_ref=y5, dst_ref=r5.at[pl.ds(8, 32)], send_sem=send5_sem, recv_sem=recv5_sem,
        device_id=(at[0], at[1] + 1, at[2]), device_id_type=MESH,
    )

    @pl.when(has_y_up)
    def _():
        copy5_out.start()
    load_force.wait()

    def send_force(k, _):
        pack(k)
        send(k)
        return 0
    lax.fori_loop(1, 4, send_force, 0)
    receive(0)

    @pl.when(has_y_down)
    def _():
        copy5_out.wait_recv()
    unpack(0)
    setup()

    def take_force(k, _):
        receive(k)
        unpack(k)
        scaled_force(k - 1)
        return 0
    lax.fori_loop(1, 4, take_force, 0)
    apply(res)

    def rows_loop(body, init, step=4):
        def block(i, carry):
            for u in range(step):
                carry = body(pl.multiple_of(i * (8 * step), 8 * step) + 8 * u, carry)
            return carry
        return lax.fori_loop(0, ROWS // (8 * step), block, init)

    def first(r, _):
        field[4, pl.ds(r, 8), :] = field[0, pl.ds(r, 8), :] * res[pl.ds(r, 8), :]
        return 0
    rows_loop(first, 0)

    def schur(k, out):
        receive(k)
        unpack(k)
        gradient()
        apply(out)

    pack(4)
    send(4)
    schur(4, wap)

    zero8 = jnp.zeros((8, 128), F32)

    def partials(gamma, delta, squares):
        sums = [jnp.broadcast_to(jnp.sum(v, axis=0, keepdims=True), (8, 128)) for v in (gamma, delta, squares)]
        return jnp.where(sub8 == 0, sums[0], jnp.where(sub8 == 1, sums[1], jnp.where(sub8 == 2, sums[2], F32(0.0))))

    def start0(r, carry):
        rr, w, e = (ref[pl.ds(r, 8), :] for ref in (res, wap, field.at[0]))
        z = e * rr
        field[5, pl.ds(r, 8), :] = e * w
        return carry[0] + rr * z, carry[1] + w * z, carry[2] + rr * rr
    sums = rows_loop(start0, (zero8, zero8, zero8))
    pack(5)
    send(5)
    reduce_start(0, partials(*sums))
    receive(5)
    reduce_middle(0)
    unpack(5)
    gradient()
    apply(nap)
    gamma, delta, squares = reduce_end(0)
    cells = float(totals[0] * totals[1] * totals[2])
    norms = [squares / cells]
    alpha = gamma / delta

    def step0(r, carry):
        at_r = pl.ds(r, 8)
        e, rr, w, n = field[0, at_r, :], res[at_r, :], wap[at_r, :], nap[at_r, :]
        p = e * rr
        sch[at_r, :] = p
        sim[at_r, :] = w
        tim[at_r, :] = n
        pre[at_r, :] = alpha * p
        rr = rr - alpha * w
        w = w - alpha * n
        res[at_r, :] = rr
        wap[at_r, :] = w
        z = e * rr
        field[6, at_r, :] = e * w
        return carry[0] + rr * z, carry[1] + w * z, carry[2] + rr * rr
    sums = rows_loop(step0, (zero8, zero8, zero8))
    pack(6)
    send(6)
    reduce_start(1, partials(*sums))
    receive(6)
    reduce_middle(1)
    unpack(6)
    gradient()
    apply(nap)
    gamma_old, alpha_old = gamma, alpha
    gamma, delta, squares = reduce_end(1)
    norms.append(squares / cells)
    beta = gamma / gamma_old
    alpha = gamma / (delta - beta * gamma / alpha_old)

    def step1(r, carry):
        at_r = pl.ds(r, 8)
        e, rr, w, n = field[0, at_r, :], res[at_r, :], wap[at_r, :], nap[at_r, :]
        p = e * rr + beta * sch[at_r, :]
        s = w + beta * sim[at_r, :]
        t = n + beta * tim[at_r, :]
        sch[at_r, :] = p
        sim[at_r, :] = s
        pre[at_r, :] = pre[at_r, :] + alpha * p
        rr = rr - alpha * s
        w = w - alpha * t
        res[at_r, :] = rr
        wap[at_r, :] = w
        z = e * rr
        return carry[0] + rr * z, carry[1] + w * z, carry[2] + rr * rr
    sums = rows_loop(step1, (zero8, zero8, zero8))
    reduce_start(2, partials(*sums))
    reduce_middle(2)
    gamma_old, alpha_old = gamma, alpha
    gamma, delta, squares = reduce_end(2)
    norms.append(squares / cells)
    beta = gamma / gamma_old
    alpha = gamma / (delta - beta * gamma / alpha_old)

    def step2(r, _):
        at_r = pl.ds(r, 8)
        rr = res[at_r, :]
        p = field[0, at_r, :] * rr + beta * sch[at_r, :]
        s = wap[at_r, :] + beta * sim[at_r, :]
        pre[at_r, :] = pre[at_r, :] + alpha * p
        res[at_r, :] = rr - alpha * s
        return 0
    rows_loop(step2, 0)
    store_press = pltpu.make_async_copy(pre, press_out, out_sem.at[0])
    store_resid = pltpu.make_async_copy(res, resid_out, out_sem.at[1])
    store_press.start()
    store_resid.start()
    norms_out[...] = jnp.where(lane8 == 0, norms[0], jnp.where(lane8 == 1, norms[1], norms[2]))

    for k in range(NSETS):
        finish_sends(k)

    @pl.when(has_y_up)
    def _():
        copy5_out.wait_send()
    store_press.wait()
    store_resid.wait()


def solution(mesh):
    sizes = (mesh.shape["gx"], mesh.shape["gy"], mesh.shape["gz"])
    nx, ny, nz = sizes

    def per_device(force, phase, table, flags):
        v = functools.partial(pltpu.VMEM)
        dma = pltpu.SemaphoreType.DMA
        scratch = [
            v((ROWS, 128), jnp.int32),
            v((NSETS, ROWS, 128), F32),
            v((NSETS, 2, 128, 128), F32),
            v((NSETS, 64, 128), F32),
            v((NSETS, 32, 128), F32),
            v((32, 128), F32),
            v((NSETS, RECV_ROWS, 128), F32),
            v((48, 128), F32),
            v((EROWS, 128), F32), v((SROWS, 128), F32),
            v((6, EROWS, 128), F32), v((6, SROWS, 128), F32),
            v((3, EROWS, 128), F32), v((3, SROWS, 128), F32),
            v((3, EROWS, 128), F32), v((3, SROWS, 128), F32),
            v((3, EROWS, 128), F32), v((3, EROWS, 128), F32),
            v((3, SROWS, 128), F32), v((3, SROWS, 128), F32),
            v((3, SROWS, 128), F32),
            *[v((ROWS, 128), F32) for _ in range(7)],
            v((ITERS, 8, 128), F32), v((ITERS, nz, 8, 128), F32), v((ITERS, nx * ny, 8, 128), F32),
            dma((2,)), dma((2,)), dma((NSETS, 26)), dma((NSETS, 26)), dma, dma,
            dma((ITERS, nz)), dma((ITERS, nz)), dma((ITERS, nx * ny)), dma((ITERS, nx * ny)),
        ]
        hbm = pl.BlockSpec(memory_space=pl.ANY)
        smem = pl.BlockSpec(memory_space=pltpu.SMEM)
        press, resid, norms = pl.pallas_call(
            functools.partial(kernel, sizes),
            out_shape=(
                jax.ShapeDtypeStruct((ROWS, 128), F32),
                jax.ShapeDtypeStruct((ROWS, 128), F32),
                jax.ShapeDtypeStruct((8, 128), F32),
            ),
            in_specs=[hbm, hbm, smem, smem],
            out_specs=(hbm, hbm, pl.BlockSpec(memory_space=pltpu.VMEM)),
            scratch_shapes=scratch,
            compiler_params=pltpu.CompilerParams(
                collective_id=0, has_side_effects=True, vmem_limit_bytes=60 * 1024 * 1024
            ),
        )(force.reshape(3, ROWS, BZ), phase.reshape(ROWS, BZ), table, flags)
        return press.reshape(BX, BY, BZ), resid.reshape(BX, BY, BZ), norms[0, :ITERS]

    return jax.shard_map(
        per_device,
        mesh=mesh,
        in_specs=(P(None, "gx", "gy", "gz"), P("gx", "gy", "gz"), P(), P()),
        out_specs=(P("gx", "gy", "gz"), P("gx", "gy", "gz"), P()),
        check_vma=False,
    )
```

```python
import functools

import jax
import jax.numpy as jnp
from jax import lax
from jax.experimental import pallas as pl
from jax.experimental.pallas import tpu as pltpu
from jax.sharding import PartitionSpec as P

ITERS = 3
OMEGA = 0.8
F32 = jnp.float32
MESH = pl.DeviceIdType.MESH

BX, BY, BZ = 32, 16, 128
ROWS = BX * BY
G = 24
EROWS = 2 * G + 40 * 24
SROWS = 2 * G + 5 * 24
NSETS = 7

DIRS = [(dx, dy, dz) for dz in (0, 1, -1) for dy in (1, -1, 0) for dx in (0, 1, -1) if (dx, dy, dz) != (0, 0, 0)]
DIRS.sort(key=lambda d: (d[1] == 0 or d[0] != 0 or d[2] != 0, sum(map(abs, d))))
DIR_AT = {d: i for i, d in enumerate(DIRS)}


def piece_rows(d):
    dx, dy, dz = d
    if dz == 0:
        if dx and dy:
            return 16
        return 128 if dy else 80
    if dx and dy:
        return 8
    if dy:
        return 32
    return 16 if dx else 64


OFFSETS = {}
RECV_ROWS = 0
for _d in DIRS:
    OFFSETS[_d] = RECV_ROWS
    RECV_ROWS += piece_rows(_d)


def iota(shape, dim):
    return lax.broadcasted_iota(jnp.int32, shape, dim)


def roll_lanes(v, by):
    by = by % 128
    return v if by == 0 else pltpu.roll(v, by, 1)


def roll_rows(v, by):
    return pltpu.roll(v, by % v.shape[0], 0)


def kernel(
    sizes,
    force_hbm, phase_hbm, table, flags,
    press_out, resid_out, norms_out,
    phase, field, ystage, cstage, dstage, y5, recv, r5,
    ext, slab, kmain, kslab, wmain, wslab, smain, sslab, va, vb, sa, sb, inj, edge,
    res, sch, wap, sim, tim, nap, pre,
    red, red1, red2,
    in_sem, out_sem, send_sem, recv_sem, send5_sem, recv5_sem, rs1, rr1, rs2, rr2,
):
    nx, ny, nz = sizes
    at = (lax.axis_index("gx"), lax.axis_index("gy"), lax.axis_index("gz"))

    def neighbour(d):
        ok = None
        for dim in range(3):
            if d[dim] == 0:
                continue
            here = at[dim] < sizes[dim] - 1 if d[dim] > 0 else at[dim] > 0
            ok = here if ok is None else jnp.logical_and(ok, here)
        return ok, tuple(at[dim] + d[dim] for dim in range(3))

    def recv_at(k, d, start=0, rows=None):
        return recv.at[k, pl.ds(OFFSETS[d] + start, piece_rows(d) if rows is None else rows)]

    def pieces(k, d):
        dx, dy, dz = d
        to = tuple(-a for a in d)
        if dz == 0:
            if dx and dy:
                side = 0 if dy < 0 else 1
                src = ystage.at[k, side, pl.ds(0 if dx < 0 else 112, 16)]
                return src, recv_at(k, to)
            if dy:
                return ystage.at[k, 0 if dy < 0 else 1], recv_at(k, to)
            if dx < 0:
                return field.at[k, pl.ds(0, 64)], recv_at(k, to, 0, 64)
            if isinstance(k, int) and k == 0:
                return field.at[k, pl.ds(ROWS - 80, 80)], recv_at(k, to)
            return field.at[k, pl.ds(ROWS - 64, 64)], recv_at(k, to, 16, 64)
        if dx and dy:
            return dstage.at[k, pl.ds(0 if dx < 0 else 24, 8)], recv_at(k, to)
        if dy:
            return dstage.at[k], recv_at(k, to)
        if dx:
            return cstage.at[k, pl.ds(0 if dx < 0 else 48, 16)], recv_at(k, to)
        return cstage.at[k], recv_at(k, to)

    def copy_of(k, d):
        src, dst = pieces(k, d)
        _, device = neighbour(d)
        to = tuple(-a for a in d)
        return pltpu.make_async_remote_copy(
            src_ref=src, dst_ref=dst,
            send_sem=send_sem.at[k, DIR_AT[d]], recv_sem=recv_sem.at[k, DIR_AT[to]],
            device_id=device, device_id_type=MESH,
        )

    def incoming(k, d):
        to = tuple(-a for a in d)
        src, dst = pieces(k, to)
        return pltpu.make_async_remote_copy(
            src_ref=src, dst_ref=dst,
            send_sem=send_sem.at[k, DIR_AT[to]], recv_sem=recv_sem.at[k, DIR_AT[d]],
            device_id=at, device_id_type=MESH,
        )

    sub8 = iota((8, 128), 0)
    lane8 = iota((8, 128), 1)
    group8, slot8 = lane8 // 16, lane8 % 16
    lane24 = iota((24, 128), 1)
    sub24 = iota((24, 128), 0)
    group24, slot24 = lane24 // 16, lane24 % 16


    def pack(k):
        def pair(xp, _):
            base = pl.multiple_of(xp * 32, 32)
            a0, a1 = field[k, pl.ds(base, 8), :], field[k, pl.ds(base + 8, 8), :]
            b0, b1 = field[k, pl.ds(base + 16, 8), :], field[k, pl.ds(base + 24, 8), :]
            to = pl.multiple_of(xp * 8, 8)
            ystage[k, 0, pl.ds(to, 8), :] = jnp.where(sub8 < 4, a0, roll_rows(b0, 4))
            ystage[k, 1, pl.ds(to, 8), :] = jnp.where(sub8 < 4, roll_rows(a1, 4), b1)
            return 0
        lax.fori_loop(0, BX // 2, pair, 0, unroll=8)

        def block(xb, _):
            acc = [[jnp.zeros((8, 128), F32) for _ in range(2)] for _ in range(3)]
            for g in range(8):
                base = pl.multiple_of(xb * 128, 128) + g * 16
                a, b = field[k, pl.ds(base, 8), :], field[k, pl.ds(base + 8, 8), :]
                for i, v in enumerate((a, b, jnp.where(sub8 < 4, a, b))):
                    acc[i][0] = jnp.where(group8 == g, roll_lanes(v, 5 + 16 * g), acc[i][0])
                    acc[i][1] = jnp.where(group8 == g, roll_lanes(v, 12 + 16 * g), acc[i][1])
            a, b, c = (jnp.where(slot8 < 9, u, v) for u, v in acc)
            to = pl.multiple_of(xb * 16, 16)
            cstage[k, pl.ds(to, 8), :] = a
            cstage[k, pl.ds(to + 8, 8), :] = b
            dstage[k, pl.ds(pl.multiple_of(xb * 8, 8), 8), :] = c
            return 0
        lax.fori_loop(0, 4, block, 0, unroll=2)

    def send(k):
        for d in DIRS:
            ok, _ = neighbour(d)

            @pl.when(ok)
            def _():
                copy_of(k, d).start()

    def receive(k):
        for d in DIRS:
            ok, _ = neighbour(d)

            @pl.when(ok)
            def _():
                incoming(k, d).wait_recv()

    def finish_sends(k):
        for d in DIRS:
            ok, _ = neighbour(d)

            @pl.when(ok)
            def _():
                copy_of(k, d).wait_send()

    def unpack(k):
        def planes(own, low, high, first, pairs):
            def pair(xp, _):
                src = pl.multiple_of(xp * 32, 32)
                side = pl.multiple_of(xp * 8, 8)
                lo, hi = low(side), high(side)
                los, his = roll_rows(lo, 4), roll_rows(hi, 4)
                for half in range(2):
                    ra, rb = roll_rows(own(src + 16 * half), 4), roll_rows(own(src + 16 * half + 8), 4)
                    to = pl.multiple_of(xp * 48, 8) + (G + (first + half) * 24)
                    ext[pl.ds(to, 8), :] = jnp.where(sub8 < 4, (lo, los)[half], ra)
                    ext[pl.ds(to + 8, 8), :] = jnp.where(sub8 < 4, ra, rb)
                    ext[pl.ds(to + 16, 8), :] = jnp.where(sub8 < 4, rb, (his, hi)[half])
                return 0
            lax.fori_loop(0, pairs, pair, 0, unroll=min(pairs, 4))

        def of(d, start=0):
            return lambda at_row: recv[k, pl.ds(at_row + (OFFSETS[d] + start), 8), :]

        planes(lambda r: field[k, pl.ds(r, 8), :], of((0, -1, 0)), of((0, 1, 0)), 4, 16)
        planes(of((-1, 0, 0), 16), of((-1, -1, 0)), of((-1, 1, 0)), 0, 2)
        planes(of((1, 0, 0)), of((1, -1, 0)), of((1, 1, 0)), 36, 2)

        def merged(d, row):
            low = recv[k, pl.ds(OFFSETS[(d[0], d[1], -1)] + row, 8), :]
            high = recv[k, pl.ds(OFFSETS[(d[0], d[1], 1)] + row, 8), :]
            return jnp.where(slot8 < 8, low, high)

        inner = []
        for t in range(2):
            inner.append([merged((-1, 0), 8 * t)] + [merged((0, 0), xb * 16 + 8 * t) for xb in range(4)] + [merged((1, 0), 8 * t)])
        sides = []
        for xb in range(6):
            dx, row = (-1, 0) if xb == 0 else (1, 0) if xb == 5 else (0, (xb - 1) * 8)
            sides.append(roll_rows(jnp.where(sub8 < 4, merged((dx, 1), row), merged((dx, -1), row)), 4))

        def shifted(parts, i):
            return roll_lanes(jnp.where(group8 < 4, parts[i + 1], parts[i]), 64)

        for i in range(5):
            a, b = roll_rows(shifted(inner[0], i), 4), roll_rows(shifted(inner[1], i), 4)
            c = shifted(sides, i)
            tiles = (jnp.where(sub8 < 4, c, a), jnp.where(sub8 < 4, a, b), jnp.where(sub8 < 4, b, c))
            for t in range(3):
                slab[pl.ds(G + i * 24 + 8 * t, 8), :] = tiles[t]

        def own(i, _):
            base = pl.multiple_of(i * 192, 8) + G
            to = pl.multiple_of(i * 24, 8) + G
            for t in range(3):
                lo, hi = jnp.zeros((8, 128), F32), jnp.zeros((8, 128), F32)
                for j in range(8):
                    v = ext[pl.ds(base + j * 24 + 8 * t, 8), :]
                    lo = jnp.where(group8 == j, roll_lanes(v, 5 + 16 * j), lo)
                    hi = jnp.where(group8 == j, roll_lanes(v, 12 + 16 * j), hi)
                mine = jnp.where(slot8 < 9, lo, hi)
                old = slab[pl.ds(to + 8 * t, 8), :]
                slab[pl.ds(to + 8 * t, 8), :] = jnp.where((slot8 >= 5) & (slot8 < 12), mine, old)
            return 0
        lax.fori_loop(0, 5, own, 0)


    def make_injection(source, c, rows0, out):
        v = source[c, pl.ds(rows0, 24), :]
        out[c, pl.ds(rows0, 24), :] = jnp.where(slot24 == 5, roll_lanes(v, -7), v)

    def make_edges(comps, first, last):
        def plane(i, j):
            for c in comps:
                v = inj[c, pl.ds(pl.multiple_of(i * 24, 8) + G, 24), :]
                edge[c, pl.ds(row_of(i, j), 24), :] = roll_lanes(v, 123 - 16 * j)
        for_planes(first, last, plane)

    def main_z(v, c, b):
        e = edge[c, pl.ds(b, 24), :]
        up = roll_lanes(jnp.where(lane24 == 0, e, v), 127)
        down = roll_lanes(jnp.where(lane24 == 127, e, v), 1)
        return up, down

    def slab_x(v, below, above):
        up = roll_lanes(jnp.where(lane24 < 16, above, v), -16)
        down = roll_lanes(jnp.where(lane24 >= 112, below, v), 16)
        return up, down

    def for_planes(first, last, body):
        for p in range(first, 8):
            body(0, p)

        def block(i, _):
            for j in range(8):
                body(i, j)
            return 0
        lax.fori_loop(1, 4, block, 0, unroll=3)
        for p in range(32, last + 1):
            body(4, p - 32)

    def row_of(i, j):
        return pl.multiple_of(i * 192, 8) + (G + j * 24)

    def shift_rows(ref, c, base, by):
        return ref[c, pl.ds(base + by, 24), :]


    walls = [jnp.where(flags[f] == 0, F32(1.0), F32(0.0)) for f in range(6)]
    totals = (nx * BX, ny * BY, nz * BZ)

    def coefficients(e, nbrs, spots):
        faces = []
        inside = None
        diag = jnp.zeros_like(e)
        extra = [jnp.zeros_like(e) for _ in range(3)]
        for axis in range(3):
            for side in range(2):
                spot = spots[axis] + (1 if side else -1)
                here = (spot >= 0) & (spot < totals[axis])
                face = 0.5 * (e + nbrs[axis][side])
                wall = walls[2 * axis + side]
                outer = jnp.where(here, F32(0.0), e)
                diag = diag + jnp.where(here, face, e * wall)
                extra[axis] = extra[axis] + outer * (1.0 - wall)
                faces.append(face)
            here = (spots[axis] >= 0) & (spots[axis] < totals[axis])
            inside = here if inside is None else inside & here
        weights = []
        for c in range(3):
            d = diag + extra[c]
            good = inside & (d > 0)
            weights.append(jnp.where(good, OMEGA / jnp.where(good, d, F32(1.0)), F32(0.0)))
        return faces, weights

    def setup():
        for t in range(2):
            v = roll_rows(recv[0, pl.ds(OFFSETS[(-1, 0, 0)] + 8 * t, 8), :], 4)
            if t == 0:
                ext[pl.ds(0, 8), :] = jnp.where(sub8 < 4, F32(0.0), v)
                keep = v
            else:
                ext[pl.ds(8, 8), :] = jnp.where(sub8 < 4, keep, v)
                ext[pl.ds(16, 8), :] = jnp.where(sub8 < 4, v, F32(0.0))

        def injection(i, _):
            base = pl.multiple_of(i * 24, 8) + G
            v = slab[pl.ds(base, 24), :]
            inj[0, pl.ds(base, 24), :] = jnp.where(slot24 == 5, roll_lanes(v, -7), v)
            return 0
        lax.fori_loop(0, 5, injection, 0)
        make_edges((0,), 0, 39)

        def main_block(i, _):
            fives = roll_rows(jnp.where(sub8 < 4, r5[pl.ds(pl.multiple_of(i * 8, 8) + 8, 8), :], r5[pl.ds(pl.multiple_of(i * 8, 8), 8), :]), 4)
            for j in range(8):
                b = row_of(i, j)
                e = ext[pl.ds(b, 24), :]
                up, down = main_z(e, 0, b)
                five = jnp.broadcast_to(fives[j:j + 1, :], (24, 128))
                below = jnp.where(sub24 == 0, five, ext[pl.ds(b - 1, 24), :])
                nbrs = (
                    (ext[pl.ds(b - 24, 24), :], ext[pl.ds(b + 24, 24), :]),
                    (below, ext[pl.ds(b + 1, 24), :]),
                    (down, up),
                )
                spots = (
                    jnp.broadcast_to(at[0] * BX + (i * 8 + j - 4), (24, 128)),
                    sub24 + (at[1] * BY - 4),
                    lane24 + at[2] * BZ,
                )
                faces, weights = coefficients(e, nbrs, spots)
                for f in range(6):
                    kmain[f, pl.ds(b, 24), :] = faces[f]
                for c in range(3):
                    wmain[c, pl.ds(b, 24), :] = weights[c]
            return 0
        lax.fori_loop(0, 5, main_block, 0)

        def slab_block(i, _):
            b = pl.multiple_of(i * 24, 8) + G
            e = slab[pl.ds(b, 24), :]
            xu, xd = slab_x(e, slab[pl.ds(b - 24, 24), :], slab[pl.ds(b + 24, 24), :])
            nbrs = (
                (xd, xu),
                (slab[pl.ds(b - 1, 24), :], slab[pl.ds(b + 1, 24), :]),
                (roll_lanes(e, 1), roll_lanes(e, 127)),
            )
            spots = (
                group24 + (at[0] * BX - 4 + i * 8),
                sub24 + (at[1] * BY - 4),
                jnp.where(slot24 < 9, slot24 - 5, slot24 + 116) + at[2] * BZ,
            )
            faces, weights = coefficients(e, nbrs, spots)
            for f in range(6):
                kslab[f, pl.ds(b, 24), :] = faces[f]
            for c in range(3):
                wslab[c, pl.ds(b, 24), :] = weights[c]
            return 0
        lax.fori_loop(0, 5, slab_block, 0)


    def gradient():
        def slab_block(i, _):
            b = pl.multiple_of(i * 24, 8) + G
            p = slab[pl.ds(b, 24), :]
            above = slab[pl.ds(b + 24, 24), :]
            xu = roll_lanes(jnp.where(lane24 < 16, above, p), -16)
            nbrs = (xu, slab[pl.ds(b + 1, 24), :], roll_lanes(p, 127))
            for c in range(3):
                sslab[c, pl.ds(b, 24), :] = wslab[c, pl.ds(b, 24), :] * (nbrs[c] - p)
            inj[0, pl.ds(b, 24), :] = jnp.where(slot24 == 5, roll_lanes(p, -7), p)
            return 0
        lax.fori_loop(0, 5, slab_block, 0)
        make_edges((0,), 0, 38)

        def plane(i, j):
            b = row_of(i, j)
            p = ext[pl.ds(b, 24), :]
            zu = roll_lanes(jnp.where(lane24 == 0, edge[0, pl.ds(b, 24), :], p), 127)
            nbrs = (ext[pl.ds(b + 24, 24), :], ext[pl.ds(b + 1, 24), :], zu)
            for c in range(3):
                smain[c, pl.ds(b, 24), :] = wmain[c, pl.ds(b, 24), :] * (nbrs[c] - p)
        for_planes(0, 38, plane)

    def scaled_force(c):
        def slab_block(i, _):
            b = pl.multiple_of(i * 24, 8) + G
            sslab[c, pl.ds(b, 24), :] = wslab[c, pl.ds(b, 24), :] * slab[pl.ds(b, 24), :]
            return 0
        lax.fori_loop(0, 5, slab_block, 0)

        def block(i, _):
            for j in range(8):
                b = row_of(i, j)
                smain[c, pl.ds(b, 24), :] = wmain[c, pl.ds(b, 24), :] * ext[pl.ds(b, 24), :]
            return 0
        lax.fori_loop(0, 5, block, 0)

    def injections(source):
        def block(i, _):
            b = pl.multiple_of(i * 24, 8) + G
            for c in range(3):
                make_injection(source, c, b, inj)
            return 0
        lax.fori_loop(0, 5, block, 0, unroll=True)

    def sweep(src, dst, ssrc, sdst, first, last, with_slab):
        injections(ssrc)
        make_edges((0, 1, 2), first, last)

        def plane(i, j):
            b = row_of(i, j)
            k = [kmain[f, pl.ds(b, 24), :] for f in range(6)]
            for c in range(3):
                v = src[c, pl.ds(b, 24), :]
                zu, zd = main_z(v, c, b)
                total = k[0] * src[c, pl.ds(b - 24, 24), :] + k[1] * src[c, pl.ds(b + 24, 24), :]
                total = total + (k[2] * shift_rows(src, c, b, -1) + k[3] * shift_rows(src, c, b, 1))
                total = total + (k[4] * zd + k[5] * zu)
                dst[c, pl.ds(b, 24), :] = (
                    (1.0 - OMEGA) * v + smain[c, pl.ds(b, 24), :] + wmain[c, pl.ds(b, 24), :] * total
                )
        for_planes(first, last, plane)

        def block(i, _):
            b = pl.multiple_of(i * 24, 8) + G
            k = [kslab[f, pl.ds(b, 24), :] for f in range(6)]
            for c in range(3):
                v = ssrc[c, pl.ds(b, 24), :]
                xu, xd = slab_x(v, ssrc[c, pl.ds(b - 24, 24), :], ssrc[c, pl.ds(b + 24, 24), :])
                total = k[0] * xd + k[1] * xu
                total = total + (k[2] * shift_rows(ssrc, c, b, -1) + k[3] * shift_rows(ssrc, c, b, 1))
                total = total + (k[4] * roll_lanes(v, 1) + k[5] * roll_lanes(v, 127))
                sdst[c, pl.ds(b, 24), :] = (
                    (1.0 - OMEGA) * v + sslab[c, pl.ds(b, 24), :] + wslab[c, pl.ds(b, 24), :] * total
                )
            return 0
        lax.fori_loop(0, 5, block, 0, unroll=True)

    def divergence(src, ssrc, out):
        def block(i, _):
            b = pl.multiple_of(i * 24, 8) + G
            make_injection(ssrc, 2, b, inj)
            return 0
        lax.fori_loop(0, 5, block, 0, unroll=True)
        make_edges((2,), 4, 35)

        def plane(i, j):
            b = row_of(i, j) + 4
            x, y, z = (src[c, pl.ds(b, 16), :] for c in range(3))
            zd = roll_lanes(jnp.where(iota((16, 128), 1) == 127, edge[2, pl.ds(b, 16), :], z), 1)
            total = (src[0, pl.ds(b - 24, 16), :] - x) + (src[1, pl.ds(b - 1, 16), :] - y) + (zd - z)
            to = pl.multiple_of(i * 128, 16) + (j * 16 - 64)
            out[pl.ds(to, 16), :] = total
        for_planes(4, 35, plane)

    def apply(out):
        sweep(smain, va, sslab, sa, 1, 37, True)
        sweep(va, vb, sa, sb, 2, 36, True)
        sweep(vb, va, sb, sa, 3, 35, True)
        divergence(va, sa, out)


    me_z = at[2]
    me_xy = at[0] * ny + at[1]
    nxy = nx * ny

    def z_copy(k, off):
        other = lax.rem(me_z + off, nz)
        return pltpu.make_async_remote_copy(
            src_ref=red.at[k], dst_ref=red1.at[k, me_z], send_sem=rs1.at[k, off], recv_sem=rr1.at[k, off],
            device_id=(at[0], at[1], other), device_id_type=MESH,
        )

    def xy_copy(k, ox, oy):
        off = ox * ny + oy
        return pltpu.make_async_remote_copy(
            src_ref=red.at[k], dst_ref=red2.at[k, me_xy], send_sem=rs2.at[k, off], recv_sem=rr2.at[k, off],
            device_id=(lax.rem(at[0] + ox, nx), lax.rem(at[1] + oy, ny), at[2]), device_id_type=MESH,
        )

    offsets_xy = [(ox, oy) for ox in range(nx) for oy in range(ny) if (ox, oy) != (0, 0)]

    def reduce_start(k, value):
        red[k] = value
        red1[k, me_z] = value
        for off in range(1, nz):
            z_copy(k, off).start()

    def reduce_middle(k):
        for off in range(1, nz):
            z_copy(k, off).wait_recv()
        for off in range(1, nz):
            z_copy(k, off).wait_send()
        value = red1[k, 0]
        for i in range(1, nz):
            value = value + red1[k, i]
        red[k] = value
        red2[k, me_xy] = value
        for ox, oy in offsets_xy:
            xy_copy(k, ox, oy).start()

    def reduce_end(k):
        for ox, oy in offsets_xy:
            xy_copy(k, ox, oy).wait_recv()
        for ox, oy in offsets_xy:
            xy_copy(k, ox, oy).wait_send()
        value = red2[k, 0]
        for i in range(1, nxy):
            value = value + red2[k, i]
        value = jnp.broadcast_to(jnp.sum(value, axis=1, keepdims=True), (8, 128))
        return [jnp.broadcast_to(value[i:i + 1, :], (8, 128)) for i in range(3)]


    load_phase = pltpu.make_async_copy(phase_hbm, phase, in_sem.at[0])
    load_force = pltpu.make_async_copy(force_hbm, field.at[pl.ds(1, 3)], in_sem.at[1])
    load_phase.start()
    load_force.start()

    def clear_recv(i, _):
        for k in range(NSETS):
            recv[k, pl.ds(pl.multiple_of(i * 8, 8), 8), :] = jnp.zeros((8, 128), F32)
        return 0
    lax.fori_loop(0, RECV_ROWS // 8, clear_recv, 0, unroll=2)

    for t in range(0, 48, 8):
        r5[pl.ds(t, 8), :] = jnp.zeros((8, 128), F32)

    barrier = pltpu.get_barrier_semaphore()
    count = jnp.int32(0)
    for d in DIRS:
        ok, device = neighbour(d)

        @pl.when(ok)
        def _():
            pl.semaphore_signal(barrier, inc=1, device_id=device, device_id_type=MESH)
        count = count + ok.astype(jnp.int32)
    for off in range(1, nz):
        pl.semaphore_signal(barrier, inc=1, device_id=(at[0], at[1], lax.rem(me_z + off, nz)), device_id_type=MESH)
    for ox, oy in offsets_xy:
        pl.semaphore_signal(
            barrier, inc=1, device_id=(lax.rem(at[0] + ox, nx), lax.rem(at[1] + oy, ny), at[2]), device_id_type=MESH
        )
    count = count + (nz - 1 + nxy - 1)

    zero24 = jnp.zeros((24, 128), F32)
    for ref, rows in ((ext, EROWS), (slab, SROWS)):
        ref[pl.ds(0, 24), :] = zero24
        ref[pl.ds(rows - 24, 24), :] = zero24
    for ref, rows in ((smain, EROWS), (va, EROWS), (vb, EROWS), (sslab, SROWS), (sa, SROWS), (sb, SROWS)):
        for c in range(3):
            ref[c, pl.ds(0, 24), :] = zero24
            ref[c, pl.ds(rows - 24, 24), :] = zero24
    for ref in (smain, va, vb):
        for c in range(3):
            for xx in (0, 1, 2, 37, 38, 39):
                ref[c, pl.ds(G + xx * 24, 24), :] = zero24

    load_phase.wait()

    def lookup(i, _):
        for u in range(4):
            r = pl.multiple_of(i * 32, 32) + 8 * u
            ids = phase[pl.ds(r, 8), :]
            eta = jnp.zeros((8, 128), F32)
            for level in range(8):
                eta = eta + jnp.where(ids == level, table[level], F32(0.0))
            field[0, pl.ds(r, 8), :] = eta
        return 0
    lax.fori_loop(0, ROWS // 32, lookup, 0)
    pack(0)
    for x in range(BX):
        y5[pl.ds(x, 1), :] = field[0, pl.ds(x * 16 + 11, 1), :]
    pl.semaphore_wait(barrier, count)
    send(0)
    has_y_up, _ = neighbour((0, 1, 0))
    has_y_down, _ = neighbour((0, -1, 0))
    copy5_out = pltpu.make_async_remote_copy(
        src_ref=y5, dst_ref=r5.at[pl.ds(8, 32)], send_sem=send5_sem, recv_sem=recv5_sem,
        device_id=(at[0], at[1] + 1, at[2]), device_id_type=MESH,
    )

    @pl.when(has_y_up)
    def _():
        copy5_out.start()
    load_force.wait()

    def send_force(k, _):
        pack(k)
        send(k)
        return 0
    lax.fori_loop(1, 4, send_force, 0)
    receive(0)

    @pl.when(has_y_down)
    def _():
        copy5_out.wait_recv()
    unpack(0)
    setup()

    def take_force(k, _):
        receive(k)
        unpack(k)
        scaled_force(k - 1)
        return 0
    lax.fori_loop(1, 4, take_force, 0)
    apply(res)

    def rows_loop(body, init, step=4):
        def block(i, carry):
            for u in range(step):
                carry = body(pl.multiple_of(i * (8 * step), 8 * step) + 8 * u, carry)
            return carry
        return lax.fori_loop(0, ROWS // (8 * step), block, init)

    def first(r, _):
        field[4, pl.ds(r, 8), :] = field[0, pl.ds(r, 8), :] * res[pl.ds(r, 8), :]
        return 0
    rows_loop(first, 0)

    def schur(k, out):
        receive(k)
        unpack(k)
        gradient()
        apply(out)

    pack(4)
    send(4)
    schur(4, wap)

    zero8 = jnp.zeros((8, 128), F32)

    def partials(gamma, delta, squares):
        sums = [jnp.broadcast_to(jnp.sum(v, axis=0, keepdims=True), (8, 128)) for v in (gamma, delta, squares)]
        return jnp.where(sub8 == 0, sums[0], jnp.where(sub8 == 1, sums[1], jnp.where(sub8 == 2, sums[2], F32(0.0))))

    def start0(r, carry):
        rr, w, e = (ref[pl.ds(r, 8), :] for ref in (res, wap, field.at[0]))
        z = e * rr
        field[5, pl.ds(r, 8), :] = e * w
        return carry[0] + rr * z, carry[1] + w * z, carry[2] + rr * rr
    sums = rows_loop(start0, (zero8, zero8, zero8))
    pack(5)
    send(5)
    reduce_start(0, partials(*sums))
    receive(5)
    reduce_middle(0)
    unpack(5)
    gradient()
    apply(nap)
    gamma, delta, squares = reduce_end(0)
    cells = float(totals[0] * totals[1] * totals[2])
    norms = [squares / cells]
    alpha = gamma / delta

    def step0(r, carry):
        at_r = pl.ds(r, 8)
        e, rr, w, n = field[0, at_r, :], res[at_r, :], wap[at_r, :], nap[at_r, :]
        p = e * rr
        sch[at_r, :] = p
        sim[at_r, :] = w
        tim[at_r, :] = n
        pre[at_r, :] = alpha * p
        rr = rr - alpha * w
        w = w - alpha * n
        res[at_r, :] = rr
        wap[at_r, :] = w
        z = e * rr
        field[6, at_r, :] = e * w
        return carry[0] + rr * z, carry[1] + w * z, carry[2] + rr * rr
    sums = rows_loop(step0, (zero8, zero8, zero8))
    pack(6)
    send(6)
    reduce_start(1, partials(*sums))
    receive(6)
    reduce_middle(1)
    unpack(6)
    gradient()
    apply(nap)
    gamma_old, alpha_old = gamma, alpha
    gamma, delta, squares = reduce_end(1)
    norms.append(squares / cells)
    beta = gamma / gamma_old
    alpha = gamma / (delta - beta * gamma / alpha_old)

    def step1(r, carry):
        at_r = pl.ds(r, 8)
        e, rr, w, n = field[0, at_r, :], res[at_r, :], wap[at_r, :], nap[at_r, :]
        p = e * rr + beta * sch[at_r, :]
        s = w + beta * sim[at_r, :]
        t = n + beta * tim[at_r, :]
        sch[at_r, :] = p
        sim[at_r, :] = s
        pre[at_r, :] = pre[at_r, :] + alpha * p
        rr = rr - alpha * s
        w = w - alpha * t
        res[at_r, :] = rr
        wap[at_r, :] = w
        z = e * rr
        return carry[0] + rr * z, carry[1] + w * z, carry[2] + rr * rr
    sums = rows_loop(step1, (zero8, zero8, zero8))
    reduce_start(2, partials(*sums))
    reduce_middle(2)
    gamma_old, alpha_old = gamma, alpha
    gamma, delta, squares = reduce_end(2)
    norms.append(squares / cells)
    beta = gamma / gamma_old
    alpha = gamma / (delta - beta * gamma / alpha_old)

    def step2(r, _):
        at_r = pl.ds(r, 8)
        rr = res[at_r, :]
        p = field[0, at_r, :] * rr + beta * sch[at_r, :]
        s = wap[at_r, :] + beta * sim[at_r, :]
        pre[at_r, :] = pre[at_r, :] + alpha * p
        res[at_r, :] = rr - alpha * s
        return 0
    rows_loop(step2, 0)
    store_press = pltpu.make_async_copy(pre, press_out, out_sem.at[0])
    store_resid = pltpu.make_async_copy(res, resid_out, out_sem.at[1])
    store_press.start()
    store_resid.start()
    norms_out[...] = jnp.where(lane8 == 0, norms[0], jnp.where(lane8 == 1, norms[1], norms[2]))

    for k in range(NSETS):
        finish_sends(k)

    @pl.when(has_y_up)
    def _():
        copy5_out.wait_send()
    store_press.wait()
    store_resid.wait()


def solution(mesh):
    sizes = (mesh.shape["gx"], mesh.shape["gy"], mesh.shape["gz"])
    nx, ny, nz = sizes

    def per_device(force, phase, table, flags):
        v = functools.partial(pltpu.VMEM)
        dma = pltpu.SemaphoreType.DMA
        scratch = [
            v((ROWS, 128), jnp.int32),
            v((NSETS, ROWS, 128), F32),
            v((NSETS, 2, 128, 128), F32),
            v((NSETS, 64, 128), F32),
            v((NSETS, 32, 128), F32),
            v((32, 128), F32),
            v((NSETS, RECV_ROWS, 128), F32),
            v((48, 128), F32),
            v((EROWS, 128), F32), v((SROWS, 128), F32),
            v((6, EROWS, 128), F32), v((6, SROWS, 128), F32),
            v((3, EROWS, 128), F32), v((3, SROWS, 128), F32),
            v((3, EROWS, 128), F32), v((3, SROWS, 128), F32),
            v((3, EROWS, 128), F32), v((3, EROWS, 128), F32),
            v((3, SROWS, 128), F32), v((3, SROWS, 128), F32),
            v((3, SROWS, 128), F32), v((3, EROWS, 128), F32),
            *[v((ROWS, 128), F32) for _ in range(7)],
            v((ITERS, 8, 128), F32), v((ITERS, nz, 8, 128), F32), v((ITERS, nx * ny, 8, 128), F32),
            dma((2,)), dma((2,)), dma((NSETS, 26)), dma((NSETS, 26)), dma, dma,
            dma((ITERS, nz)), dma((ITERS, nz)), dma((ITERS, nx * ny)), dma((ITERS, nx * ny)),
        ]
        hbm = pl.BlockSpec(memory_space=pl.ANY)
        smem = pl.BlockSpec(memory_space=pltpu.SMEM)
        press, resid, norms = pl.pallas_call(
            functools.partial(kernel, sizes),
            out_shape=(
                jax.ShapeDtypeStruct((ROWS, 128), F32),
                jax.ShapeDtypeStruct((ROWS, 128), F32),
                jax.ShapeDtypeStruct((8, 128), F32),
            ),
            in_specs=[hbm, hbm, smem, smem],
            out_specs=(hbm, hbm, pl.BlockSpec(memory_space=pltpu.VMEM)),
            scratch_shapes=scratch,
            compiler_params=pltpu.CompilerParams(
                collective_id=0, has_side_effects=True, vmem_limit_bytes=60 * 1024 * 1024
            ),
        )(force.reshape(3, ROWS, BZ), phase.reshape(ROWS, BZ), table, flags)
        return press.reshape(BX, BY, BZ), resid.reshape(BX, BY, BZ), norms[0, :ITERS]

    return jax.shard_map(
        per_device,
        mesh=mesh,
        in_specs=(P(None, "gx", "gy", "gz"), P("gx", "gy", "gz"), P(), P()),
        out_specs=(P("gx", "gy", "gz"), P("gx", "gy", "gz"), P()),
        check_vma=False,
    )
```

```python
import functools

import jax
import jax.numpy as jnp
from jax import lax
from jax.experimental import pallas as pl
from jax.experimental.pallas import tpu as pltpu
from jax.sharding import PartitionSpec as P

ITERS = 3
OMEGA = 0.8
F32 = jnp.float32
MESH = pl.DeviceIdType.MESH

BX, BY, BZ = 32, 16, 128
ROWS = BX * BY
PLANES = 53
EROWS = PLANES * 24
NSETS = 7

DIRS = [(dx, dy, dz) for dz in (0, 1, -1) for dy in (1, -1, 0) for dx in (0, 1, -1) if (dx, dy, dz) != (0, 0, 0)]
DIRS.sort(key=lambda d: (d[1] == 0 or d[0] != 0 or d[2] != 0, sum(map(abs, d))))
DIR_AT = {d: i for i, d in enumerate(DIRS)}


def piece_rows(d):
    dx, dy, dz = d
    if dz == 0:
        if dx and dy:
            return 16
        return 128 if dy else 80
    if dx and dy:
        return 8
    if dy:
        return 32
    return 16 if dx else 64


OFFSETS = {}
RECV_ROWS = 0
for _d in DIRS:
    OFFSETS[_d] = RECV_ROWS
    RECV_ROWS += piece_rows(_d)


def iota(shape, dim):
    return lax.broadcasted_iota(jnp.int32, shape, dim)


def roll_lanes(v, by):
    by = by % 128
    return v if by == 0 else pltpu.roll(v, by, 1)


def roll_rows(v, by):
    return pltpu.roll(v, by % v.shape[0], 0)


def kernel(
    sizes,
    force_hbm, phase_hbm, table, flags,
    press_out, resid_out, norms_out,
    phase, field, ystage, cstage, dstage, y5, recv, r5, f5,
    ext, faces, weights, source, va, vb, halo, dslab,
    res, sch, wap, sim, tim, nap, pre,
    red, red1, red2, scal, norm,
    in_sem, send_sem, recv_sem, send5_sem, recv5_sem, rs1, rr1, rs2, rr2,
):
    nx, ny, nz = sizes
    at = (lax.axis_index("gx"), lax.axis_index("gy"), lax.axis_index("gz"))

    def neighbour(d):
        ok = None
        for dim in range(3):
            if d[dim] == 0:
                continue
            here = at[dim] < sizes[dim] - 1 if d[dim] > 0 else at[dim] > 0
            ok = here if ok is None else jnp.logical_and(ok, here)
        return ok, tuple(at[dim] + d[dim] for dim in range(3))

    def recv_at(k, d, start=0, rows=None):
        return recv.at[k, pl.ds(OFFSETS[d] + start, piece_rows(d) if rows is None else rows)]

    def pieces(k, d):
        dx, dy, dz = d
        to = tuple(-a for a in d)
        if dz == 0:
            if dx and dy:
                side = 0 if dy < 0 else 1
                src = ystage.at[k, side, pl.ds(0 if dx < 0 else 112, 16)]
                return src, recv_at(k, to)
            if dy:
                return ystage.at[k, 0 if dy < 0 else 1], recv_at(k, to)
            if dx < 0:
                return field.at[k, pl.ds(0, 64)], recv_at(k, to, 0, 64)
            return field.at[k, pl.ds(ROWS - 80, 80)], recv_at(k, to)
        if dx and dy:
            return dstage.at[k, pl.ds(0 if dx < 0 else 24, 8)], recv_at(k, to)
        if dy:
            return dstage.at[k], recv_at(k, to)
        if dx:
            return cstage.at[k, pl.ds(0 if dx < 0 else 48, 16)], recv_at(k, to)
        return cstage.at[k], recv_at(k, to)

    def copy_of(k, d):
        src, dst = pieces(k, d)
        _, device = neighbour(d)
        to = tuple(-a for a in d)
        return pltpu.make_async_remote_copy(
            src_ref=src, dst_ref=dst,
            send_sem=send_sem.at[k, DIR_AT[d]], recv_sem=recv_sem.at[k, DIR_AT[to]],
            device_id=device, device_id_type=MESH,
        )

    def incoming(k, d):
        to = tuple(-a for a in d)
        src, dst = pieces(k, to)
        return pltpu.make_async_remote_copy(
            src_ref=src, dst_ref=dst,
            send_sem=send_sem.at[k, DIR_AT[to]], recv_sem=recv_sem.at[k, DIR_AT[d]],
            device_id=at, device_id_type=MESH,
        )

    sub8 = iota((8, 128), 0)
    lane8 = iota((8, 128), 1)
    group8, slot8 = lane8 // 16, lane8 % 16
    lane24 = iota((24, 128), 1)
    sub24 = iota((24, 128), 0)
    group24, slot24 = lane24 // 32, lane24 % 32
    bigroup8, bislot8 = lane8 // 32, lane8 % 32


    def pack_y(k):
        def pair(xp, _):
            base = pl.multiple_of(xp * 32, 32)
            a0, a1 = field[k, pl.ds(base, 8), :], field[k, pl.ds(base + 8, 8), :]
            b0, b1 = field[k, pl.ds(base + 16, 8), :], field[k, pl.ds(base + 24, 8), :]
            to = pl.multiple_of(xp * 8, 8)
            ystage[k, 0, pl.ds(to, 8), :] = jnp.where(sub8 < 4, a0, roll_rows(b0, 4))
            ystage[k, 1, pl.ds(to, 8), :] = jnp.where(sub8 < 4, roll_rows(a1, 4), b1)
            return 0
        lax.fori_loop(0, BX // 2, pair, 0, unroll=16)

    def pack_z(k):
        def block(xb, _):
            acc = [[jnp.zeros((8, 128), F32) for _ in range(2)] for _ in range(3)]
            for g in range(8):
                base = pl.multiple_of(xb * 128, 128) + g * 16
                a, b = field[k, pl.ds(base, 8), :], field[k, pl.ds(base + 8, 8), :]
                for i, v in enumerate((a, b, jnp.where(sub8 < 4, a, b))):
                    acc[i][0] = jnp.where(group8 == g, roll_lanes(v, 16 * g), acc[i][0])
                    acc[i][1] = jnp.where(group8 == g, roll_lanes(v, 9 + 16 * g), acc[i][1])
            a, b, c = (jnp.where(slot8 < 4, u, v) for u, v in acc)
            to = pl.multiple_of(xb * 16, 16)
            cstage[k, pl.ds(to, 8), :] = a
            cstage[k, pl.ds(to + 8, 8), :] = b
            dstage[k, pl.ds(pl.multiple_of(xb * 8, 8), 8), :] = c
            return 0
        lax.fori_loop(0, 4, block, 0, unroll=4)

    flat = [d for d in DIRS if d[2] == 0]
    deep = [d for d in DIRS if d[2] != 0]

    def send(k, dirs):
        for d in dirs:
            ok, _ = neighbour(d)

            @pl.when(ok)
            def _():
                copy_of(k, d).start()

    def exchange_start(k):
        pack_y(k)
        send(k, flat)
        pack_z(k)
        send(k, deep)

    def receive(k, dirs):
        for d in dirs:
            ok, _ = neighbour(d)

            @pl.when(ok)
            def _():
                incoming(k, d).wait_recv()

    def finish_sends(k):
        for d in DIRS:
            ok, _ = neighbour(d)

            @pl.when(ok)
            def _():
                copy_of(k, d).wait_send()

    def main_row(x):
        return (1 + x) * 24

    def slab_row(l):
        return (42 + l) * 24

    def refresh(ref):
        low, high = pl.ds(slab_row(9), 24), pl.ds(slab_row(0), 24)
        ref[pl.ds(slab_row(-1), 24), :] = roll_lanes(ref[low, :], 32)
        ref[pl.ds(slab_row(10), 24), :] = roll_lanes(ref[high, :], -32)

    def unpack(k):
        receive(k, flat)

        def planes(own, low, high, first, pairs):
            for xp in range(pairs):
                lo, hi = low(xp * 8), high(xp * 8)
                los, his = roll_rows(lo, 4), roll_rows(hi, 4)
                for half in range(2):
                    ra, rb = (roll_rows(own(xp * 32 + 16 * half + 8 * t), 4) for t in range(2))
                    to = main_row(first + 2 * xp + half)
                    ext[pl.ds(to, 8), :] = jnp.where(sub8 < 4, (lo, los)[half], ra)
                    ext[pl.ds(to + 8, 8), :] = jnp.where(sub8 < 4, ra, rb)
                    ext[pl.ds(to + 16, 8), :] = jnp.where(sub8 < 4, rb, (his, hi)[half])

        def of(d, start=0):
            return lambda row: recv[k, pl.ds(row + (OFFSETS[d] + start), 8), :]

        planes(lambda r: field[k, pl.ds(r, 8), :], of((0, -1, 0)), of((0, 1, 0)), 4, 16)
        planes(of((-1, 0, 0), 16), of((-1, -1, 0)), of((-1, 1, 0)), 0, 2)
        planes(of((1, 0, 0)), of((1, -1, 0)), of((1, 1, 0)), 36, 2)

        def own(i, _):
            for u in range(5):
                for t in range(3):
                    lo, hi = None, None
                    for h in range(4):
                        v = ext[pl.ds(pl.multiple_of(i * 120, 8) + (main_row(10 * h + u) + 8 * t), 8), :]
                        a, b = roll_lanes(v, 32 * h + 9), roll_lanes(v, 32 * h + 18)
                        lo = a if h == 0 else jnp.where(bigroup8 == h, a, lo)
                        hi = b if h == 0 else jnp.where(bigroup8 == h, b, hi)
                    to = pl.ds(pl.multiple_of(i * 120, 8) + (slab_row(u) + 8 * t), 8)
                    ext[to, :] = jnp.where(bislot8 < 9, lo, hi)
            return 0
        lax.fori_loop(0, 2, own, 0)
        receive(k, deep)

        def merged(d, row):
            low = recv[k, pl.ds(OFFSETS[(d[0], d[1], -1)] + row, 8), :]
            high = recv[k, pl.ds(OFFSETS[(d[0], d[1], 1)] + row, 8), :]
            return jnp.where(slot8 < 4, high, low)

        inner = []
        for t in range(2):
            inner.append([merged((-1, 0), 8 * t)] + [merged((0, 0), xb * 16 + 8 * t) for xb in range(4)] + [merged((1, 0), 8 * t)])
        sides = []
        for xb in range(6):
            dx, row = (-1, 0) if xb == 0 else (1, 0) if xb == 5 else (0, (xb - 1) * 8)
            sides.append(roll_rows(jnp.where(sub8 < 4, merged((dx, 1), row), merged((dx, -1), row)), 4))

        def shifted(parts, i):
            return roll_lanes(jnp.where(group8 < 4, parts[i + 1], parts[i]), 64)

        def arrived(_, carry):
            for i in range(5):
                a, b = roll_rows(shifted(inner[0], i), 4), roll_rows(shifted(inner[1], i), 4)
                c = shifted(sides, i)
                tiles = (jnp.where(sub8 < 4, c, a), jnp.where(sub8 < 4, a, b), jnp.where(sub8 < 4, b, c))
                for t in range(3):
                    halo[pl.ds(i * 24 + 8 * t, 8), :] = tiles[t]
            return carry
        lax.fori_loop(0, 1, arrived, 0)

        def outer(l, _):
            for t in range(3):
                acc = None
                for h in range(4):
                    x = 10 * h + l
                    v = halo[pl.ds(x // 8 * 24 + 8 * t, 8), :]
                    a = roll_lanes(v, 32 * h + 9 - 16 * (x % 8))
                    acc = a if h == 0 else jnp.where(bigroup8 == h, a, acc)
                to = pl.ds(slab_row(l) + 8 * t, 8)
                ext[to, :] = jnp.where((bislot8 >= 9) & (bislot8 < 18), acc, ext[to, :])
            return 0
        for l in range(10):
            outer(l, 0)


    walls = [jnp.where(flags[f] == 0, F32(1.0), F32(0.0)) for f in range(6)]
    totals = (nx * BX, ny * BY, nz * BZ)

    def coefficients(b, e, nbrs, spots):
        inside = None
        diag = jnp.zeros_like(e)
        extra = [jnp.zeros_like(e) for _ in range(3)]
        for axis in range(3):
            for side in range(2):
                spot = spots[axis] + (1 if side else -1)
                here = (spot >= 0) & (spot < totals[axis])
                face = 0.5 * (e + nbrs[axis][side])
                wall = walls[2 * axis + side]
                outer = jnp.where(here, F32(0.0), e)
                diag = diag + jnp.where(here, face, e * wall)
                extra[axis] = extra[axis] + outer * (1.0 - wall)
                faces[2 * axis + side, pl.ds(b, 24), :] = face
            here = (spots[axis] >= 0) & (spots[axis] < totals[axis])
            inside = here if inside is None else inside & here
        for c in range(3):
            d = diag + extra[c]
            good = inside & (d > 0)
            weights[c, pl.ds(b, 24), :] = jnp.where(good, OMEGA / jnp.where(good, d, F32(1.0)), F32(0.0))

    def setup():
        keep = None
        for t in range(2):
            v = roll_rows(recv[0, pl.ds(OFFSETS[(-1, 0, 0)] + 8 * t, 8), :], 4)
            if t == 0:
                ext[pl.ds(0, 8), :] = jnp.where(sub8 < 4, F32(0.0), v)
                keep = v
            else:
                ext[pl.ds(8, 8), :] = jnp.where(sub8 < 4, keep, v)
                ext[pl.ds(16, 8), :] = jnp.where(sub8 < 4, v, F32(0.0))
        first = ext[pl.ds(0, 24), :]
        first = jnp.where(slot24 < 9, roll_lanes(first, 9), roll_lanes(first, 18))
        low = pl.ds(slab_row(-1), 24)
        ext[low, :] = jnp.where(group24 == 0, first, ext[low, :])
        five = None
        lane16 = iota((16, 128), 1)
        for h in range(4):
            v = r5[pl.ds(10 * h + 4, 16), :]
            v = jnp.where(lane16 % 32 < 9, roll_lanes(v, 32 * h + 9), roll_lanes(v, 32 * h + 18))
            five = v if h == 0 else jnp.where(lane16 // 32 == h, v, five)
        f5[...] = five

        def neighbours(b, below):
            e = ext[pl.ds(b, 24), :]
            return e, (
                (ext[pl.ds(b - 24, 24), :], ext[pl.ds(b + 24, 24), :]),
                (jnp.where(sub24 == 0, below, ext[pl.ds(b - 1, 24), :]), ext[pl.ds(b + 1, 24), :]),
                (roll_lanes(e, 1), roll_lanes(e, 127)),
            )

        ys = sub24 + (at[1] * BY - 4)

        def main_block(i, _):
            fives = roll_rows(jnp.where(sub8 < 4, r5[pl.ds(pl.multiple_of(i * 8, 8) + 8, 8), :], r5[pl.ds(pl.multiple_of(i * 8, 8), 8), :]), 4)
            for j in range(8):
                b = pl.multiple_of(i * 192, 8) + main_row(j)
                e, nbrs = neighbours(b, jnp.broadcast_to(fives[j:j + 1, :], (24, 128)))
                coefficients(b, e, nbrs, (
                    jnp.broadcast_to(at[0] * BX + (i * 8 + j - 4), (24, 128)), ys, lane24 + at[2] * BZ,
                ))
            return 0
        lax.fori_loop(0, 5, main_block, 0)
        zs = jnp.where(slot24 < 13, slot24 + 119, slot24 - 18) + at[2] * BZ

        for l in range(10):
            b = slab_row(l)
            e, nbrs = neighbours(b, jnp.broadcast_to(f5[l:l + 1, :], (24, 128)))
            coefficients(b, e, nbrs, (group24 * 10 + (at[0] * BX - 4 + l), ys, zs))


    SLAB = [slab_row(l) for l in range(10)]

    def gradient():
        for b in SLAB + [main_row(x) for x in range(39)]:
            p = ext[pl.ds(b, 24), :]
            nbrs = (ext[pl.ds(b + 24, 24), :], ext[pl.ds(b + 1, 24), :], roll_lanes(p, 127))
            for c in range(3):
                source[c, pl.ds(b, 24), :] = weights[c, pl.ds(b, 24), :] * (nbrs[c] - p)

    def scaled_force(c):
        def block(i, _):
            for u in range(13):
                b = pl.multiple_of(i * 312, 8) + 24 * (u + 1)
                source[c, pl.ds(b, 24), :] = weights[c, pl.ds(b, 24), :] * ext[pl.ds(b, 24), :]
            return 0
        lax.fori_loop(0, 4, block, 0)

    def ends(ref):
        def each(c, _):
            refresh(ref.at[c])
            return 0
        lax.fori_loop(0, 3, each, 0, unroll=3)

    def sweep(src, dst, first, last):
        for b in SLAB + [main_row(x) for x in range(first, last + 1)]:
            k = [faces[f, pl.ds(b, 24), :] for f in range(6)]
            for c in range(3):
                v = src[c, pl.ds(b, 24), :]
                total = k[0] * src[c, pl.ds(b - 24, 24), :] + k[1] * src[c, pl.ds(b + 24, 24), :]
                total = total + (k[2] * src[c, pl.ds(b - 1, 24), :] + k[3] * src[c, pl.ds(b + 1, 24), :])
                total = total + (k[4] * roll_lanes(v, 1) + k[5] * roll_lanes(v, 127))
                dst[c, pl.ds(b, 24), :] = (
                    (1.0 - OMEGA) * v + source[c, pl.ds(b, 24), :] + weights[c, pl.ds(b, 24), :] * total
                )
        ends(dst)

    def minus_divergence(src, b, rows):
        x, y, z = (src[c, pl.ds(b, rows), :] for c in range(3))
        return (src[0, pl.ds(b - 24, rows), :] - x) + (src[1, pl.ds(b - 1, rows), :] - y) + (roll_lanes(z, 1) - z)

    def divergence(src, out):
        def slab_part(i, _):
            for u in range(5):
                b = pl.multiple_of(i * 120, 8) + slab_row(u)
                dslab[pl.ds(pl.multiple_of(i * 120, 8) + u * 24, 24), :] = minus_divergence(src, b, 24)
            return 0
        lax.fori_loop(0, 2, slab_part, 0)

        def together(i, _):
            for u in range(5):
                b = pl.ds(pl.multiple_of(i * 120, 8) + u * 24, 24)
                v = dslab[b, :]
                dslab[b, :] = jnp.where(slot24 < 9, v, roll_lanes(v, -9))
            return 0
        lax.fori_loop(0, 2, together, 0)
        lane16 = iota((16, 128), 1)
        for x in range(4, 36):
            h, l = divmod(x, 10)
            total = minus_divergence(src, main_row(x) + 4, 16)
            edge = roll_lanes(dslab[pl.ds(l * 24 + 4, 16), :], -(9 + 32 * h))
            out[pl.ds((x - 4) * 16, 16), :] = jnp.where((lane16 < 8) | (lane16 >= 124), edge, total)

    def apply(out):
        ends(source)
        sweep(source, va, 1, 37)
        sweep(va, vb, 2, 36)
        sweep(vb, va, 3, 35)
        divergence(va, out)


    me_z = at[2]
    me_xy = at[0] * ny + at[1]
    nxy = nx * ny

    def z_copy(k, off):
        other = lax.rem(me_z + off, nz)
        return pltpu.make_async_remote_copy(
            src_ref=red.at[k], dst_ref=red1.at[k, me_z], send_sem=rs1.at[k, off], recv_sem=rr1.at[k, off],
            device_id=(at[0], at[1], other), device_id_type=MESH,
        )

    def xy_copy(k, ox, oy):
        off = ox * ny + oy
        return pltpu.make_async_remote_copy(
            src_ref=red.at[k], dst_ref=red2.at[k, me_xy], send_sem=rs2.at[k, off], recv_sem=rr2.at[k, off],
            device_id=(lax.rem(at[0] + ox, nx), lax.rem(at[1] + oy, ny), at[2]), device_id_type=MESH,
        )

    offsets_xy = [(ox, oy) for ox in range(nx) for oy in range(ny) if (ox, oy) != (0, 0)]

    def reduce_start(k):
        red1[k, me_z] = red[k]
        for off in range(1, nz):
            z_copy(k, off).start()

    def reduce_middle(k):
        for off in range(1, nz):
            z_copy(k, off).wait_recv()
        for off in range(1, nz):
            z_copy(k, off).wait_send()
        value = red1[k, 0]
        for i in range(1, nz):
            value = value + red1[k, i]
        red[k] = value
        red2[k, me_xy] = value
        for ox, oy in offsets_xy:
            xy_copy(k, ox, oy).start()

    cells = float(totals[0] * totals[1] * totals[2])

    def reduce_end(k):
        for ox, oy in offsets_xy:
            xy_copy(k, ox, oy).wait_recv()
        for ox, oy in offsets_xy:
            xy_copy(k, ox, oy).wait_send()
        value = red2[k, 0]
        for i in range(1, nxy):
            value = value + red2[k, i]
        value = jnp.broadcast_to(jnp.sum(value, axis=1, keepdims=True), (8, 128))
        gamma, delta, squares = (jnp.broadcast_to(value[i:i + 1, :], (8, 128)) for i in range(3))
        norm[k] = squares / cells
        gamma_old, alpha_old = scal[0], scal[1]
        if isinstance(k, int):
            beta = gamma / gamma_old
            alpha = gamma / (delta - beta * gamma / alpha_old)
        else:
            beta = jnp.where(k == 0, F32(0.0), gamma / gamma_old)
            alpha = gamma / (delta - jnp.where(k == 0, F32(0.0), beta * gamma / alpha_old))
        scal[0] = gamma
        scal[1] = alpha
        return alpha, beta


    load_phase = pltpu.make_async_copy(phase_hbm, phase, in_sem.at[0])
    load_force = pltpu.make_async_copy(force_hbm, field.at[pl.ds(1, 3)], in_sem.at[1])
    load_phase.start()
    load_force.start()

    def clear_recv(i, _):
        for k in range(NSETS):
            recv[k, pl.ds(pl.multiple_of(i * 8, 8), 8), :] = jnp.zeros((8, 128), F32)
        return 0
    lax.fori_loop(0, RECV_ROWS // 8, clear_recv, 0, unroll=2)

    for t in range(0, 56, 8):
        r5[pl.ds(t, 8), :] = jnp.zeros((8, 128), F32)

    barrier = pltpu.get_barrier_semaphore()
    count = jnp.int32(0)
    for d in DIRS:
        ok, device = neighbour(d)

        @pl.when(ok)
        def _():
            pl.semaphore_signal(barrier, inc=1, device_id=device, device_id_type=MESH)
        count = count + ok.astype(jnp.int32)
    for off in range(1, nz):
        pl.semaphore_signal(barrier, inc=1, device_id=(at[0], at[1], lax.rem(me_z + off, nz)), device_id_type=MESH)
    for ox, oy in offsets_xy:
        pl.semaphore_signal(
            barrier, inc=1, device_id=(lax.rem(at[0] + ox, nx), lax.rem(at[1] + oy, ny), at[2]), device_id_type=MESH
        )
    count = count + (nz - 1 + nxy - 1)

    zero24 = jnp.zeros((24, 128), F32)
    ext[pl.ds(0, 24), :] = zero24
    for ref in (source, va, vb):
        for c in range(3):
            for plane in (0, 1, 2, 3, 38, 39, 40, 41, 52):
                ref[c, pl.ds(plane * 24, 24), :] = zero24
    for f in range(6):
        faces[f, pl.ds(41 * 24, 24), :] = zero24
    for c in range(3):
        weights[c, pl.ds(41 * 24, 24), :] = zero24
        weights[c, pl.ds(52 * 24, 24), :] = zero24
    zero8 = jnp.zeros((8, 128), F32)
    scal[0] = zero8 + 1.0
    scal[1] = zero8 + 1.0
    for ref in (sch, sim, tim, pre):
        def clear(i, _):
            ref[pl.ds(pl.multiple_of(i * 64, 64), 64), :] = jnp.zeros((64, 128), F32)
            return 0
        lax.fori_loop(0, ROWS // 64, clear, 0)

    load_phase.wait()

    def lookup(i, _):
        for u in range(4):
            r = pl.multiple_of(i * 32, 32) + 8 * u
            ids = phase[pl.ds(r, 8), :]
            eta = jnp.zeros((8, 128), F32)
            for level in range(8):
                eta = eta + jnp.where(ids == level, table[level], F32(0.0))
            field[0, pl.ds(r, 8), :] = eta
        return 0
    lax.fori_loop(0, ROWS // 32, lookup, 0)
    for x in range(BX):
        y5[pl.ds(x, 1), :] = field[0, pl.ds(x * 16 + 11, 1), :]
    pl.semaphore_wait(barrier, count)
    has_y_up, _ = neighbour((0, 1, 0))
    has_y_down, _ = neighbour((0, -1, 0))
    copy5_out = pltpu.make_async_remote_copy(
        src_ref=y5, dst_ref=r5.at[pl.ds(8, 32)], send_sem=send5_sem, recv_sem=recv5_sem,
        device_id=(at[0], at[1] + 1, at[2]), device_id_type=MESH,
    )

    @pl.when(has_y_up)
    def _():
        copy5_out.start()

    def send_first(k, _):
        @pl.when(k == 1)
        def _():
            load_force.wait()
        exchange_start(k)
        return 0
    lax.fori_loop(0, 4, send_first, 0)

    def rows_loop(body, init, step=8):
        def block(i, carry):
            for u in range(step):
                carry = body(pl.ds(pl.multiple_of(i * (8 * step), 8 * step) + 8 * u, 8), carry)
            return carry
        return lax.fori_loop(0, ROWS // (8 * step), block, init)

    def partials(sums):
        sums = [jnp.broadcast_to(jnp.sum(v, axis=0, keepdims=True), (8, 128)) for v in sums]
        return jnp.where(sub8 == 0, sums[0], jnp.where(sub8 == 1, sums[1], jnp.where(sub8 == 2, sums[2], F32(0.0))))

    def advance(alpha, beta, last):
        def step(at_r, carry):
            e, rr, w, n = field[0, at_r, :], res[at_r, :], wap[at_r, :], nap[at_r, :]
            p = e * rr + beta * sch[at_r, :]
            s = w + beta * sim[at_r, :]
            t = n + beta * tim[at_r, :]
            sch[at_r, :] = p
            sim[at_r, :] = s
            tim[at_r, :] = t
            pre[at_r, :] = pre[at_r, :] + alpha * p
            rr = rr - alpha * s
            w = w - alpha * t
            res[at_r, :] = rr
            wap[at_r, :] = w
            field[last, at_r, :] = e * w
            return carry[0] + rr * (e * rr), carry[1] + w * (e * rr), carry[2] + rr * rr
        return partials(rows_loop(step, (zero8, zero8, zero8)))

    def stage(k, _):
        unpack(k)

        @pl.when(k == 0)
        def _():
            @pl.when(has_y_down)
            def _():
                copy5_out.wait_recv()
            refresh(ext)
            setup()

        @pl.when((k >= 1) & (k < 4))
        def _():
            scaled_force(k - 1)

        @pl.when(k >= 5)
        def _():
            reduce_middle(k - 5)

        @pl.when(k >= 4)
        def _():
            refresh(ext)
            gradient()

        @pl.when(k >= 3)
        def _():
            apply(nap)

        @pl.when(k == 3)
        def _():
            def step(at_r, _):
                r = nap[at_r, :]
                res[at_r, :] = r
                field[4, at_r, :] = field[0, at_r, :] * r
                return 0
            rows_loop(step, 0)

        @pl.when(k == 4)
        def _():
            def step(at_r, carry):
                e, rr, w = field[0, at_r, :], res[at_r, :], nap[at_r, :]
                z = e * rr
                wap[at_r, :] = w
                field[5, at_r, :] = e * w
                return carry[0] + rr * z, carry[1] + w * z, carry[2] + rr * rr
            red[0] = partials(rows_loop(step, (zero8, zero8, zero8)))

        @pl.when(k >= 5)
        def _():
            alpha, beta = reduce_end(k - 5)
            red[k - 4] = advance(alpha, beta, k + 1)

        @pl.when((k >= 3) & (k < 6))
        def _():
            exchange_start(k + 1)

        @pl.when(k >= 4)
        def _():
            reduce_start(k - 4)
        return 0
    lax.fori_loop(0, NSETS, stage, 0)

    reduce_middle(2)
    alpha, beta = reduce_end(2)

    def step2(at_r, _):
        rr = res[at_r, :]
        p = field[0, at_r, :] * rr + beta * sch[at_r, :]
        s = wap[at_r, :] + beta * sim[at_r, :]
        press_out[at_r, :] = pre[at_r, :] + alpha * p
        resid_out[at_r, :] = rr - alpha * s
        return 0
    rows_loop(step2, 0)
    norms_out[...] = jnp.where(lane8 == 0, norm[0], jnp.where(lane8 == 1, norm[1], norm[2]))

    def finish(k, _):
        finish_sends(k)
        return 0
    lax.fori_loop(0, NSETS, finish, 0)

    @pl.when(has_y_up)
    def _():
        copy5_out.wait_send()


def solution(mesh):
    sizes = (mesh.shape["gx"], mesh.shape["gy"], mesh.shape["gz"])
    nx, ny, nz = sizes

    def per_device(force, phase, table, flags):
        v = functools.partial(pltpu.VMEM)
        dma = pltpu.SemaphoreType.DMA
        scratch = [
            v((ROWS, 128), jnp.int32),
            v((NSETS + 1, ROWS, 128), F32),
            v((NSETS, 2, 128, 128), F32),
            v((NSETS, 64, 128), F32),
            v((NSETS, 32, 128), F32),
            v((32, 128), F32),
            v((NSETS, RECV_ROWS, 128), F32),
            v((56, 128), F32), v((16, 128), F32),
            v((EROWS, 128), F32),
            v((6, EROWS, 128), F32), v((3, EROWS, 128), F32), v((3, EROWS, 128), F32),
            v((3, EROWS, 128), F32), v((3, EROWS, 128), F32),
            v((120, 128), F32), v((240, 128), F32),
            *[v((ROWS, 128), F32) for _ in range(7)],
            v((ITERS, 8, 128), F32), v((ITERS, nz, 8, 128), F32), v((ITERS, nx * ny, 8, 128), F32),
            v((2, 8, 128), F32), v((ITERS, 8, 128), F32),
            dma((2,)), dma((NSETS, 26)), dma((NSETS, 26)), dma, dma,
            dma((ITERS, nz)), dma((ITERS, nz)), dma((ITERS, nx * ny)), dma((ITERS, nx * ny)),
        ]
        hbm = pl.BlockSpec(memory_space=pl.ANY)
        smem = pl.BlockSpec(memory_space=pltpu.SMEM)
        press, resid, norms = pl.pallas_call(
            functools.partial(kernel, sizes),
            out_shape=(
                pltpu.VMEM((ROWS, 128), F32),
                pltpu.VMEM((ROWS, 128), F32),
                jax.ShapeDtypeStruct((8, 128), F32),
            ),
            in_specs=[hbm, hbm, smem, smem],
            out_specs=(pl.BlockSpec(memory_space=pltpu.VMEM), pl.BlockSpec(memory_space=pltpu.VMEM), pl.BlockSpec(memory_space=pltpu.VMEM)),
            scratch_shapes=scratch,
            compiler_params=pltpu.CompilerParams(
                collective_id=0, has_side_effects=True, vmem_limit_bytes=60 * 1024 * 1024
            ),
        )(force.reshape(3, ROWS, BZ), phase.reshape(ROWS, BZ), table, flags)
        return press.reshape(BX, BY, BZ), resid.reshape(BX, BY, BZ), norms[0, :ITERS]

    return jax.shard_map(
        per_device,
        mesh=mesh,
        in_specs=(P(None, "gx", "gy", "gz"), P("gx", "gy", "gz"), P(), P()),
        out_specs=(P("gx", "gy", "gz"), P("gx", "gy", "gz"), P()),
        check_vma=False,
    )
```

```python
import functools

import jax
import jax.numpy as jnp
from jax import lax
from jax.experimental import pallas as pl
from jax.experimental.pallas import tpu as pltpu
from jax.sharding import PartitionSpec as P

ITERS = 3
OMEGA = 0.8
F32 = jnp.float32
MESH = pl.DeviceIdType.MESH

BX, BY, BZ = 32, 16, 128
ROWS = BX * BY
PLANES = 53
EROWS = PLANES * 24
NSETS = 7

DIRS = [(dx, dy, dz) for dz in (0, 1, -1) for dy in (1, -1, 0) for dx in (0, 1, -1) if (dx, dy, dz) != (0, 0, 0)]
DIRS.sort(key=lambda d: (d[1] == 0 or d[0] != 0 or d[2] != 0, sum(map(abs, d))))
DIR_AT = {d: i for i, d in enumerate(DIRS)}


def piece_rows(d):
    dx, dy, dz = d
    if dz == 0:
        if dx and dy:
            return 16
        return 128 if dy else 80
    if dx and dy:
        return 8
    if dy:
        return 16
    return 16 if dx else 64


OFFSETS = {}
RECV_ROWS = 0
for _d in DIRS:
    OFFSETS[_d] = RECV_ROWS
    RECV_ROWS += piece_rows(_d)


def iota(shape, dim):
    return lax.broadcasted_iota(jnp.int32, shape, dim)


def roll_lanes(v, by):
    by = by % 128
    return v if by == 0 else pltpu.roll(v, by, 1)


def roll_rows(v, by):
    return pltpu.roll(v, by % v.shape[0], 0)


def kernel(
    sizes,
    force_hbm, phase_hbm, table, flags,
    press_out, resid_out, norms_out,
    phase, field, ystage, cstage, dstage, y5, recv, r5, f5,
    ext, faces, weights, source, va, vb, halo, dslab,
    res, sch, wap, sim, tim, nap, pre,
    red, total1, red1, red2, scal, norm,
    in_sem, send_sem, recv_sem, send5_sem, recv5_sem, rs1, rr1, rs2, rr2,
):
    nx, ny, nz = sizes
    at = (lax.axis_index("gx"), lax.axis_index("gy"), lax.axis_index("gz"))

    def neighbour(d):
        ok = None
        for dim in range(3):
            if d[dim] == 0:
                continue
            here = at[dim] < sizes[dim] - 1 if d[dim] > 0 else at[dim] > 0
            ok = here if ok is None else jnp.logical_and(ok, here)
        return ok, tuple(at[dim] + d[dim] for dim in range(3))

    def recv_at(k, d, start=0, rows=None):
        return recv.at[k, pl.ds(OFFSETS[d] + start, piece_rows(d) if rows is None else rows)]

    def pieces(k, d):
        dx, dy, dz = d
        to = tuple(-a for a in d)
        if dz == 0:
            if dx and dy:
                side = 0 if dy < 0 else 1
                src = ystage.at[k, side, pl.ds(0 if dx < 0 else 112, 16)]
                return src, recv_at(k, to)
            if dy:
                return ystage.at[k, 0 if dy < 0 else 1], recv_at(k, to)
            if dx < 0:
                return field.at[k, pl.ds(0, 64)], recv_at(k, to, 0, 64)
            return field.at[k, pl.ds(ROWS - 80, 80)], recv_at(k, to)
        side = 0 if dy < 0 else 1
        if dx and dy:
            return dstage.at[k, side, pl.ds(0 if dx < 0 else 8, 8)], recv_at(k, to)
        if dy:
            return dstage.at[k, side], recv_at(k, to)
        if dx:
            return cstage.at[k, pl.ds(0 if dx < 0 else 48, 16)], recv_at(k, to)
        return cstage.at[k], recv_at(k, to)

    def copy_of(k, d):
        src, dst = pieces(k, d)
        _, device = neighbour(d)
        to = tuple(-a for a in d)
        return pltpu.make_async_remote_copy(
            src_ref=src, dst_ref=dst,
            send_sem=send_sem.at[k, DIR_AT[d]], recv_sem=recv_sem.at[k, DIR_AT[to]],
            device_id=device, device_id_type=MESH,
        )

    def incoming(k, d):
        to = tuple(-a for a in d)
        src, dst = pieces(k, to)
        return pltpu.make_async_remote_copy(
            src_ref=src, dst_ref=dst,
            send_sem=send_sem.at[k, DIR_AT[to]], recv_sem=recv_sem.at[k, DIR_AT[d]],
            device_id=at, device_id_type=MESH,
        )

    sub8 = iota((8, 128), 0)
    lane8 = iota((8, 128), 1)
    group8, slot8 = lane8 // 16, lane8 % 16
    lane24 = iota((24, 128), 1)
    sub24 = iota((24, 128), 0)
    group24, slot24 = lane24 // 32, lane24 % 32
    bigroup8, bislot8 = lane8 // 32, lane8 % 32


    def pack_y(k):
        def pair(xp, _):
            base = pl.multiple_of(xp * 32, 32)
            a0, a1 = field[k, pl.ds(base, 8), :], field[k, pl.ds(base + 8, 8), :]
            b0, b1 = field[k, pl.ds(base + 16, 8), :], field[k, pl.ds(base + 24, 8), :]
            to = pl.multiple_of(xp * 8, 8)
            ystage[k, 0, pl.ds(to, 8), :] = jnp.where(sub8 < 4, a0, roll_rows(b0, 4))
            ystage[k, 1, pl.ds(to, 8), :] = jnp.where(sub8 < 4, roll_rows(a1, 4), b1)
            return 0
        lax.fori_loop(0, BX // 2, pair, 0, unroll=16)

    def pack_z(k):
        def block(xp, _):
            ends = []
            for u in range(2):
                acc = [[None, None] for _ in range(3)]
                for g in range(8):
                    base = pl.multiple_of(xp * 256, 256) + (u * 128 + g * 16)
                    a, b = field[k, pl.ds(base, 8), :], field[k, pl.ds(base + 8, 8), :]
                    for i, v in enumerate((a, b, jnp.where(sub8 < 4, a, b))):
                        for m in range(2):
                            r = roll_lanes(v, 9 * m + 16 * g)
                            acc[i][m] = r if g == 0 else jnp.where(group8 == g, r, acc[i][m])
                a, b, c = (jnp.where(slot8 < 4, lo, hi) for lo, hi in acc)
                to = pl.multiple_of(xp * 32, 32) + u * 16
                cstage[k, pl.ds(to, 8), :] = a
                cstage[k, pl.ds(to + 8, 8), :] = b
                ends.append(c)
            to = pl.ds(pl.multiple_of(xp * 8, 8), 8)
            dstage[k, 0, to, :] = jnp.where(sub8 < 4, ends[0], roll_rows(ends[1], 4))
            dstage[k, 1, to, :] = jnp.where(sub8 < 4, roll_rows(ends[0], 4), ends[1])
            return 0
        lax.fori_loop(0, 2, block, 0, unroll=2)

    flat = [d for d in DIRS if d[2] == 0]
    deep = [d for d in DIRS if d[2] != 0]

    def send(k, dirs):
        for d in dirs:
            ok, _ = neighbour(d)

            @pl.when(ok)
            def _():
                copy_of(k, d).start()

    def exchange_start(k):
        pack_y(k)
        send(k, flat)
        pack_z(k)
        send(k, deep)

    def pack_first(k, _):
        @pl.when(k == 1)
        def _():
            load_force.wait()
        pack_y(k)
        pack_z(k)
        return 0

    def receive(k, dirs):
        for d in dirs:
            ok, _ = neighbour(d)

            @pl.when(ok)
            def _():
                incoming(k, d).wait_recv()

    def finish_sends(k):
        for d in DIRS:
            ok, _ = neighbour(d)

            @pl.when(ok)
            def _():
                copy_of(k, d).wait_send()

    def main_row(x):
        return (1 + x) * 24

    def slab_row(l):
        return (42 + l) * 24

    def refresh(ref):
        low, high = pl.ds(slab_row(9), 24), pl.ds(slab_row(0), 24)
        ref[pl.ds(slab_row(-1), 24), :] = roll_lanes(ref[low, :], 32)
        ref[pl.ds(slab_row(10), 24), :] = roll_lanes(ref[high, :], -32)

    def unpack(k):
        receive(k, flat)

        def planes(own, low, high, first, pairs):
            for xp in range(pairs):
                lo, hi = low(xp * 8), high(xp * 8)
                los, his = roll_rows(lo, 4), roll_rows(hi, 4)
                for half in range(2):
                    ra, rb = (roll_rows(own(xp * 32 + 16 * half + 8 * t), 4) for t in range(2))
                    to = main_row(first + 2 * xp + half)
                    ext[pl.ds(to, 8), :] = jnp.where(sub8 < 4, (lo, los)[half], ra)
                    ext[pl.ds(to + 8, 8), :] = jnp.where(sub8 < 4, ra, rb)
                    ext[pl.ds(to + 16, 8), :] = jnp.where(sub8 < 4, rb, (his, hi)[half])

        def of(d, start=0):
            return lambda row: recv[k, pl.ds(row + (OFFSETS[d] + start), 8), :]

        planes(lambda r: field[k, pl.ds(r, 8), :], of((0, -1, 0)), of((0, 1, 0)), 4, 16)
        planes(of((-1, 0, 0), 16), of((-1, -1, 0)), of((-1, 1, 0)), 0, 2)
        planes(of((1, 0, 0)), of((1, -1, 0)), of((1, 1, 0)), 36, 2)

        def own(i, _):
            for u in range(5):
                for t in range(3):
                    lo, hi = None, None
                    for h in range(4):
                        v = ext[pl.ds(pl.multiple_of(i * 120, 8) + (main_row(10 * h + u) + 8 * t), 8), :]
                        a, b = roll_lanes(v, 32 * h + 9), roll_lanes(v, 32 * h + 18)
                        lo = a if h == 0 else jnp.where(bigroup8 == h, a, lo)
                        hi = b if h == 0 else jnp.where(bigroup8 == h, b, hi)
                    to = pl.ds(pl.multiple_of(i * 120, 8) + (slab_row(u) + 8 * t), 8)
                    ext[to, :] = jnp.where(bislot8 < 9, lo, hi)
            return 0
        lax.fori_loop(0, 2, own, 0)
        receive(k, deep)

        def merged(d, row):
            low = recv[k, pl.ds(OFFSETS[(d[0], d[1], -1)] + row, 8), :]
            high = recv[k, pl.ds(OFFSETS[(d[0], d[1], 1)] + row, 8), :]
            return jnp.where(slot8 < 4, high, low)

        inner = []
        for t in range(2):
            inner.append([merged((-1, 0), 8 * t)] + [merged((0, 0), xb * 16 + 8 * t) for xb in range(4)] + [merged((1, 0), 8 * t)])
        sides = []
        for xb in range(6):
            dx, row = (-1, 0) if xb == 0 else (1, 0) if xb == 5 else (0, (xb - 1) // 2 * 8)
            above, below = merged((dx, 1), row), merged((dx, -1), row)
            if xb % 2 == 1:
                sides.append(jnp.where(sub8 < 4, below, roll_rows(above, 4)))
            else:
                sides.append(jnp.where(sub8 < 4, roll_rows(below, 4), above))

        def shifted(parts, i):
            return roll_lanes(jnp.where(group8 < 4, parts[i + 1], parts[i]), 64)

        def arrived(_, carry):
            for i in range(5):
                a, b = roll_rows(shifted(inner[0], i), 4), roll_rows(shifted(inner[1], i), 4)
                c = shifted(sides, i)
                tiles = (jnp.where(sub8 < 4, c, a), jnp.where(sub8 < 4, a, b), jnp.where(sub8 < 4, b, c))
                for t in range(3):
                    halo[pl.ds(i * 24 + 8 * t, 8), :] = tiles[t]
            return carry
        lax.fori_loop(0, 1, arrived, 0)

        def outer(l, _):
            for t in range(3):
                acc = None
                for h in range(4):
                    x = 10 * h + l
                    v = halo[pl.ds(x // 8 * 24 + 8 * t, 8), :]
                    a = roll_lanes(v, 32 * h + 9 - 16 * (x % 8))
                    acc = a if h == 0 else jnp.where(bigroup8 == h, a, acc)
                to = pl.ds(slab_row(l) + 8 * t, 8)
                ext[to, :] = jnp.where((bislot8 >= 9) & (bislot8 < 18), acc, ext[to, :])
            return 0
        for l in range(10):
            outer(l, 0)


    walls = [jnp.where(flags[f] == 0, F32(1.0), F32(0.0)) for f in range(6)]
    totals = (nx * BX, ny * BY, nz * BZ)

    def coefficients(b, e, nbrs, spots):
        inside = None
        diag = jnp.zeros_like(e)
        extra = [jnp.zeros_like(e) for _ in range(3)]
        for axis in range(3):
            for side in range(2):
                spot = spots[axis] + (1 if side else -1)
                here = (spot >= 0) & (spot < totals[axis])
                face = 0.5 * (e + nbrs[axis][side])
                wall = walls[2 * axis + side]
                outer = jnp.where(here, F32(0.0), e)
                diag = diag + jnp.where(here, face, e * wall)
                extra[axis] = extra[axis] + outer * (1.0 - wall)
                faces[2 * axis + side, pl.ds(b, 24), :] = face
            here = (spots[axis] >= 0) & (spots[axis] < totals[axis])
            inside = here if inside is None else inside & here
        for c in range(3):
            d = diag + extra[c]
            good = inside & (d > 0)
            weights[c, pl.ds(b, 24), :] = jnp.where(good, OMEGA / jnp.where(good, d, F32(1.0)), F32(0.0))

    def setup():
        keep = None
        for t in range(2):
            v = roll_rows(recv[0, pl.ds(OFFSETS[(-1, 0, 0)] + 8 * t, 8), :], 4)
            if t == 0:
                ext[pl.ds(0, 8), :] = jnp.where(sub8 < 4, F32(0.0), v)
                keep = v
            else:
                ext[pl.ds(8, 8), :] = jnp.where(sub8 < 4, keep, v)
                ext[pl.ds(16, 8), :] = jnp.where(sub8 < 4, v, F32(0.0))
        first = ext[pl.ds(0, 24), :]
        first = jnp.where(slot24 < 9, roll_lanes(first, 9), roll_lanes(first, 18))
        low = pl.ds(slab_row(-1), 24)
        ext[low, :] = jnp.where(group24 == 0, first, ext[low, :])
        five = None
        lane16 = iota((16, 128), 1)
        for h in range(4):
            v = r5[pl.ds(10 * h + 4, 16), :]
            v = jnp.where(lane16 % 32 < 9, roll_lanes(v, 32 * h + 9), roll_lanes(v, 32 * h + 18))
            five = v if h == 0 else jnp.where(lane16 // 32 == h, v, five)
        f5[...] = five

        def neighbours(b, below):
            e = ext[pl.ds(b, 24), :]
            return e, (
                (ext[pl.ds(b - 24, 24), :], ext[pl.ds(b + 24, 24), :]),
                (jnp.where(sub24 == 0, below, ext[pl.ds(b - 1, 24), :]), ext[pl.ds(b + 1, 24), :]),
                (roll_lanes(e, 1), roll_lanes(e, 127)),
            )

        ys = sub24 + (at[1] * BY - 4)

        def main_block(i, _):
            fives = roll_rows(jnp.where(sub8 < 4, r5[pl.ds(pl.multiple_of(i * 8, 8) + 8, 8), :], r5[pl.ds(pl.multiple_of(i * 8, 8), 8), :]), 4)
            for j in range(8):
                b = pl.multiple_of(i * 192, 8) + main_row(j)
                e, nbrs = neighbours(b, jnp.broadcast_to(fives[j:j + 1, :], (24, 128)))
                coefficients(b, e, nbrs, (
                    jnp.broadcast_to(at[0] * BX + (i * 8 + j - 4), (24, 128)), ys, lane24 + at[2] * BZ,
                ))
            return 0
        lax.fori_loop(0, 5, main_block, 0)
        zs = jnp.where(slot24 < 13, slot24 + 119, slot24 - 18) + at[2] * BZ

        for l in range(10):
            b = slab_row(l)
            e, nbrs = neighbours(b, jnp.broadcast_to(f5[l:l + 1, :], (24, 128)))
            coefficients(b, e, nbrs, (group24 * 10 + (at[0] * BX - 4 + l), ys, zs))


    SLAB = [slab_row(l) for l in range(10)]

    def gradient():
        for b in SLAB + [main_row(x) for x in range(39)]:
            p = ext[pl.ds(b, 24), :]
            nbrs = (ext[pl.ds(b + 24, 24), :], ext[pl.ds(b + 1, 24), :], roll_lanes(p, 127))
            for c in range(3):
                source[c, pl.ds(b, 24), :] = weights[c, pl.ds(b, 24), :] * (nbrs[c] - p)

    def scaled_force(c):
        def block(i, _):
            for u in range(13):
                b = pl.multiple_of(i * 312, 8) + 24 * (u + 1)
                source[c, pl.ds(b, 24), :] = weights[c, pl.ds(b, 24), :] * ext[pl.ds(b, 24), :]
            return 0
        lax.fori_loop(0, 4, block, 0)

    def ends(ref):
        def each(c, _):
            refresh(ref.at[c])
            return 0
        lax.fori_loop(0, 3, each, 0, unroll=3)

    def sweep(src, dst, first, last):
        for b in SLAB + [main_row(x) for x in range(first, last + 1)]:
            k = [faces[f, pl.ds(b, 24), :] for f in range(6)]
            for c in range(3):
                v = src[c, pl.ds(b, 24), :]
                total = k[0] * src[c, pl.ds(b - 24, 24), :] + k[1] * src[c, pl.ds(b + 24, 24), :]
                total = total + (k[2] * src[c, pl.ds(b - 1, 24), :] + k[3] * src[c, pl.ds(b + 1, 24), :])
                total = total + (k[4] * roll_lanes(v, 1) + k[5] * roll_lanes(v, 127))
                dst[c, pl.ds(b, 24), :] = (
                    (1.0 - OMEGA) * v + source[c, pl.ds(b, 24), :] + weights[c, pl.ds(b, 24), :] * total
                )
        ends(dst)

    def minus_divergence(src, b, rows):
        x, y, z = (src[c, pl.ds(b, rows), :] for c in range(3))
        return (src[0, pl.ds(b - 24, rows), :] - x) + (src[1, pl.ds(b - 1, rows), :] - y) + (roll_lanes(z, 1) - z)

    def divergence(src, out):
        def slab_part(i, _):
            for u in range(5):
                b = pl.multiple_of(i * 120, 8) + slab_row(u)
                dslab[pl.ds(pl.multiple_of(i * 120, 8) + u * 24, 24), :] = minus_divergence(src, b, 24)
            return 0
        lax.fori_loop(0, 2, slab_part, 0)

        def together(i, _):
            for u in range(5):
                b = pl.ds(pl.multiple_of(i * 120, 8) + u * 24, 24)
                v = dslab[b, :]
                dslab[b, :] = jnp.where(slot24 < 9, v, roll_lanes(v, -9))
            return 0
        lax.fori_loop(0, 2, together, 0)
        lane16 = iota((16, 128), 1)
        for x in range(4, 36):
            h, l = divmod(x, 10)
            total = minus_divergence(src, main_row(x) + 4, 16)
            edge = roll_lanes(dslab[pl.ds(l * 24 + 4, 16), :], -(9 + 32 * h))
            out[pl.ds((x - 4) * 16, 16), :] = jnp.where((lane16 < 8) | (lane16 >= 124), edge, total)

    def apply(out):
        ends(source)
        sweep(source, va, 1, 37)
        sweep(va, vb, 2, 36)
        sweep(vb, va, 3, 35)
        divergence(va, out)


    me_z = at[2]
    me_xy = at[0] * ny + at[1]
    nxy = nx * ny

    def z_copy(k, off):
        return pltpu.make_async_remote_copy(
            src_ref=red.at[k], dst_ref=red1.at[k, me_z], send_sem=rs1.at[k], recv_sem=rr1.at[k],
            device_id=(at[0], at[1], lax.rem(me_z + off, nz)), device_id_type=MESH,
        )

    def xy_copy(k, ox, oy):
        return pltpu.make_async_remote_copy(
            src_ref=total1.at[k], dst_ref=red2.at[k, me_xy], send_sem=rs2.at[k], recv_sem=rr2.at[k],
            device_id=(lax.rem(at[0] + ox, nx), lax.rem(at[1] + oy, ny), at[2]), device_id_type=MESH,
        )

    def all_of(k, ref, count, sent, arrived):
        part = ref.at[k, pl.ds(0, count)]
        return pltpu.make_async_remote_copy(
            src_ref=part, dst_ref=part, send_sem=sent.at[k], recv_sem=arrived.at[k],
            device_id=at, device_id_type=MESH,
        )

    offsets_xy = [(ox, oy) for ox in range(nx) for oy in range(ny) if (ox, oy) != (0, 0)]

    def reduce_start(k):
        red1[k, me_z] = red[k]
        for off in range(1, nz):
            z_copy(k, off).start()

    def reduce_middle(k):
        all_of(k, red1, nz - 1, rs1, rr1).wait_recv()
        value = red1[k, 0]
        for i in range(1, nz):
            value = value + red1[k, i]
        total1[k] = value
        red2[k, me_xy] = value
        for ox, oy in offsets_xy:
            xy_copy(k, ox, oy).start()

    cells = float(totals[0] * totals[1] * totals[2])

    def reduce_end(k):
        all_of(k, red2, nxy - 1, rs2, rr2).wait_recv()
        value = red2[k, 0]
        for i in range(1, nxy):
            value = value + red2[k, i]
        gamma, delta, squares = (
            jnp.broadcast_to(jnp.sum(value[i], axis=1, keepdims=True), (8, 128)) for i in range(3)
        )
        norm[k] = squares / cells
        gamma_old, alpha_old = scal[0], scal[1]
        if isinstance(k, int):
            beta = gamma / gamma_old
            alpha = gamma / (delta - beta * gamma / alpha_old)
        else:
            beta = jnp.where(k == 0, F32(0.0), gamma / gamma_old)
            alpha = gamma / (delta - jnp.where(k == 0, F32(0.0), beta * gamma / alpha_old))
        scal[0] = gamma
        scal[1] = alpha
        return alpha, beta


    load_phase = pltpu.make_async_copy(phase_hbm, phase, in_sem.at[0])
    load_force = pltpu.make_async_copy(force_hbm, field.at[pl.ds(1, 3)], in_sem.at[1])
    load_phase.start()
    load_force.start()

    def clear_recv(i, _):
        for k in range(NSETS):
            recv[k, pl.ds(pl.multiple_of(i * 8, 8), 8), :] = jnp.zeros((8, 128), F32)
        return 0
    lax.fori_loop(0, RECV_ROWS // 8, clear_recv, 0, unroll=2)

    for t in range(0, 56, 8):
        r5[pl.ds(t, 8), :] = jnp.zeros((8, 128), F32)

    barrier = pltpu.get_barrier_semaphore()
    count = jnp.int32(0)
    for d in DIRS:
        ok, device = neighbour(d)

        @pl.when(ok)
        def _():
            pl.semaphore_signal(barrier, inc=1, device_id=device, device_id_type=MESH)
        count = count + ok.astype(jnp.int32)
    for off in range(1, nz):
        pl.semaphore_signal(barrier, inc=1, device_id=(at[0], at[1], lax.rem(me_z + off, nz)), device_id_type=MESH)
    for ox, oy in offsets_xy:
        pl.semaphore_signal(
            barrier, inc=1, device_id=(lax.rem(at[0] + ox, nx), lax.rem(at[1] + oy, ny), at[2]), device_id_type=MESH
        )
    count = count + (nz - 1 + nxy - 1)

    zero24 = jnp.zeros((24, 128), F32)
    ext[pl.ds(0, 24), :] = zero24
    for ref in (source, va, vb):
        for c in range(3):
            for plane in (0, 1, 2, 3, 38, 39, 40, 41, 52):
                ref[c, pl.ds(plane * 24, 24), :] = zero24
    for f in range(6):
        faces[f, pl.ds(41 * 24, 24), :] = zero24
    for c in range(3):
        weights[c, pl.ds(41 * 24, 24), :] = zero24
        weights[c, pl.ds(52 * 24, 24), :] = zero24
    zero8 = jnp.zeros((8, 128), F32)
    scal[0] = zero8 + 1.0
    scal[1] = zero8 + 1.0
    for ref in (sch, sim, tim, pre):
        def clear(i, _):
            ref[pl.ds(pl.multiple_of(i * 64, 64), 64), :] = jnp.zeros((64, 128), F32)
            return 0
        lax.fori_loop(0, ROWS // 64, clear, 0)

    load_phase.wait()

    def lookup(i, _):
        for u in range(4):
            r = pl.multiple_of(i * 32, 32) + 8 * u
            ids = phase[pl.ds(r, 8), :]
            eta = jnp.zeros((8, 128), F32)
            for level in range(8):
                eta = eta + jnp.where(ids == level, table[level], F32(0.0))
            field[0, pl.ds(r, 8), :] = eta
        return 0
    lax.fori_loop(0, ROWS // 32, lookup, 0)
    for x in range(BX):
        y5[pl.ds(x, 1), :] = field[0, pl.ds(x * 16 + 11, 1), :]
    lax.fori_loop(0, 4, pack_first, 0)
    pl.semaphore_wait(barrier, count)
    has_y_up, _ = neighbour((0, 1, 0))
    has_y_down, _ = neighbour((0, -1, 0))
    copy5_out = pltpu.make_async_remote_copy(
        src_ref=y5, dst_ref=r5.at[pl.ds(8, 32)], send_sem=send5_sem, recv_sem=recv5_sem,
        device_id=(at[0], at[1] + 1, at[2]), device_id_type=MESH,
    )

    @pl.when(has_y_up)
    def _():
        copy5_out.start()

    def send_first(k, _):
        send(k, flat)
        send(k, deep)
        return 0
    lax.fori_loop(0, 4, send_first, 0)

    def rows_loop(body, init, step=8):
        def block(i, carry):
            for u in range(step):
                carry = body(pl.ds(pl.multiple_of(i * (8 * step), 8 * step) + 8 * u, 8), carry)
            return carry
        return lax.fori_loop(0, ROWS // (8 * step), block, init)

    def keep_partials(k, sums):
        for i in range(3):
            red[k, i] = jnp.sum(sums[i], axis=0, keepdims=True)

    def advance(alpha, beta, last):
        def step(at_r, carry):
            e, rr, w, n = field[0, at_r, :], res[at_r, :], wap[at_r, :], nap[at_r, :]
            p = e * rr + beta * sch[at_r, :]
            s = w + beta * sim[at_r, :]
            t = n + beta * tim[at_r, :]
            sch[at_r, :] = p
            sim[at_r, :] = s
            tim[at_r, :] = t
            pre[at_r, :] = pre[at_r, :] + alpha * p
            rr = rr - alpha * s
            w = w - alpha * t
            res[at_r, :] = rr
            wap[at_r, :] = w
            field[last, at_r, :] = e * w
            return carry[0] + rr * (e * rr), carry[1] + w * (e * rr), carry[2] + rr * rr
        return rows_loop(step, (zero8, zero8, zero8))

    def stage(k, _):
        unpack(k)

        @pl.when(k == 0)
        def _():
            @pl.when(has_y_down)
            def _():
                copy5_out.wait_recv()
            refresh(ext)
            setup()

        @pl.when((k >= 1) & (k < 4))
        def _():
            scaled_force(k - 1)

        @pl.when(k >= 5)
        def _():
            reduce_middle(k - 5)

        @pl.when(k >= 4)
        def _():
            refresh(ext)
            gradient()

        @pl.when(k >= 3)
        def _():
            apply(nap)

        @pl.when(k == 3)
        def _():
            def step(at_r, _):
                r = nap[at_r, :]
                res[at_r, :] = r
                field[4, at_r, :] = field[0, at_r, :] * r
                return 0
            rows_loop(step, 0)

        @pl.when(k == 4)
        def _():
            def step(at_r, carry):
                e, rr, w = field[0, at_r, :], res[at_r, :], nap[at_r, :]
                z = e * rr
                wap[at_r, :] = w
                field[5, at_r, :] = e * w
                return carry[0] + rr * z, carry[1] + w * z, carry[2] + rr * rr
            keep_partials(0, rows_loop(step, (zero8, zero8, zero8)))

        @pl.when(k >= 5)
        def _():
            alpha, beta = reduce_end(k - 5)
            keep_partials(k - 4, advance(alpha, beta, k + 1))

        @pl.when((k >= 3) & (k < 6))
        def _():
            exchange_start(k + 1)

        @pl.when(k >= 4)
        def _():
            reduce_start(k - 4)
        return 0
    lax.fori_loop(0, NSETS, stage, 0)

    reduce_middle(2)
    alpha, beta = reduce_end(2)

    def step2(at_r, _):
        rr = res[at_r, :]
        p = field[0, at_r, :] * rr + beta * sch[at_r, :]
        s = wap[at_r, :] + beta * sim[at_r, :]
        press_out[at_r, :] = pre[at_r, :] + alpha * p
        resid_out[at_r, :] = rr - alpha * s
        return 0
    rows_loop(step2, 0)
    norms_out[...] = jnp.where(lane8 == 0, norm[0], jnp.where(lane8 == 1, norm[1], norm[2]))

    def finish(k, _):
        finish_sends(k)

        @pl.when(k < ITERS)
        def _():
            all_of(k, red1, nz - 1, rs1, rr1).wait_send()
            all_of(k, red2, nxy - 1, rs2, rr2).wait_send()
        return 0
    lax.fori_loop(0, NSETS, finish, 0)

    @pl.when(has_y_up)
    def _():
        copy5_out.wait_send()


def solution(mesh):
    sizes = (mesh.shape["gx"], mesh.shape["gy"], mesh.shape["gz"])
    nx, ny, nz = sizes

    def per_device(force, phase, table, flags):
        v = functools.partial(pltpu.VMEM)
        dma = pltpu.SemaphoreType.DMA
        scratch = [
            v((ROWS, 128), jnp.int32),
            v((NSETS + 1, ROWS, 128), F32),
            v((NSETS, 2, 128, 128), F32),
            v((NSETS, 64, 128), F32),
            v((NSETS, 2, 16, 128), F32),
            v((32, 128), F32),
            v((NSETS, RECV_ROWS, 128), F32),
            v((56, 128), F32), v((16, 128), F32),
            v((EROWS, 128), F32),
            v((6, EROWS, 128), F32), v((3, EROWS, 128), F32), v((3, EROWS, 128), F32),
            v((3, EROWS, 128), F32), v((3, EROWS, 128), F32),
            v((120, 128), F32), v((240, 128), F32),
            *[v((ROWS, 128), F32) for _ in range(7)],
            v((ITERS, 3, 1, 128), F32), v((ITERS, 3, 1, 128), F32),
            v((ITERS, nz, 3, 1, 128), F32), v((ITERS, nx * ny, 3, 1, 128), F32),
            v((2, 8, 128), F32), v((ITERS, 8, 128), F32),
            dma((2,)), dma((NSETS, 26)), dma((NSETS, 26)), dma, dma,
            dma((ITERS,)), dma((ITERS,)), dma((ITERS,)), dma((ITERS,)),
        ]
        hbm = pl.BlockSpec(memory_space=pl.ANY)
        smem = pl.BlockSpec(memory_space=pltpu.SMEM)
        press, resid, norms = pl.pallas_call(
            functools.partial(kernel, sizes),
            out_shape=(
                pltpu.VMEM((ROWS, 128), F32),
                pltpu.VMEM((ROWS, 128), F32),
                jax.ShapeDtypeStruct((8, 128), F32),
            ),
            in_specs=[hbm, hbm, smem, smem],
            out_specs=(pl.BlockSpec(memory_space=pltpu.VMEM), pl.BlockSpec(memory_space=pltpu.VMEM), pl.BlockSpec(memory_space=pltpu.VMEM)),
            scratch_shapes=scratch,
            compiler_params=pltpu.CompilerParams(
                collective_id=0, has_side_effects=True, vmem_limit_bytes=60 * 1024 * 1024
            ),
        )(force.reshape(3, ROWS, BZ), phase.reshape(ROWS, BZ), table, flags)
        return press.reshape(BX, BY, BZ), resid.reshape(BX, BY, BZ), norms[0, :ITERS]

    return jax.shard_map(
        per_device,
        mesh=mesh,
        in_specs=(P(None, "gx", "gy", "gz"), P("gx", "gy", "gz"), P(), P()),
        out_specs=(P("gx", "gy", "gz"), P("gx", "gy", "gz"), P()),
        check_vma=False,
    )
```

```python
import functools

import jax
import jax.numpy as jnp
from jax import lax
from jax.experimental import pallas as pl
from jax.experimental.pallas import tpu as pltpu
from jax.sharding import PartitionSpec as P

ITERS = 3
OMEGA = 0.8
F32 = jnp.float32
MESH = pl.DeviceIdType.MESH

BX, BY, BZ = 32, 16, 128
ROWS = BX * BY
PLANES = 53
EROWS = PLANES * 24
NSETS = 7

DIRS = [(dx, dy, dz) for dz in (0, 1, -1) for dy in (1, -1, 0) for dx in (0, 1, -1) if (dx, dy, dz) != (0, 0, 0)]
DIRS.sort(key=lambda d: (d[1] == 0 or d[0] != 0 or d[2] != 0, sum(map(abs, d))))
DIR_AT = {d: i for i, d in enumerate(DIRS)}


def piece_rows(d):
    dx, dy, dz = d
    if dz == 0:
        if dx and dy:
            return 16
        return 128 if dy else 80
    if dx and dy:
        return 8
    if dy:
        return 16
    return 16 if dx else 64


OFFSETS = {}
RECV_ROWS = 0
for _d in DIRS:
    OFFSETS[_d] = RECV_ROWS
    RECV_ROWS += piece_rows(_d)


def iota(shape, dim):
    return lax.broadcasted_iota(jnp.int32, shape, dim)


def roll_lanes(v, by):
    by = by % 128
    return v if by == 0 else pltpu.roll(v, by, 1)


def roll_rows(v, by):
    return pltpu.roll(v, by % v.shape[0], 0)


def kernel(
    sizes,
    force_hbm, phase_hbm, table, flags,
    press_out, resid_out, norms_out,
    phase, field, ystage, cstage, dstage, y5, recv, r5, f5,
    ext, faces, weights, source, va, vb, halo, dslab,
    res, sch, wap, sim, tim, nap, pre,
    red, total1, red1, red2, scal, norm,
    in_sem, send_sem, recv_sem, send5_sem, recv5_sem, rs1, rr1, rs2, rr2,
):
    nx, ny, nz = sizes
    at = (lax.axis_index("gx"), lax.axis_index("gy"), lax.axis_index("gz"))

    def neighbour(d):
        ok = None
        for dim in range(3):
            if d[dim] == 0:
                continue
            here = at[dim] < sizes[dim] - 1 if d[dim] > 0 else at[dim] > 0
            ok = here if ok is None else jnp.logical_and(ok, here)
        return ok, tuple(at[dim] + d[dim] for dim in range(3))

    def recv_at(k, d, start=0, rows=None):
        return recv.at[k, pl.ds(OFFSETS[d] + start, piece_rows(d) if rows is None else rows)]

    def pieces(k, d):
        dx, dy, dz = d
        to = tuple(-a for a in d)
        if dz == 0:
            if dx and dy:
                side = 0 if dy < 0 else 1
                src = ystage.at[k, side, pl.ds(0 if dx < 0 else 112, 16)]
                return src, recv_at(k, to)
            if dy:
                return ystage.at[k, 0 if dy < 0 else 1], recv_at(k, to)
            if dx < 0:
                return field.at[k, pl.ds(0, 64)], recv_at(k, to, 0, 64)
            return field.at[k, pl.ds(ROWS - 80, 80)], recv_at(k, to)
        side = 0 if dy < 0 else 1
        if dx and dy:
            return dstage.at[k, side, pl.ds(0 if dx < 0 else 8, 8)], recv_at(k, to)
        if dy:
            return dstage.at[k, side], recv_at(k, to)
        if dx:
            return cstage.at[k, pl.ds(0 if dx < 0 else 48, 16)], recv_at(k, to)
        return cstage.at[k], recv_at(k, to)

    def copy_of(k, d):
        src, dst = pieces(k, d)
        _, device = neighbour(d)
        to = tuple(-a for a in d)
        return pltpu.make_async_remote_copy(
            src_ref=src, dst_ref=dst,
            send_sem=send_sem.at[DIR_AT[d]], recv_sem=recv_sem.at[lax.rem(k, 5), DIR_AT[to]],
            device_id=device, device_id_type=MESH,
        )

    def incoming(k, d):
        to = tuple(-a for a in d)
        src, dst = pieces(k, to)
        return pltpu.make_async_remote_copy(
            src_ref=src, dst_ref=dst,
            send_sem=send_sem.at[DIR_AT[to]], recv_sem=recv_sem.at[lax.rem(k, 5), DIR_AT[d]],
            device_id=at, device_id_type=MESH,
        )

    sub8 = iota((8, 128), 0)
    lane8 = iota((8, 128), 1)
    group8, slot8 = lane8 // 16, lane8 % 16
    lane24 = iota((24, 128), 1)
    sub24 = iota((24, 128), 0)
    group24, slot24 = lane24 // 32, lane24 % 32
    bigroup8, bislot8 = lane8 // 32, lane8 % 32


    def pack_y(k):
        def pair(xp, _):
            base = pl.multiple_of(xp * 32, 32)
            a0, a1 = field[k, pl.ds(base, 8), :], field[k, pl.ds(base + 8, 8), :]
            b0, b1 = field[k, pl.ds(base + 16, 8), :], field[k, pl.ds(base + 24, 8), :]
            to = pl.multiple_of(xp * 8, 8)
            ystage[k, 0, pl.ds(to, 8), :] = jnp.where(sub8 < 4, a0, roll_rows(b0, 4))
            ystage[k, 1, pl.ds(to, 8), :] = jnp.where(sub8 < 4, roll_rows(a1, 4), b1)
            return 0
        lax.fori_loop(0, BX // 2, pair, 0, unroll=16)

    def pack_z(k):
        def block(xp, _):
            ends = []
            for u in range(2):
                acc = [[None, None] for _ in range(3)]
                for g in range(8):
                    base = pl.multiple_of(xp * 256, 256) + (u * 128 + g * 16)
                    a, b = field[k, pl.ds(base, 8), :], field[k, pl.ds(base + 8, 8), :]
                    for i, v in enumerate((a, b, jnp.where(sub8 < 4, a, b))):
                        for m in range(2):
                            r = roll_lanes(v, 9 * m + 16 * g)
                            acc[i][m] = r if g == 0 else jnp.where(group8 == g, r, acc[i][m])
                a, b, c = (jnp.where(slot8 < 4, lo, hi) for lo, hi in acc)
                to = pl.multiple_of(xp * 32, 32) + u * 16
                cstage[k, pl.ds(to, 8), :] = a
                cstage[k, pl.ds(to + 8, 8), :] = b
                ends.append(c)
            to = pl.ds(pl.multiple_of(xp * 8, 8), 8)
            dstage[k, 0, to, :] = jnp.where(sub8 < 4, ends[0], roll_rows(ends[1], 4))
            dstage[k, 1, to, :] = jnp.where(sub8 < 4, roll_rows(ends[0], 4), ends[1])
            return 0
        lax.fori_loop(0, 2, block, 0, unroll=2)

    flat = [d for d in DIRS if d[2] == 0]
    deep = [d for d in DIRS if d[2] != 0]

    def send(k, dirs):
        for d in dirs:
            ok, _ = neighbour(d)

            @pl.when(ok)
            def _():
                copy_of(k, d).start()

    def exchange_start(k):
        pack_y(k)
        send(k, flat)
        pack_z(k)
        send(k, deep)

    def pack_first(k, _):
        @pl.when(k == 1)
        def _():
            load_force.wait()
        pack_y(k)
        pack_z(k)
        return 0

    def receive(k, dirs):
        for d in dirs:
            ok, _ = neighbour(d)

            @pl.when(ok)
            def _():
                incoming(k, d).wait_recv()

    def finish_sends():
        for d in DIRS:
            ok, device = neighbour(d)
            rows = 64 if d == (-1, 0, 0) else piece_rows(d)

            @pl.when(ok)
            def _():
                part = recv.at[pl.ds(0, NSETS), pl.ds(0, rows)]
                pltpu.make_async_remote_copy(
                    src_ref=part, dst_ref=part, send_sem=send_sem.at[DIR_AT[d]], recv_sem=recv_sem.at[0, DIR_AT[d]],
                    device_id=device, device_id_type=MESH,
                ).wait_send()

    def main_row(x):
        return (1 + x) * 24

    def slab_row(l):
        return (42 + l) * 24

    def refresh(ref):
        low, high = pl.ds(slab_row(9), 24), pl.ds(slab_row(0), 24)
        ref[pl.ds(slab_row(-1), 24), :] = roll_lanes(ref[low, :], 32)
        ref[pl.ds(slab_row(10), 24), :] = roll_lanes(ref[high, :], -32)

    def unpack_flat(k):
        receive(k, flat)

        def planes(own, low, high, first, pairs):
            for xp in range(pairs):
                lo, hi = low(xp * 8), high(xp * 8)
                los, his = roll_rows(lo, 4), roll_rows(hi, 4)
                for half in range(2):
                    ra, rb = (roll_rows(own(xp * 32 + 16 * half + 8 * t), 4) for t in range(2))
                    to = main_row(first + 2 * xp + half)
                    ext[pl.ds(to, 8), :] = jnp.where(sub8 < 4, (lo, los)[half], ra)
                    ext[pl.ds(to + 8, 8), :] = jnp.where(sub8 < 4, ra, rb)
                    ext[pl.ds(to + 16, 8), :] = jnp.where(sub8 < 4, rb, (his, hi)[half])

        def of(d, start=0):
            return lambda row: recv[k, pl.ds(row + (OFFSETS[d] + start), 8), :]

        planes(lambda r: field[k, pl.ds(r, 8), :], of((0, -1, 0)), of((0, 1, 0)), 4, 16)
        planes(of((-1, 0, 0), 16), of((-1, -1, 0)), of((-1, 1, 0)), 0, 2)
        planes(of((1, 0, 0)), of((1, -1, 0)), of((1, 1, 0)), 36, 2)

        def own(i, _):
            for u in range(5):
                for t in range(3):
                    lo, hi = None, None
                    for h in range(4):
                        v = ext[pl.ds(pl.multiple_of(i * 120, 8) + (main_row(10 * h + u) + 8 * t), 8), :]
                        a, b = roll_lanes(v, 32 * h + 9), roll_lanes(v, 32 * h + 18)
                        lo = a if h == 0 else jnp.where(bigroup8 == h, a, lo)
                        hi = b if h == 0 else jnp.where(bigroup8 == h, b, hi)
                    to = pl.ds(pl.multiple_of(i * 120, 8) + (slab_row(u) + 8 * t), 8)
                    ext[to, :] = jnp.where(bislot8 < 9, lo, hi)
            return 0
        lax.fori_loop(0, 2, own, 0)

    def unpack_deep(k):
        receive(k, deep)

        def merged(d, row):
            low = recv[k, pl.ds(OFFSETS[(d[0], d[1], -1)] + row, 8), :]
            high = recv[k, pl.ds(OFFSETS[(d[0], d[1], 1)] + row, 8), :]
            return jnp.where(slot8 < 4, high, low)

        inner = []
        for t in range(2):
            inner.append([merged((-1, 0), 8 * t)] + [merged((0, 0), xb * 16 + 8 * t) for xb in range(4)] + [merged((1, 0), 8 * t)])
        sides = []
        for xb in range(6):
            dx, row = (-1, 0) if xb == 0 else (1, 0) if xb == 5 else (0, (xb - 1) // 2 * 8)
            above, below = merged((dx, 1), row), merged((dx, -1), row)
            if xb % 2 == 1:
                sides.append(jnp.where(sub8 < 4, below, roll_rows(above, 4)))
            else:
                sides.append(jnp.where(sub8 < 4, roll_rows(below, 4), above))

        def shifted(parts, i):
            return roll_lanes(jnp.where(group8 < 4, parts[i + 1], parts[i]), 64)

        def arrived(_, carry):
            for i in range(5):
                a, b = roll_rows(shifted(inner[0], i), 4), roll_rows(shifted(inner[1], i), 4)
                c = shifted(sides, i)
                tiles = (jnp.where(sub8 < 4, c, a), jnp.where(sub8 < 4, a, b), jnp.where(sub8 < 4, b, c))
                for t in range(3):
                    halo[pl.ds(i * 24 + 8 * t, 8), :] = tiles[t]
            return carry
        lax.fori_loop(0, 1, arrived, 0)

        def outer(l, _):
            for t in range(3):
                acc = None
                for h in range(4):
                    x = 10 * h + l
                    v = halo[pl.ds(x // 8 * 24 + 8 * t, 8), :]
                    a = roll_lanes(v, 32 * h + 9 - 16 * (x % 8))
                    acc = a if h == 0 else jnp.where(bigroup8 == h, a, acc)
                to = pl.ds(slab_row(l) + 8 * t, 8)
                ext[to, :] = jnp.where((bislot8 >= 9) & (bislot8 < 18), acc, ext[to, :])
            return 0
        for l in range(10):
            outer(l, 0)


    walls = [jnp.where(flags[f] == 0, F32(1.0), F32(0.0)) for f in range(6)]
    totals = (nx * BX, ny * BY, nz * BZ)

    def coefficients(b, e, nbrs, spots):
        inside = None
        diag = jnp.zeros_like(e)
        extra = [jnp.zeros_like(e) for _ in range(3)]
        for axis in range(3):
            for side in range(2):
                spot = spots[axis] + (1 if side else -1)
                here = (spot >= 0) & (spot < totals[axis])
                face = 0.5 * (e + nbrs[axis][side])
                wall = walls[2 * axis + side]
                outer = jnp.where(here, F32(0.0), e)
                diag = diag + jnp.where(here, face, e * wall)
                extra[axis] = extra[axis] + outer * (1.0 - wall)
                faces[2 * axis + side, pl.ds(b, 24), :] = face
            here = (spots[axis] >= 0) & (spots[axis] < totals[axis])
            inside = here if inside is None else inside & here
        for c in range(3):
            d = diag + extra[c]
            good = inside & (d > 0)
            weights[c, pl.ds(b, 24), :] = jnp.where(good, OMEGA / jnp.where(good, d, F32(1.0)), F32(0.0))

    def setup():
        keep = None
        for t in range(2):
            v = roll_rows(recv[0, pl.ds(OFFSETS[(-1, 0, 0)] + 8 * t, 8), :], 4)
            if t == 0:
                ext[pl.ds(0, 8), :] = jnp.where(sub8 < 4, F32(0.0), v)
                keep = v
            else:
                ext[pl.ds(8, 8), :] = jnp.where(sub8 < 4, keep, v)
                ext[pl.ds(16, 8), :] = jnp.where(sub8 < 4, v, F32(0.0))
        first = ext[pl.ds(0, 24), :]
        first = jnp.where(slot24 < 9, roll_lanes(first, 9), roll_lanes(first, 18))
        low = pl.ds(slab_row(-1), 24)
        ext[low, :] = jnp.where(group24 == 0, first, ext[low, :])
        five = None
        lane16 = iota((16, 128), 1)
        for h in range(4):
            v = r5[pl.ds(10 * h + 4, 16), :]
            v = jnp.where(lane16 % 32 < 9, roll_lanes(v, 32 * h + 9), roll_lanes(v, 32 * h + 18))
            five = v if h == 0 else jnp.where(lane16 // 32 == h, v, five)
        f5[...] = five

        def neighbours(b, below):
            e = ext[pl.ds(b, 24), :]
            return e, (
                (ext[pl.ds(b - 24, 24), :], ext[pl.ds(b + 24, 24), :]),
                (jnp.where(sub24 == 0, below, ext[pl.ds(b - 1, 24), :]), ext[pl.ds(b + 1, 24), :]),
                (roll_lanes(e, 1), roll_lanes(e, 127)),
            )

        ys = sub24 + (at[1] * BY - 4)

        def main_block(i, _):
            fives = roll_rows(jnp.where(sub8 < 4, r5[pl.ds(pl.multiple_of(i * 8, 8) + 8, 8), :], r5[pl.ds(pl.multiple_of(i * 8, 8), 8), :]), 4)
            for j in range(8):
                b = pl.multiple_of(i * 192, 8) + main_row(j)
                e, nbrs = neighbours(b, jnp.broadcast_to(fives[j:j + 1, :], (24, 128)))
                coefficients(b, e, nbrs, (
                    jnp.broadcast_to(at[0] * BX + (i * 8 + j - 4), (24, 128)), ys, lane24 + at[2] * BZ,
                ))
            return 0
        lax.fori_loop(0, 5, main_block, 0)
        zs = jnp.where(slot24 < 13, slot24 + 119, slot24 - 18) + at[2] * BZ

        for l in range(10):
            b = slab_row(l)
            e, nbrs = neighbours(b, jnp.broadcast_to(f5[l:l + 1, :], (24, 128)))
            coefficients(b, e, nbrs, (group24 * 10 + (at[0] * BX - 4 + l), ys, zs))


    SLAB = [slab_row(l) for l in range(10)]

    def gradient(planes):
        for b in planes:
            p = ext[pl.ds(b, 24), :]
            nbrs = (ext[pl.ds(b + 24, 24), :], ext[pl.ds(b + 1, 24), :], roll_lanes(p, 127))
            for c in range(3):
                source[c, pl.ds(b, 24), :] = weights[c, pl.ds(b, 24), :] * (nbrs[c] - p)

    def scaled_force(c, first, count):
        def block(i, _):
            for u in range(10):
                b = pl.multiple_of(i * 240, 8) + (first + 24 * u)
                source[c, pl.ds(b, 24), :] = weights[c, pl.ds(b, 24), :] * ext[pl.ds(b, 24), :]
            return 0
        lax.fori_loop(0, count // 10, block, 0)

    def ends(ref):
        def each(c, _):
            refresh(ref.at[c])
            return 0
        lax.fori_loop(0, 3, each, 0, unroll=3)

    def sweep(src, dst, planes):
        for b in planes:
            k = [faces[f, pl.ds(b, 24), :] for f in range(6)]
            for c in range(3):
                v = src[c, pl.ds(b, 24), :]
                total = k[0] * src[c, pl.ds(b - 24, 24), :] + k[1] * src[c, pl.ds(b + 24, 24), :]
                total = total + (k[2] * src[c, pl.ds(b - 1, 24), :] + k[3] * src[c, pl.ds(b + 1, 24), :])
                total = total + (k[4] * roll_lanes(v, 1) + k[5] * roll_lanes(v, 127))
                dst[c, pl.ds(b, 24), :] = (
                    (1.0 - OMEGA) * v + source[c, pl.ds(b, 24), :] + weights[c, pl.ds(b, 24), :] * total
                )

    def minus_divergence(src, b, rows):
        x, y, z = (src[c, pl.ds(b, rows), :] for c in range(3))
        return (src[0, pl.ds(b - 24, rows), :] - x) + (src[1, pl.ds(b - 1, rows), :] - y) + (roll_lanes(z, 1) - z)

    def divergence(src, out):
        def slab_part(i, _):
            for u in range(5):
                b = pl.multiple_of(i * 120, 8) + slab_row(u)
                dslab[pl.ds(pl.multiple_of(i * 120, 8) + u * 24, 24), :] = minus_divergence(src, b, 24)
            return 0
        lax.fori_loop(0, 2, slab_part, 0)

        def together(i, _):
            for u in range(5):
                b = pl.ds(pl.multiple_of(i * 120, 8) + u * 24, 24)
                v = dslab[b, :]
                dslab[b, :] = jnp.where(slot24 < 9, v, roll_lanes(v, -9))
            return 0
        lax.fori_loop(0, 2, together, 0)
        lane16 = iota((16, 128), 1)
        for x in range(4, 36):
            h, l = divmod(x, 10)
            total = minus_divergence(src, main_row(x) + 4, 16)
            edge = roll_lanes(dslab[pl.ds(l * 24 + 4, 16), :], -(9 + 32 * h))
            out[pl.ds((x - 4) * 16, 16), :] = jnp.where((lane16 < 8) | (lane16 >= 124), edge, total)

    def main_rows(first, last):
        return [main_row(x) for x in range(first, last + 1)]

    def apply(out):
        ends(source)
        sweep(source, va, SLAB)
        ends(va)
        sweep(va, vb, SLAB + main_rows(2, 36))
        ends(vb)
        sweep(vb, va, SLAB + main_rows(3, 35))
        ends(va)
        divergence(va, out)


    me_z = at[2]
    me_xy = at[0] * ny + at[1]
    nxy = nx * ny

    def z_copy(k, off):
        return pltpu.make_async_remote_copy(
            src_ref=red.at[k], dst_ref=red1.at[k, me_z], send_sem=rs1.at[k], recv_sem=rr1.at[k],
            device_id=(at[0], at[1], lax.rem(me_z + off, nz)), device_id_type=MESH,
        )

    def xy_copy(k, ox, oy):
        return pltpu.make_async_remote_copy(
            src_ref=total1.at[k], dst_ref=red2.at[k, me_xy], send_sem=rs2.at[k], recv_sem=rr2.at[k],
            device_id=(lax.rem(at[0] + ox, nx), lax.rem(at[1] + oy, ny), at[2]), device_id_type=MESH,
        )

    def all_of(k, ref, count, sent, arrived):
        part = ref.at[k, pl.ds(0, count)]
        return pltpu.make_async_remote_copy(
            src_ref=part, dst_ref=part, send_sem=sent.at[k], recv_sem=arrived.at[k],
            device_id=at, device_id_type=MESH,
        )

    offsets_xy = [(ox, oy) for ox in range(nx) for oy in range(ny) if (ox, oy) != (0, 0)]

    def reduce_start(k):
        red1[k, me_z] = red[k]
        for off in range(1, nz):
            z_copy(k, off).start()

    def reduce_middle(k):
        all_of(k, red1, nz - 1, rs1, rr1).wait_recv()
        value = red1[k, 0]
        for i in range(1, nz):
            value = value + red1[k, i]
        total1[k] = value
        red2[k, me_xy] = value
        for ox, oy in offsets_xy:
            xy_copy(k, ox, oy).start()

    cells = float(totals[0] * totals[1] * totals[2])

    def reduce_end(k):
        all_of(k, red2, nxy - 1, rs2, rr2).wait_recv()
        value = red2[k, 0]
        for i in range(1, nxy):
            value = value + red2[k, i]
        gamma, delta, squares = (
            jnp.broadcast_to(jnp.sum(value[i], axis=1, keepdims=True), (8, 128)) for i in range(3)
        )
        norm[k] = squares / cells
        gamma_old, alpha_old = scal[0], scal[1]
        if isinstance(k, int):
            beta = gamma / gamma_old
            alpha = gamma / (delta - beta * gamma / alpha_old)
        else:
            beta = jnp.where(k == 0, F32(0.0), gamma / gamma_old)
            alpha = gamma / (delta - jnp.where(k == 0, F32(0.0), beta * gamma / alpha_old))
        scal[0] = gamma
        scal[1] = alpha
        return alpha, beta


    load_phase = pltpu.make_async_copy(phase_hbm, phase, in_sem.at[0])
    load_force = pltpu.make_async_copy(force_hbm, field.at[pl.ds(1, 3)], in_sem.at[1])
    load_phase.start()
    load_force.start()

    for t in range(0, 56, 8):
        r5[pl.ds(t, 8), :] = jnp.zeros((8, 128), F32)

    barrier = pltpu.get_barrier_semaphore()
    count = jnp.int32(0)
    for d in DIRS:
        ok, device = neighbour(d)

        @pl.when(ok)
        def _():
            pl.semaphore_signal(barrier, inc=1, device_id=device, device_id_type=MESH)
        count = count + ok.astype(jnp.int32)
    for off in range(1, nz):
        pl.semaphore_signal(barrier, inc=1, device_id=(at[0], at[1], lax.rem(me_z + off, nz)), device_id_type=MESH)
    for ox, oy in offsets_xy:
        pl.semaphore_signal(
            barrier, inc=1, device_id=(lax.rem(at[0] + ox, nx), lax.rem(at[1] + oy, ny), at[2]), device_id_type=MESH
        )
    count = count + (nz - 1 + nxy - 1)

    for d in DIRS:
        ok, _ = neighbour(d)

        @pl.when(jnp.logical_not(ok))
        def _():
            def clear_recv(k, _):
                for row in range(0, piece_rows(d), 8):
                    recv[k, pl.ds(OFFSETS[d] + row, 8), :] = jnp.zeros((8, 128), F32)
                return 0
            lax.fori_loop(0, NSETS, clear_recv, 0)

    zero24 = jnp.zeros((24, 128), F32)
    ext[pl.ds(0, 24), :] = zero24
    for ref in (source, va, vb):
        for c in range(3):
            for plane in (0, 1, 2, 3, 38, 39, 40, 41, 52):
                ref[c, pl.ds(plane * 24, 24), :] = zero24
    for f in range(6):
        faces[f, pl.ds(41 * 24, 24), :] = zero24
    for c in range(3):
        weights[c, pl.ds(41 * 24, 24), :] = zero24
        weights[c, pl.ds(52 * 24, 24), :] = zero24
    zero8 = jnp.zeros((8, 128), F32)
    scal[0] = zero8 + 1.0
    scal[1] = zero8 + 1.0
    for ref in (sch, sim, tim, pre):
        def clear(i, _):
            ref[pl.ds(pl.multiple_of(i * 64, 64), 64), :] = jnp.zeros((64, 128), F32)
            return 0
        lax.fori_loop(0, ROWS // 64, clear, 0)

    load_phase.wait()

    def lookup(i, _):
        for u in range(4):
            r = pl.multiple_of(i * 32, 32) + 8 * u
            ids = phase[pl.ds(r, 8), :]
            eta = jnp.zeros((8, 128), F32)
            for level in range(8):
                eta = eta + jnp.where(ids == level, table[level], F32(0.0))
            field[0, pl.ds(r, 8), :] = eta
        return 0
    lax.fori_loop(0, ROWS // 32, lookup, 0)
    for x in range(BX):
        y5[pl.ds(x, 1), :] = field[0, pl.ds(x * 16 + 11, 1), :]
    lax.fori_loop(0, 4, pack_first, 0)
    pl.semaphore_wait(barrier, count)
    has_y_up, _ = neighbour((0, 1, 0))
    has_y_down, _ = neighbour((0, -1, 0))
    copy5_out = pltpu.make_async_remote_copy(
        src_ref=y5, dst_ref=r5.at[pl.ds(8, 32)], send_sem=send5_sem, recv_sem=recv5_sem,
        device_id=(at[0], at[1] + 1, at[2]), device_id_type=MESH,
    )

    @pl.when(has_y_up)
    def _():
        copy5_out.start()

    def send_first(k, _):
        send(k, flat)
        send(k, deep)
        return 0
    lax.fori_loop(0, 4, send_first, 0)

    def rows_loop(body, init, step=8):
        def block(i, carry):
            for u in range(step):
                carry = body(pl.ds(pl.multiple_of(i * (8 * step), 8 * step) + 8 * u, 8), carry)
            return carry
        return lax.fori_loop(0, ROWS // (8 * step), block, init)

    def keep_partials(k, sums):
        for i in range(3):
            red[k, i] = jnp.sum(sums[i], axis=0, keepdims=True)

    def advance(alpha, beta, last):
        def step(at_r, carry):
            e, rr, w, n = field[0, at_r, :], res[at_r, :], wap[at_r, :], nap[at_r, :]
            p = e * rr + beta * sch[at_r, :]
            s = w + beta * sim[at_r, :]
            t = n + beta * tim[at_r, :]
            sch[at_r, :] = p
            sim[at_r, :] = s
            tim[at_r, :] = t
            pre[at_r, :] = pre[at_r, :] + alpha * p
            rr = rr - alpha * s
            w = w - alpha * t
            res[at_r, :] = rr
            wap[at_r, :] = w
            field[last, at_r, :] = e * w
            return carry[0] + rr * (e * rr), carry[1] + w * (e * rr), carry[2] + rr * rr
        return rows_loop(step, (zero8, zero8, zero8))

    def stage(k, _):
        unpack_flat(k)

        @pl.when(k >= 5)
        def _():
            reduce_middle(k - 5)

        @pl.when((k >= 1) & (k < 4))
        def _():
            scaled_force(k - 1, main_row(0), 40)

        @pl.when(k >= 4)
        def _():
            gradient(main_rows(0, 38))

        @pl.when(k >= 3)
        def _():
            sweep(source, va, main_rows(1, 37))
        unpack_deep(k)

        @pl.when(k == 0)
        def _():
            @pl.when(has_y_down)
            def _():
                copy5_out.wait_recv()
            refresh(ext)
            setup()

        @pl.when((k >= 1) & (k < 4))
        def _():
            scaled_force(k - 1, slab_row(0), 10)

        @pl.when(k >= 4)
        def _():
            refresh(ext)
            gradient(SLAB)

        @pl.when(k >= 3)
        def _():
            apply(nap)

        @pl.when(k == 3)
        def _():
            def step(at_r, _):
                r = nap[at_r, :]
                res[at_r, :] = r
                field[4, at_r, :] = field[0, at_r, :] * r
                return 0
            rows_loop(step, 0)

        @pl.when(k == 4)
        def _():
            def step(at_r, carry):
                e, rr, w = field[0, at_r, :], res[at_r, :], nap[at_r, :]
                z = e * rr
                wap[at_r, :] = w
                field[5, at_r, :] = e * w
                return carry[0] + rr * z, carry[1] + w * z, carry[2] + rr * rr
            keep_partials(0, rows_loop(step, (zero8, zero8, zero8)))

        @pl.when(k >= 5)
        def _():
            alpha, beta = reduce_end(k - 5)
            keep_partials(k - 4, advance(alpha, beta, k + 1))

        @pl.when((k >= 3) & (k < 6))
        def _():
            exchange_start(k + 1)

        @pl.when(k >= 4)
        def _():
            reduce_start(k - 4)
        return 0
    lax.fori_loop(0, NSETS, stage, 0)

    reduce_middle(2)
    finish_sends()

    @pl.when(has_y_up)
    def _():
        copy5_out.wait_send()
    for k in range(ITERS):
        all_of(k, red1, nz - 1, rs1, rr1).wait_send()
        all_of(k, red2, nxy - 1, rs2, rr2).wait_send()
    alpha, beta = reduce_end(2)

    def step2(at_r, _):
        rr = res[at_r, :]
        p = field[0, at_r, :] * rr + beta * sch[at_r, :]
        s = wap[at_r, :] + beta * sim[at_r, :]
        press_out[at_r, :] = pre[at_r, :] + alpha * p
        resid_out[at_r, :] = rr - alpha * s
        return 0
    rows_loop(step2, 0)
    norms_out[...] = jnp.where(lane8 == 0, norm[0], jnp.where(lane8 == 1, norm[1], norm[2]))


def solution(mesh):
    sizes = (mesh.shape["gx"], mesh.shape["gy"], mesh.shape["gz"])
    nx, ny, nz = sizes

    def per_device(force, phase, table, flags):
        v = functools.partial(pltpu.VMEM)
        dma = pltpu.SemaphoreType.DMA
        scratch = [
            v((ROWS, 128), jnp.int32),
            v((NSETS + 1, ROWS, 128), F32),
            v((NSETS, 2, 128, 128), F32),
            v((NSETS, 64, 128), F32),
            v((NSETS, 2, 16, 128), F32),
            v((32, 128), F32),
            v((NSETS, RECV_ROWS, 128), F32),
            v((56, 128), F32), v((16, 128), F32),
            v((EROWS, 128), F32),
            v((6, EROWS, 128), F32), v((3, EROWS, 128), F32), v((3, EROWS, 128), F32),
            v((3, EROWS, 128), F32), v((3, EROWS, 128), F32),
            v((120, 128), F32), v((240, 128), F32),
            *[v((ROWS, 128), F32) for _ in range(7)],
            v((ITERS, 3, 1, 128), F32), v((ITERS, 3, 1, 128), F32),
            v((ITERS, nz, 3, 1, 128), F32), v((ITERS, nx * ny, 3, 1, 128), F32),
            v((2, 8, 128), F32), v((ITERS, 8, 128), F32),
            dma((2,)), dma((26,)), dma((5, 26)), dma, dma,
            dma((ITERS,)), dma((ITERS,)), dma((ITERS,)), dma((ITERS,)),
        ]
        hbm = pl.BlockSpec(memory_space=pl.ANY)
        smem = pl.BlockSpec(memory_space=pltpu.SMEM)
        press, resid, norms = pl.pallas_call(
            functools.partial(kernel, sizes),
            out_shape=(
                pltpu.VMEM((ROWS, 128), F32),
                pltpu.VMEM((ROWS, 128), F32),
                pltpu.VMEM((8, 128), F32),
            ),
            in_specs=[hbm, hbm, smem, smem],
            out_specs=(pl.BlockSpec(memory_space=pltpu.VMEM), pl.BlockSpec(memory_space=pltpu.VMEM), pl.BlockSpec(memory_space=pltpu.VMEM)),
            scratch_shapes=scratch,
            compiler_params=pltpu.CompilerParams(
                collective_id=0, has_side_effects=True, vmem_limit_bytes=60 * 1024 * 1024
            ),
        )(force.reshape(3, ROWS, BZ), phase.reshape(ROWS, BZ), table, flags)
        return press.reshape(BX, BY, BZ), resid.reshape(BX, BY, BZ), norms[0, :ITERS]

    return jax.shard_map(
        per_device,
        mesh=mesh,
        in_specs=(P(None, "gx", "gy", "gz"), P("gx", "gy", "gz"), P(), P()),
        out_specs=(P("gx", "gy", "gz"), P("gx", "gy", "gz"), P()),
        check_vma=False,
    )
```

```python
import functools

import jax
import jax.numpy as jnp
from jax import lax
from jax.experimental import pallas as pl
from jax.experimental.pallas import tpu as pltpu
from jax.sharding import PartitionSpec as P

ITERS = 3
OMEGA = 0.8
F32 = jnp.float32
MESH = pl.DeviceIdType.MESH

BX, BY, BZ = 32, 16, 128
ROWS = BX * BY
PLANES = 53
EROWS = PLANES * 24
NSETS = 7

DIRS = [(dx, dy, dz) for dz in (0, 1, -1) for dy in (1, -1, 0) for dx in (0, 1, -1) if (dx, dy, dz) != (0, 0, 0)]
DIRS.sort(key=lambda d: -sum(map(abs, d)))
DIR_AT = {d: i for i, d in enumerate(DIRS)}


def piece_rows(d):
    dx, dy, dz = d
    if dz == 0:
        if dx and dy:
            return 16
        return 128 if dy else 80
    if dx and dy:
        return 8
    if dy:
        return 16
    return 16 if dx else 64


OFFSETS = {}
RECV_ROWS = 0
for _d in DIRS:
    OFFSETS[_d] = RECV_ROWS
    RECV_ROWS += piece_rows(_d)


def iota(shape, dim):
    return lax.broadcasted_iota(jnp.int32, shape, dim)


def roll_lanes(v, by):
    by = by % 128
    return v if by == 0 else pltpu.roll(v, by, 1)


def roll_rows(v, by):
    return pltpu.roll(v, by % v.shape[0], 0)


def kernel(
    sizes,
    force_hbm, phase_hbm, table, flags,
    press_out, resid_out, norms_out,
    phase, field, ystage, cstage, dstage, y5, recv, r5, f5,
    ext, faces, weights, source, va, vb, halo, dslab,
    res, sch, wap, sim, tim, nap, pre,
    red, total1, red1, red2, scal, norm,
    in_sem, send_sem, recv_sem, send5_sem, recv5_sem, rs1, rr1, rs2, rr2,
):
    nx, ny, nz = sizes
    at = (lax.axis_index("gx"), lax.axis_index("gy"), lax.axis_index("gz"))

    def neighbour(d):
        ok = None
        for dim in range(3):
            if d[dim] == 0:
                continue
            here = at[dim] < sizes[dim] - 1 if d[dim] > 0 else at[dim] > 0
            ok = here if ok is None else jnp.logical_and(ok, here)
        return ok, tuple(at[dim] + d[dim] for dim in range(3))

    def recv_at(k, d, start=0, rows=None):
        return recv.at[k, pl.ds(OFFSETS[d] + start, piece_rows(d) if rows is None else rows)]

    def pieces(k, d):
        dx, dy, dz = d
        to = tuple(-a for a in d)
        if dz == 0:
            if dx and dy:
                side = 0 if dy < 0 else 1
                src = ystage.at[k, side, pl.ds(0 if dx < 0 else 112, 16)]
                return src, recv_at(k, to)
            if dy:
                return ystage.at[k, 0 if dy < 0 else 1], recv_at(k, to)
            if dx < 0:
                return field.at[k, pl.ds(0, 64)], recv_at(k, to, 0, 64)
            return field.at[k, pl.ds(ROWS - 80, 80)], recv_at(k, to)
        side = 0 if dy < 0 else 1
        if dx and dy:
            return dstage.at[k, side, pl.ds(0 if dx < 0 else 8, 8)], recv_at(k, to)
        if dy:
            return dstage.at[k, side], recv_at(k, to)
        if dx:
            return cstage.at[k, pl.ds(0 if dx < 0 else 48, 16)], recv_at(k, to)
        return cstage.at[k], recv_at(k, to)

    def copy_of(k, d):
        src, dst = pieces(k, d)
        _, device = neighbour(d)
        to = tuple(-a for a in d)
        return pltpu.make_async_remote_copy(
            src_ref=src, dst_ref=dst,
            send_sem=send_sem.at[DIR_AT[d]], recv_sem=recv_sem.at[lax.rem(k, 5), DIR_AT[to]],
            device_id=device, device_id_type=MESH,
        )

    def incoming(k, d):
        to = tuple(-a for a in d)
        src, dst = pieces(k, to)
        return pltpu.make_async_remote_copy(
            src_ref=src, dst_ref=dst,
            send_sem=send_sem.at[DIR_AT[to]], recv_sem=recv_sem.at[lax.rem(k, 5), DIR_AT[d]],
            device_id=at, device_id_type=MESH,
        )

    sub8 = iota((8, 128), 0)
    lane8 = iota((8, 128), 1)
    group8, slot8 = lane8 // 16, lane8 % 16
    lane24 = iota((24, 128), 1)
    sub24 = iota((24, 128), 0)
    group24, slot24 = lane24 // 32, lane24 % 32
    bigroup8, bislot8 = lane8 // 32, lane8 % 32


    def pack_y(k):
        def pair(xp, _):
            base = pl.multiple_of(xp * 32, 32)
            a0, a1 = field[k, pl.ds(base, 8), :], field[k, pl.ds(base + 8, 8), :]
            b0, b1 = field[k, pl.ds(base + 16, 8), :], field[k, pl.ds(base + 24, 8), :]
            to = pl.multiple_of(xp * 8, 8)
            ystage[k, 0, pl.ds(to, 8), :] = jnp.where(sub8 < 4, a0, roll_rows(b0, 4))
            ystage[k, 1, pl.ds(to, 8), :] = jnp.where(sub8 < 4, roll_rows(a1, 4), b1)
            return 0
        lax.fori_loop(0, BX // 2, pair, 0, unroll=16)

    def pack_z(k):
        def block(xp, _):
            ends = []
            for u in range(2):
                acc = [[None, None] for _ in range(3)]
                for g in range(8):
                    base = pl.multiple_of(xp * 256, 256) + (u * 128 + g * 16)
                    a, b = field[k, pl.ds(base, 8), :], field[k, pl.ds(base + 8, 8), :]
                    for i, v in enumerate((a, b, jnp.where(sub8 < 4, a, b))):
                        for m in range(2):
                            r = roll_lanes(v, 9 * m + 16 * g)
                            acc[i][m] = r if g == 0 else jnp.where(group8 == g, r, acc[i][m])
                a, b, c = (jnp.where(slot8 < 4, lo, hi) for lo, hi in acc)
                to = pl.multiple_of(xp * 32, 32) + u * 16
                cstage[k, pl.ds(to, 8), :] = a
                cstage[k, pl.ds(to + 8, 8), :] = b
                ends.append(c)
            to = pl.ds(pl.multiple_of(xp * 8, 8), 8)
            dstage[k, 0, to, :] = jnp.where(sub8 < 4, ends[0], roll_rows(ends[1], 4))
            dstage[k, 1, to, :] = jnp.where(sub8 < 4, roll_rows(ends[0], 4), ends[1])
            return 0
        lax.fori_loop(0, 2, block, 0, unroll=2)

    flat = [d for d in DIRS if d[2] == 0]
    deep = [d for d in DIRS if d[2] != 0]

    def send(k, dirs):
        for d in dirs:
            ok, _ = neighbour(d)

            @pl.when(ok)
            def _():
                copy_of(k, d).start()

    def exchange_start(k):
        pack_y(k)
        send(k, flat)
        pack_z(k)
        send(k, deep)

    def pack_first(k, _):
        @pl.when(k == 1)
        def _():
            load_force.wait()
        pack_y(k)
        pack_z(k)
        return 0

    def receive(k, dirs):
        for d in dirs:
            ok, _ = neighbour(d)

            @pl.when(ok)
            def _():
                incoming(k, d).wait_recv()

    def finish_sends():
        for d in DIRS:
            ok, device = neighbour(d)
            rows = 64 if d == (-1, 0, 0) else piece_rows(d)

            @pl.when(ok)
            def _():
                part = recv.at[pl.ds(0, NSETS), pl.ds(0, rows)]
                pltpu.make_async_remote_copy(
                    src_ref=part, dst_ref=part, send_sem=send_sem.at[DIR_AT[d]], recv_sem=recv_sem.at[0, DIR_AT[d]],
                    device_id=device, device_id_type=MESH,
                ).wait_send()

    def main_row(x):
        return (1 + x) * 24

    def slab_row(l):
        return (42 + l) * 24

    def refresh(ref):
        low, high = pl.ds(slab_row(9), 24), pl.ds(slab_row(0), 24)
        ref[pl.ds(slab_row(-1), 24), :] = roll_lanes(ref[low, :], 32)
        ref[pl.ds(slab_row(10), 24), :] = roll_lanes(ref[high, :], -32)

    def unpack_flat(k):
        receive(k, flat)

        def planes(own, low, high, first, pairs):
            for xp in range(pairs):
                lo, hi = low(xp * 8), high(xp * 8)
                los, his = roll_rows(lo, 4), roll_rows(hi, 4)
                for half in range(2):
                    ra, rb = (roll_rows(own(xp * 32 + 16 * half + 8 * t), 4) for t in range(2))
                    to = main_row(first + 2 * xp + half)
                    ext[pl.ds(to, 8), :] = jnp.where(sub8 < 4, (lo, los)[half], ra)
                    ext[pl.ds(to + 8, 8), :] = jnp.where(sub8 < 4, ra, rb)
                    ext[pl.ds(to + 16, 8), :] = jnp.where(sub8 < 4, rb, (his, hi)[half])

        def of(d, start=0):
            return lambda row: recv[k, pl.ds(row + (OFFSETS[d] + start), 8), :]

        planes(lambda r: field[k, pl.ds(r, 8), :], of((0, -1, 0)), of((0, 1, 0)), 4, 16)
        planes(of((-1, 0, 0), 16), of((-1, -1, 0)), of((-1, 1, 0)), 0, 2)
        planes(of((1, 0, 0)), of((1, -1, 0)), of((1, 1, 0)), 36, 2)

        def own(i, _):
            for u in range(5):
                for t in range(3):
                    lo, hi = None, None
                    for h in range(4):
                        v = ext[pl.ds(pl.multiple_of(i * 120, 8) + (main_row(10 * h + u) + 8 * t), 8), :]
                        a, b = roll_lanes(v, 32 * h + 9), roll_lanes(v, 32 * h + 18)
                        lo = a if h == 0 else jnp.where(bigroup8 == h, a, lo)
                        hi = b if h == 0 else jnp.where(bigroup8 == h, b, hi)
                    to = pl.ds(pl.multiple_of(i * 120, 8) + (slab_row(u) + 8 * t), 8)
                    ext[to, :] = jnp.where(bislot8 < 9, lo, hi)
            return 0
        lax.fori_loop(0, 2, own, 0, unroll=2)

    def unpack_deep(k):
        receive(k, deep)

        def merged(d, row):
            low = recv[k, pl.ds(OFFSETS[(d[0], d[1], -1)] + row, 8), :]
            high = recv[k, pl.ds(OFFSETS[(d[0], d[1], 1)] + row, 8), :]
            return jnp.where(slot8 < 4, high, low)

        inner = []
        for t in range(2):
            inner.append([merged((-1, 0), 8 * t)] + [merged((0, 0), xb * 16 + 8 * t) for xb in range(4)] + [merged((1, 0), 8 * t)])
        sides = []
        for xb in range(6):
            dx, row = (-1, 0) if xb == 0 else (1, 0) if xb == 5 else (0, (xb - 1) // 2 * 8)
            above, below = merged((dx, 1), row), merged((dx, -1), row)
            if xb % 2 == 1:
                sides.append(jnp.where(sub8 < 4, below, roll_rows(above, 4)))
            else:
                sides.append(jnp.where(sub8 < 4, roll_rows(below, 4), above))

        def shifted(parts, i):
            return roll_lanes(jnp.where(group8 < 4, parts[i + 1], parts[i]), 64)

        def arrived(_, carry):
            for i in range(5):
                a, b = roll_rows(shifted(inner[0], i), 4), roll_rows(shifted(inner[1], i), 4)
                c = shifted(sides, i)
                tiles = (jnp.where(sub8 < 4, c, a), jnp.where(sub8 < 4, a, b), jnp.where(sub8 < 4, b, c))
                for t in range(3):
                    halo[pl.ds(i * 24 + 8 * t, 8), :] = tiles[t]
            return carry
        lax.fori_loop(0, 1, arrived, 0)

        def outer(l, _):
            for t in range(3):
                acc = None
                for h in range(4):
                    x = 10 * h + l
                    v = halo[pl.ds(x // 8 * 24 + 8 * t, 8), :]
                    a = roll_lanes(v, 32 * h + 9 - 16 * (x % 8))
                    acc = a if h == 0 else jnp.where(bigroup8 == h, a, acc)
                to = pl.ds(slab_row(l) + 8 * t, 8)
                ext[to, :] = jnp.where((bislot8 >= 9) & (bislot8 < 18), acc, ext[to, :])
            return 0
        for l in range(10):
            outer(l, 0)


    walls = [jnp.where(flags[f] == 0, F32(1.0), F32(0.0)) for f in range(6)]
    totals = (nx * BX, ny * BY, nz * BZ)

    def coefficients(b, e, nbrs, spots):
        inside = None
        diag = jnp.zeros_like(e)
        extra = [jnp.zeros_like(e) for _ in range(3)]
        for axis in range(3):
            for side in range(2):
                spot = spots[axis] + (1 if side else -1)
                here = (spot >= 0) & (spot < totals[axis])
                face = 0.5 * (e + nbrs[axis][side])
                wall = walls[2 * axis + side]
                outer = jnp.where(here, F32(0.0), e)
                diag = diag + jnp.where(here, face, e * wall)
                extra[axis] = extra[axis] + outer * (1.0 - wall)
                faces[2 * axis + side, pl.ds(b, 24), :] = face
            here = (spots[axis] >= 0) & (spots[axis] < totals[axis])
            inside = here if inside is None else inside & here
        for c in range(3):
            d = diag + extra[c]
            good = inside & (d > 0)
            weights[c, pl.ds(b, 24), :] = jnp.where(good, OMEGA / jnp.where(good, d, F32(1.0)), F32(0.0))

    def setup():
        keep = None
        for t in range(2):
            v = roll_rows(recv[0, pl.ds(OFFSETS[(-1, 0, 0)] + 8 * t, 8), :], 4)
            if t == 0:
                ext[pl.ds(0, 8), :] = jnp.where(sub8 < 4, F32(0.0), v)
                keep = v
            else:
                ext[pl.ds(8, 8), :] = jnp.where(sub8 < 4, keep, v)
                ext[pl.ds(16, 8), :] = jnp.where(sub8 < 4, v, F32(0.0))
        first = ext[pl.ds(0, 24), :]
        first = jnp.where(slot24 < 9, roll_lanes(first, 9), roll_lanes(first, 18))
        low = pl.ds(slab_row(-1), 24)
        ext[low, :] = jnp.where(group24 == 0, first, ext[low, :])
        five = None
        lane16 = iota((16, 128), 1)
        for h in range(4):
            v = r5[pl.ds(10 * h + 4, 16), :]
            v = jnp.where(lane16 % 32 < 9, roll_lanes(v, 32 * h + 9), roll_lanes(v, 32 * h + 18))
            five = v if h == 0 else jnp.where(lane16 // 32 == h, v, five)
        f5[...] = five

        def neighbours(b, below):
            e = ext[pl.ds(b, 24), :]
            return e, (
                (ext[pl.ds(b - 24, 24), :], ext[pl.ds(b + 24, 24), :]),
                (jnp.where(sub24 == 0, below, ext[pl.ds(b - 1, 24), :]), ext[pl.ds(b + 1, 24), :]),
                (roll_lanes(e, 1), roll_lanes(e, 127)),
            )

        ys = sub24 + (at[1] * BY - 4)

        def main_block(i, _):
            fives = roll_rows(jnp.where(sub8 < 4, r5[pl.ds(pl.multiple_of(i * 8, 8) + 8, 8), :], r5[pl.ds(pl.multiple_of(i * 8, 8), 8), :]), 4)
            for j in range(8):
                b = pl.multiple_of(i * 192, 8) + main_row(j)
                e, nbrs = neighbours(b, jnp.broadcast_to(fives[j:j + 1, :], (24, 128)))
                coefficients(b, e, nbrs, (
                    jnp.broadcast_to(at[0] * BX + (i * 8 + j - 4), (24, 128)), ys, lane24 + at[2] * BZ,
                ))
            return 0
        lax.fori_loop(0, 5, main_block, 0)
        zs = jnp.where(slot24 < 13, slot24 + 119, slot24 - 18) + at[2] * BZ

        for l in range(10):
            b = slab_row(l)
            e, nbrs = neighbours(b, jnp.broadcast_to(f5[l:l + 1, :], (24, 128)))
            coefficients(b, e, nbrs, (group24 * 10 + (at[0] * BX - 4 + l), ys, zs))


    SLAB = [slab_row(l) for l in (9, 0, 1, 2, 3, 4, 5, 6, 7, 8)]

    def gradient(planes):
        for b in planes:
            p = ext[pl.ds(b, 24), :]
            nbrs = (ext[pl.ds(b + 24, 24), :], ext[pl.ds(b + 1, 24), :], roll_lanes(p, 127))
            for c in range(3):
                source[c, pl.ds(b, 24), :] = weights[c, pl.ds(b, 24), :] * (nbrs[c] - p)

    def scaled_force(c, first, count):
        def block(i, _):
            for u in range(10):
                b = pl.multiple_of(i * 240, 8) + (first + 24 * u)
                source[c, pl.ds(b, 24), :] = weights[c, pl.ds(b, 24), :] * ext[pl.ds(b, 24), :]
            return 0
        lax.fori_loop(0, count // 10, block, 0)

    def ends(ref):
        def each(c, _):
            refresh(ref.at[c])
            return 0
        lax.fori_loop(0, 3, each, 0, unroll=3)

    def sweep(src, dst, planes):
        for b in planes:
            k = [faces[f, pl.ds(b, 24), :] for f in range(6)]
            for c in range(3):
                v = src[c, pl.ds(b, 24), :]
                total = k[0] * src[c, pl.ds(b - 24, 24), :] + k[1] * src[c, pl.ds(b + 24, 24), :]
                total = total + (k[2] * src[c, pl.ds(b - 1, 24), :] + k[3] * src[c, pl.ds(b + 1, 24), :])
                total = total + (k[4] * roll_lanes(v, 1) + k[5] * roll_lanes(v, 127))
                dst[c, pl.ds(b, 24), :] = (
                    (1.0 - OMEGA) * v + source[c, pl.ds(b, 24), :] + weights[c, pl.ds(b, 24), :] * total
                )

    def minus_divergence(src, b, rows):
        x, y, z = (src[c, pl.ds(b, rows), :] for c in range(3))
        return (src[0, pl.ds(b - 24, rows), :] - x) + (src[1, pl.ds(b - 1, rows), :] - y) + (roll_lanes(z, 1) - z)

    def divergence(src, out):
        def slab_part(i, _):
            for u in range(5):
                b = pl.multiple_of(i * 120, 8) + slab_row(u)
                dslab[pl.ds(pl.multiple_of(i * 120, 8) + u * 24, 24), :] = minus_divergence(src, b, 24)
            return 0
        lax.fori_loop(0, 2, slab_part, 0, unroll=2)

        def together(i, _):
            for u in range(5):
                b = pl.ds(pl.multiple_of(i * 120, 8) + u * 24, 24)
                v = dslab[b, :]
                dslab[b, :] = jnp.where(slot24 < 9, v, roll_lanes(v, -9))
            return 0
        lax.fori_loop(0, 2, together, 0, unroll=2)
        lane16 = iota((16, 128), 1)
        for x in range(4, 36):
            h, l = divmod(x, 10)
            total = minus_divergence(src, main_row(x) + 4, 16)
            edge = roll_lanes(dslab[pl.ds(l * 24 + 4, 16), :], -(9 + 32 * h))
            out[pl.ds((x - 4) * 16, 16), :] = jnp.where((lane16 < 8) | (lane16 >= 124), edge, total)

    def main_rows(first, last):
        return [main_row(x) for x in range(first, last + 1)]

    def apply(out):
        ends(source)
        sweep(source, va, SLAB)
        ends(va)
        sweep(va, vb, SLAB + main_rows(2, 36))
        ends(vb)
        sweep(vb, va, SLAB + main_rows(3, 35))
        ends(va)
        divergence(va, out)


    me_z = at[2]
    me_xy = at[0] * ny + at[1]
    nxy = nx * ny

    def z_copy(k, off):
        return pltpu.make_async_remote_copy(
            src_ref=red.at[k], dst_ref=red1.at[k, me_z], send_sem=rs1.at[k], recv_sem=rr1.at[k],
            device_id=(at[0], at[1], lax.rem(me_z + off, nz)), device_id_type=MESH,
        )

    def xy_copy(k, ox, oy):
        return pltpu.make_async_remote_copy(
            src_ref=total1.at[k], dst_ref=red2.at[k, me_xy], send_sem=rs2.at[k], recv_sem=rr2.at[k],
            device_id=(lax.rem(at[0] + ox, nx), lax.rem(at[1] + oy, ny), at[2]), device_id_type=MESH,
        )

    def all_of(k, ref, count, sent, arrived):
        part = ref.at[k, pl.ds(0, count)]
        return pltpu.make_async_remote_copy(
            src_ref=part, dst_ref=part, send_sem=sent.at[k], recv_sem=arrived.at[k],
            device_id=at, device_id_type=MESH,
        )

    offsets_xy = [(ox, oy) for ox in range(nx) for oy in range(ny) if (ox, oy) != (0, 0)]

    def reduce_start(k):
        red1[k, me_z] = red[k]
        for off in range(1, nz):
            z_copy(k, off).start()

    def reduce_middle(k):
        all_of(k, red1, nz - 1, rs1, rr1).wait_recv()
        value = red1[k, 0]
        for i in range(1, nz):
            value = value + red1[k, i]
        total1[k] = value
        red2[k, me_xy] = value
        for ox, oy in offsets_xy:
            xy_copy(k, ox, oy).start()

    cells = float(totals[0] * totals[1] * totals[2])

    def reduce_end(k):
        all_of(k, red2, nxy - 1, rs2, rr2).wait_recv()
        value = red2[k, 0]
        for i in range(1, nxy):
            value = value + red2[k, i]
        gamma, delta, squares = (
            jnp.broadcast_to(jnp.sum(value[i], axis=1, keepdims=True), (8, 128)) for i in range(3)
        )
        norm[k] = squares / cells
        gamma_old, alpha_old = scal[0], scal[1]
        if isinstance(k, int):
            beta = gamma / gamma_old
            alpha = gamma / (delta - beta * gamma / alpha_old)
        else:
            beta = jnp.where(k == 0, F32(0.0), gamma / gamma_old)
            alpha = gamma / (delta - jnp.where(k == 0, F32(0.0), beta * gamma / alpha_old))
        scal[0] = gamma
        scal[1] = alpha
        return alpha, beta


    load_phase = pltpu.make_async_copy(phase_hbm, phase, in_sem.at[0])
    load_force = pltpu.make_async_copy(force_hbm, field.at[pl.ds(1, 3)], in_sem.at[1])
    load_phase.start()
    load_force.start()

    for t in range(0, 56, 8):
        r5[pl.ds(t, 8), :] = jnp.zeros((8, 128), F32)

    barrier = pltpu.get_barrier_semaphore()
    count = jnp.int32(0)
    for d in DIRS:
        ok, device = neighbour(d)

        @pl.when(ok)
        def _():
            pl.semaphore_signal(barrier, inc=1, device_id=device, device_id_type=MESH)
        count = count + ok.astype(jnp.int32)
    for off in range(1, nz):
        pl.semaphore_signal(barrier, inc=1, device_id=(at[0], at[1], lax.rem(me_z + off, nz)), device_id_type=MESH)
    for ox, oy in offsets_xy:
        pl.semaphore_signal(
            barrier, inc=1, device_id=(lax.rem(at[0] + ox, nx), lax.rem(at[1] + oy, ny), at[2]), device_id_type=MESH
        )
    count = count + (nz - 1 + nxy - 1)

    for d in DIRS:
        ok, _ = neighbour(d)

        @pl.when(jnp.logical_not(ok))
        def _():
            def clear_recv(k, _):
                for row in range(0, piece_rows(d), 8):
                    recv[k, pl.ds(OFFSETS[d] + row, 8), :] = jnp.zeros((8, 128), F32)
                return 0
            lax.fori_loop(0, NSETS, clear_recv, 0)

    zero24 = jnp.zeros((24, 128), F32)
    ext[pl.ds(0, 24), :] = zero24
    for ref in (source, va, vb):
        for c in range(3):
            for plane in (0, 1, 2, 3, 38, 39, 40, 41, 52):
                ref[c, pl.ds(plane * 24, 24), :] = zero24
    for f in range(6):
        faces[f, pl.ds(41 * 24, 24), :] = zero24
    for c in range(3):
        weights[c, pl.ds(41 * 24, 24), :] = zero24
        weights[c, pl.ds(52 * 24, 24), :] = zero24
    zero8 = jnp.zeros((8, 128), F32)
    scal[0] = zero8 + 1.0
    scal[1] = zero8 + 1.0
    for ref in (sch, sim, tim, pre):
        def clear(i, _):
            ref[pl.ds(pl.multiple_of(i * 64, 64), 64), :] = jnp.zeros((64, 128), F32)
            return 0
        lax.fori_loop(0, ROWS // 64, clear, 0)

    load_phase.wait()

    def lookup(i, _):
        for u in range(4):
            r = pl.multiple_of(i * 32, 32) + 8 * u
            ids = phase[pl.ds(r, 8), :]
            eta = jnp.zeros((8, 128), F32)
            for level in range(8):
                eta = eta + jnp.where(ids == level, table[level], F32(0.0))
            field[0, pl.ds(r, 8), :] = eta
        return 0
    lax.fori_loop(0, ROWS // 32, lookup, 0)
    for x in range(BX):
        y5[pl.ds(x, 1), :] = field[0, pl.ds(x * 16 + 11, 1), :]
    lax.fori_loop(0, 4, pack_first, 0)
    pl.semaphore_wait(barrier, count)
    has_y_up, _ = neighbour((0, 1, 0))
    has_y_down, _ = neighbour((0, -1, 0))
    copy5_out = pltpu.make_async_remote_copy(
        src_ref=y5, dst_ref=r5.at[pl.ds(8, 32)], send_sem=send5_sem, recv_sem=recv5_sem,
        device_id=(at[0], at[1] + 1, at[2]), device_id_type=MESH,
    )

    @pl.when(has_y_up)
    def _():
        copy5_out.start()

    def send_first(k, _):
        send(k, flat)
        send(k, deep)
        return 0
    lax.fori_loop(0, 4, send_first, 0)

    def rows_loop(body, init, step=8):
        def block(i, carry):
            for u in range(step):
                carry = body(pl.ds(pl.multiple_of(i * (8 * step), 8 * step) + 8 * u, 8), carry)
            return carry
        return lax.fori_loop(0, ROWS // (8 * step), block, init)

    def keep_partials(k, sums):
        for i in range(3):
            red[k, i] = jnp.sum(sums[i], axis=0, keepdims=True)

    def advance(alpha, beta, last):
        def step(at_r, carry):
            e, rr, w, n = field[0, at_r, :], res[at_r, :], wap[at_r, :], nap[at_r, :]
            p = e * rr + beta * sch[at_r, :]
            s = w + beta * sim[at_r, :]
            t = n + beta * tim[at_r, :]
            sch[at_r, :] = p
            sim[at_r, :] = s
            tim[at_r, :] = t
            pre[at_r, :] = pre[at_r, :] + alpha * p
            rr = rr - alpha * s
            w = w - alpha * t
            res[at_r, :] = rr
            wap[at_r, :] = w
            field[last, at_r, :] = e * w
            return carry[0] + rr * (e * rr), carry[1] + w * (e * rr), carry[2] + rr * rr
        return rows_loop(step, (zero8, zero8, zero8))

    def stage(k, _):
        unpack_flat(k)

        @pl.when(k >= 5)
        def _():
            reduce_middle(k - 5)

        @pl.when((k >= 1) & (k < 4))
        def _():
            scaled_force(k - 1, main_row(0), 40)

        @pl.when(k >= 4)
        def _():
            gradient(main_rows(0, 38))

        @pl.when(k >= 3)
        def _():
            sweep(source, va, main_rows(1, 37))
        unpack_deep(k)

        @pl.when(k == 0)
        def _():
            @pl.when(has_y_down)
            def _():
                copy5_out.wait_recv()
            refresh(ext)
            setup()

        @pl.when((k >= 1) & (k < 4))
        def _():
            scaled_force(k - 1, slab_row(0), 10)

        @pl.when(k >= 4)
        def _():
            refresh(ext)
            gradient(SLAB)

        @pl.when(k >= 3)
        def _():
            apply(nap)

        @pl.when(k == 3)
        def _():
            def step(at_r, _):
                r = nap[at_r, :]
                res[at_r, :] = r
                field[4, at_r, :] = field[0, at_r, :] * r
                return 0
            rows_loop(step, 0)

        @pl.when(k == 4)
        def _():
            def step(at_r, carry):
                e, rr, w = field[0, at_r, :], res[at_r, :], nap[at_r, :]
                z = e * rr
                wap[at_r, :] = w
                field[5, at_r, :] = e * w
                return carry[0] + rr * z, carry[1] + w * z, carry[2] + rr * rr
            keep_partials(0, rows_loop(step, (zero8, zero8, zero8)))

        @pl.when(k >= 5)
        def _():
            alpha, beta = reduce_end(k - 5)
            keep_partials(k - 4, advance(alpha, beta, k + 1))

        @pl.when((k >= 3) & (k < 6))
        def _():
            exchange_start(k + 1)

        @pl.when(k >= 4)
        def _():
            reduce_start(k - 4)
        return 0
    lax.fori_loop(0, NSETS, stage, 0)

    reduce_middle(2)
    finish_sends()

    @pl.when(has_y_up)
    def _():
        copy5_out.wait_send()
    for k in range(ITERS):
        all_of(k, red1, nz - 1, rs1, rr1).wait_send()
        all_of(k, red2, nxy - 1, rs2, rr2).wait_send()
    alpha, beta = reduce_end(2)

    def step2(at_r, _):
        rr = res[at_r, :]
        p = field[0, at_r, :] * rr + beta * sch[at_r, :]
        s = wap[at_r, :] + beta * sim[at_r, :]
        press_out[at_r, :] = pre[at_r, :] + alpha * p
        resid_out[at_r, :] = rr - alpha * s
        return 0
    rows_loop(step2, 0)
    norms_out[...] = jnp.where(lane8 == 0, norm[0], jnp.where(lane8 == 1, norm[1], norm[2]))


def solution(mesh):
    sizes = (mesh.shape["gx"], mesh.shape["gy"], mesh.shape["gz"])
    nx, ny, nz = sizes

    def per_device(force, phase, table, flags):
        v = functools.partial(pltpu.VMEM)
        dma = pltpu.SemaphoreType.DMA
        scratch = [
            v((ROWS, 128), jnp.int32),
            v((NSETS + 1, ROWS, 128), F32),
            v((NSETS, 2, 128, 128), F32),
            v((NSETS, 64, 128), F32),
            v((NSETS, 2, 16, 128), F32),
            v((32, 128), F32),
            v((NSETS, RECV_ROWS, 128), F32),
            v((56, 128), F32), v((16, 128), F32),
            v((EROWS, 128), F32),
            v((6, EROWS, 128), F32), v((3, EROWS, 128), F32), v((3, EROWS, 128), F32),
            v((3, EROWS, 128), F32), v((3, EROWS, 128), F32),
            v((120, 128), F32), v((240, 128), F32),
            *[v((ROWS, 128), F32) for _ in range(7)],
            v((ITERS, 3, 1, 128), F32), v((ITERS, 3, 1, 128), F32),
            v((ITERS, nz, 3, 1, 128), F32), v((ITERS, nx * ny, 3, 1, 128), F32),
            v((2, 8, 128), F32), v((ITERS, 8, 128), F32),
            dma((2,)), dma((26,)), dma((5, 26)), dma, dma,
            dma((ITERS,)), dma((ITERS,)), dma((ITERS,)), dma((ITERS,)),
        ]
        hbm = pl.BlockSpec(memory_space=pl.ANY)
        smem = pl.BlockSpec(memory_space=pltpu.SMEM)
        press, resid, norms = pl.pallas_call(
            functools.partial(kernel, sizes),
            out_shape=(
                pltpu.VMEM((ROWS, 128), F32),
                pltpu.VMEM((ROWS, 128), F32),
                pltpu.VMEM((8, 128), F32),
            ),
            in_specs=[hbm, hbm, smem, smem],
            out_specs=(pl.BlockSpec(memory_space=pltpu.VMEM), pl.BlockSpec(memory_space=pltpu.VMEM), pl.BlockSpec(memory_space=pltpu.VMEM)),
            scratch_shapes=scratch,
            compiler_params=pltpu.CompilerParams(
                collective_id=0, has_side_effects=True, vmem_limit_bytes=60 * 1024 * 1024
            ),
        )(force.reshape(3, ROWS, BZ), phase.reshape(ROWS, BZ), table, flags)
        return press.reshape(BX, BY, BZ), resid.reshape(BX, BY, BZ), norms[0, :ITERS]

    return jax.shard_map(
        per_device,
        mesh=mesh,
        in_specs=(P(None, "gx", "gy", "gz"), P("gx", "gy", "gz"), P(), P()),
        out_specs=(P("gx", "gy", "gz"), P("gx", "gy", "gz"), P()),
        check_vma=False,
    )
```

```python
import functools

import jax
import jax.numpy as jnp
from jax import lax
from jax.experimental import pallas as pl
from jax.experimental.pallas import tpu as pltpu
from jax.sharding import PartitionSpec as P

ITERS = 3
OMEGA = 0.8
F32 = jnp.float32
MESH = pl.DeviceIdType.MESH

BX, BY, BZ = 32, 16, 128
ROWS = BX * BY
PLANES = 53
EROWS = PLANES * 24
NSETS = 7

DIRS = [(dx, dy, dz) for dz in (0, 1, -1) for dy in (1, -1, 0) for dx in (0, 1, -1) if (dx, dy, dz) != (0, 0, 0)]
DIRS.sort(key=lambda d: -sum(map(abs, d)))
DIR_AT = {d: i for i, d in enumerate(DIRS)}


def piece_rows(d):
    dx, dy, dz = d
    if dz == 0:
        if dx and dy:
            return 16
        return 128 if dy else 80
    if dx and dy:
        return 8
    if dy:
        return 16
    return 16 if dx else 64


OFFSETS = {}
RECV_ROWS = 0
for _d in DIRS:
    OFFSETS[_d] = RECV_ROWS
    RECV_ROWS += piece_rows(_d)


def iota(shape, dim):
    return lax.broadcasted_iota(jnp.int32, shape, dim)


def roll_lanes(v, by):
    by = by % 128
    return v if by == 0 else pltpu.roll(v, by, 1)


def roll_rows(v, by):
    return pltpu.roll(v, by % v.shape[0], 0)


def kernel(
    sizes,
    force_hbm, phase_hbm, table, flags,
    press_out, resid_out, norms_out,
    phase, field, ystage, cstage, dstage, y5, recv, r5, f5,
    ext, faces, weights, source, va, vb, halo, dslab,
    res, sch, wap, sim, tim, nap, pre,
    red, total1, red1, red2, scal, norm,
    in_sem, send_sem, recv_sem, send5_sem, recv5_sem, rs1, rr1, rs2, rr2,
):
    nx, ny, nz = sizes
    at = (lax.axis_index("gx"), lax.axis_index("gy"), lax.axis_index("gz"))

    def neighbour(d):
        ok = None
        for dim in range(3):
            if d[dim] == 0:
                continue
            here = at[dim] < sizes[dim] - 1 if d[dim] > 0 else at[dim] > 0
            ok = here if ok is None else jnp.logical_and(ok, here)
        return ok, tuple(at[dim] + d[dim] for dim in range(3))

    def recv_at(k, d, start=0, rows=None):
        return recv.at[k, pl.ds(OFFSETS[d] + start, piece_rows(d) if rows is None else rows)]

    def pieces(k, d):
        dx, dy, dz = d
        to = tuple(-a for a in d)
        if dz == 0:
            if dx and dy:
                side = 0 if dy < 0 else 1
                src = ystage.at[k, side, pl.ds(0 if dx < 0 else 112, 16)]
                return src, recv_at(k, to)
            if dy:
                return ystage.at[k, 0 if dy < 0 else 1], recv_at(k, to)
            if dx < 0:
                return field.at[k, pl.ds(0, 64)], recv_at(k, to, 0, 64)
            return field.at[k, pl.ds(ROWS - 80, 80)], recv_at(k, to)
        side = 0 if dy < 0 else 1
        if dx and dy:
            return dstage.at[k, side, pl.ds(0 if dx < 0 else 8, 8)], recv_at(k, to)
        if dy:
            return dstage.at[k, side], recv_at(k, to)
        if dx:
            return cstage.at[k, pl.ds(0 if dx < 0 else 48, 16)], recv_at(k, to)
        return cstage.at[k], recv_at(k, to)

    def copy_of(k, d):
        src, dst = pieces(k, d)
        _, device = neighbour(d)
        to = tuple(-a for a in d)
        return pltpu.make_async_remote_copy(
            src_ref=src, dst_ref=dst,
            send_sem=send_sem.at[DIR_AT[d]], recv_sem=recv_sem.at[lax.rem(k, 5), DIR_AT[to]],
            device_id=device, device_id_type=MESH,
        )

    def incoming(k, d):
        to = tuple(-a for a in d)
        src, dst = pieces(k, to)
        return pltpu.make_async_remote_copy(
            src_ref=src, dst_ref=dst,
            send_sem=send_sem.at[DIR_AT[to]], recv_sem=recv_sem.at[lax.rem(k, 5), DIR_AT[d]],
            device_id=at, device_id_type=MESH,
        )

    sub8 = iota((8, 128), 0)
    lane8 = iota((8, 128), 1)
    group8, slot8 = lane8 // 16, lane8 % 16
    lane24 = iota((24, 128), 1)
    sub24 = iota((24, 128), 0)
    group24, slot24 = lane24 // 32, lane24 % 32
    bigroup8, bislot8 = lane8 // 32, lane8 % 32


    def pack_y(k):
        def pair(xp, _):
            base = pl.multiple_of(xp * 32, 32)
            a0, a1 = field[k, pl.ds(base, 8), :], field[k, pl.ds(base + 8, 8), :]
            b0, b1 = field[k, pl.ds(base + 16, 8), :], field[k, pl.ds(base + 24, 8), :]
            to = pl.multiple_of(xp * 8, 8)
            ystage[k, 0, pl.ds(to, 8), :] = jnp.where(sub8 < 4, a0, roll_rows(b0, 4))
            ystage[k, 1, pl.ds(to, 8), :] = jnp.where(sub8 < 4, roll_rows(a1, 4), b1)
            return 0
        lax.fori_loop(0, BX // 2, pair, 0, unroll=16)

    def pack_z(k):
        def block(xp, _):
            ends = []
            for u in range(2):
                acc = [[None, None] for _ in range(3)]
                for g in range(8):
                    base = pl.multiple_of(xp * 256, 256) + (u * 128 + g * 16)
                    a, b = field[k, pl.ds(base, 8), :], field[k, pl.ds(base + 8, 8), :]
                    for i, v in enumerate((a, b, jnp.where(sub8 < 4, a, b))):
                        for m in range(2):
                            r = roll_lanes(v, 9 * m + 16 * g)
                            acc[i][m] = r if g == 0 else jnp.where(group8 == g, r, acc[i][m])
                a, b, c = (jnp.where(slot8 < 4, lo, hi) for lo, hi in acc)
                to = pl.multiple_of(xp * 32, 32) + u * 16
                cstage[k, pl.ds(to, 8), :] = a
                cstage[k, pl.ds(to + 8, 8), :] = b
                ends.append(c)
            to = pl.ds(pl.multiple_of(xp * 8, 8), 8)
            dstage[k, 0, to, :] = jnp.where(sub8 < 4, ends[0], roll_rows(ends[1], 4))
            dstage[k, 1, to, :] = jnp.where(sub8 < 4, roll_rows(ends[0], 4), ends[1])
            return 0
        lax.fori_loop(0, 2, block, 0, unroll=2)

    flat = [d for d in DIRS if d[2] == 0]
    deep = [d for d in DIRS if d[2] != 0]

    def send(k, dirs):
        for d in dirs:
            ok, _ = neighbour(d)

            @pl.when(ok)
            def _():
                copy_of(k, d).start()

    def exchange_start(k):
        pack_y(k)
        send(k, flat)
        pack_z(k)
        send(k, deep)

    def pack_first(k, _):
        @pl.when(k == 1)
        def _():
            load_force.wait()
        pack_y(k)
        pack_z(k)
        return 0

    def receive(k, dirs):
        for d in dirs:
            ok, _ = neighbour(d)

            @pl.when(ok)
            def _():
                incoming(k, d).wait_recv()

    def finish_sends():
        for d in DIRS:
            ok, device = neighbour(d)
            rows = 64 if d == (-1, 0, 0) else piece_rows(d)

            @pl.when(ok)
            def _():
                part = recv.at[pl.ds(0, NSETS), pl.ds(0, rows)]
                pltpu.make_async_remote_copy(
                    src_ref=part, dst_ref=part, send_sem=send_sem.at[DIR_AT[d]], recv_sem=recv_sem.at[0, DIR_AT[d]],
                    device_id=device, device_id_type=MESH,
                ).wait_send()

    def main_row(x):
        return (1 + x) * 24

    def slab_row(l):
        return (42 + l) * 24

    def refresh(ref):
        low, high = pl.ds(slab_row(9), 24), pl.ds(slab_row(0), 24)
        ref[pl.ds(slab_row(-1), 24), :] = roll_lanes(ref[low, :], 32)
        ref[pl.ds(slab_row(10), 24), :] = roll_lanes(ref[high, :], -32)

    def unpack_flat(k):
        receive(k, flat)

        def planes(own, low, high, first, pairs):
            for xp in range(pairs):
                lo, hi = low(xp * 8), high(xp * 8)
                los, his = roll_rows(lo, 4), roll_rows(hi, 4)
                for half in range(2):
                    ra, rb = (roll_rows(own(xp * 32 + 16 * half + 8 * t), 4) for t in range(2))
                    to = main_row(first + 2 * xp + half)
                    ext[pl.ds(to, 8), :] = jnp.where(sub8 < 4, (lo, los)[half], ra)
                    ext[pl.ds(to + 8, 8), :] = jnp.where(sub8 < 4, ra, rb)
                    ext[pl.ds(to + 16, 8), :] = jnp.where(sub8 < 4, rb, (his, hi)[half])

        def of(d, start=0):
            return lambda row: recv[k, pl.ds(row + (OFFSETS[d] + start), 8), :]

        planes(lambda r: field[k, pl.ds(r, 8), :], of((0, -1, 0)), of((0, 1, 0)), 4, 16)
        planes(of((-1, 0, 0), 16), of((-1, -1, 0)), of((-1, 1, 0)), 0, 2)
        planes(of((1, 0, 0)), of((1, -1, 0)), of((1, 1, 0)), 36, 2)

        def own(i, _):
            for u in range(5):
                for t in range(3):
                    lo, hi = None, None
                    for h in range(4):
                        v = ext[pl.ds(pl.multiple_of(i * 120, 8) + (main_row(10 * h + u) + 8 * t), 8), :]
                        a, b = roll_lanes(v, 32 * h + 9), roll_lanes(v, 32 * h + 18)
                        lo = a if h == 0 else jnp.where(bigroup8 == h, a, lo)
                        hi = b if h == 0 else jnp.where(bigroup8 == h, b, hi)
                    to = pl.ds(pl.multiple_of(i * 120, 8) + (slab_row(u) + 8 * t), 8)
                    ext[to, :] = jnp.where(bislot8 < 9, lo, hi)
            return 0
        lax.fori_loop(0, 2, own, 0, unroll=2)

    def unpack_deep(k):
        receive(k, deep)

        def merged(d, row):
            low = recv[k, pl.ds(OFFSETS[(d[0], d[1], -1)] + row, 8), :]
            high = recv[k, pl.ds(OFFSETS[(d[0], d[1], 1)] + row, 8), :]
            return jnp.where(slot8 < 4, high, low)

        inner = []
        for t in range(2):
            inner.append([merged((-1, 0), 8 * t)] + [merged((0, 0), xb * 16 + 8 * t) for xb in range(4)] + [merged((1, 0), 8 * t)])
        sides = []
        for xb in range(6):
            dx, row = (-1, 0) if xb == 0 else (1, 0) if xb == 5 else (0, (xb - 1) // 2 * 8)
            above, below = merged((dx, 1), row), merged((dx, -1), row)
            if xb % 2 == 1:
                sides.append(jnp.where(sub8 < 4, below, roll_rows(above, 4)))
            else:
                sides.append(jnp.where(sub8 < 4, roll_rows(below, 4), above))

        def shifted(parts, i):
            return roll_lanes(jnp.where(group8 < 4, parts[i + 1], parts[i]), 64)

        def arrived(_, carry):
            for i in range(5):
                a, b = roll_rows(shifted(inner[0], i), 4), roll_rows(shifted(inner[1], i), 4)
                c = shifted(sides, i)
                tiles = (jnp.where(sub8 < 4, c, a), jnp.where(sub8 < 4, a, b), jnp.where(sub8 < 4, b, c))
                for t in range(3):
                    halo[pl.ds(i * 24 + 8 * t, 8), :] = tiles[t]
            return carry
        lax.fori_loop(0, 1, arrived, 0)

        def outer(l, _):
            for t in range(3):
                acc = None
                for h in range(4):
                    x = 10 * h + l
                    v = halo[pl.ds(x // 8 * 24 + 8 * t, 8), :]
                    a = roll_lanes(v, 32 * h + 9 - 16 * (x % 8))
                    acc = a if h == 0 else jnp.where(bigroup8 == h, a, acc)
                to = pl.ds(slab_row(l) + 8 * t, 8)
                ext[to, :] = jnp.where((bislot8 >= 9) & (bislot8 < 18), acc, ext[to, :])
            return 0
        for l in range(10):
            outer(l, 0)


    walls = [jnp.where(flags[f] == 0, F32(1.0), F32(0.0)) for f in range(6)]
    totals = (nx * BX, ny * BY, nz * BZ)

    def coefficients(b, e, nbrs, spots):
        inside = None
        diag = jnp.zeros_like(e)
        extra = [jnp.zeros_like(e) for _ in range(3)]
        for axis in range(3):
            for side in range(2):
                spot = spots[axis] + (1 if side else -1)
                here = (spot >= 0) & (spot < totals[axis])
                face = 0.5 * (e + nbrs[axis][side])
                wall = walls[2 * axis + side]
                outer = jnp.where(here, F32(0.0), e)
                diag = diag + jnp.where(here, face, e * wall)
                extra[axis] = extra[axis] + outer * (1.0 - wall)
                faces[2 * axis + side, pl.ds(b, 24), :] = face
            here = (spots[axis] >= 0) & (spots[axis] < totals[axis])
            inside = here if inside is None else inside & here
        for c in range(3):
            d = diag + extra[c]
            good = inside & (d > 0)
            weights[c, pl.ds(b, 24), :] = jnp.where(good, OMEGA / jnp.where(good, d, F32(1.0)), F32(0.0))

    def setup():
        keep = None
        for t in range(2):
            v = roll_rows(recv[0, pl.ds(OFFSETS[(-1, 0, 0)] + 8 * t, 8), :], 4)
            if t == 0:
                ext[pl.ds(0, 8), :] = jnp.where(sub8 < 4, F32(0.0), v)
                keep = v
            else:
                ext[pl.ds(8, 8), :] = jnp.where(sub8 < 4, keep, v)
                ext[pl.ds(16, 8), :] = jnp.where(sub8 < 4, v, F32(0.0))
        first = ext[pl.ds(0, 24), :]
        first = jnp.where(slot24 < 9, roll_lanes(first, 9), roll_lanes(first, 18))
        low = pl.ds(slab_row(-1), 24)
        ext[low, :] = jnp.where(group24 == 0, first, ext[low, :])
        five = None
        lane16 = iota((16, 128), 1)
        for h in range(4):
            v = r5[pl.ds(10 * h + 4, 16), :]
            v = jnp.where(lane16 % 32 < 9, roll_lanes(v, 32 * h + 9), roll_lanes(v, 32 * h + 18))
            five = v if h == 0 else jnp.where(lane16 // 32 == h, v, five)
        f5[...] = five

        def neighbours(b, below):
            e = ext[pl.ds(b, 24), :]
            return e, (
                (ext[pl.ds(b - 24, 24), :], ext[pl.ds(b + 24, 24), :]),
                (jnp.where(sub24 == 0, below, ext[pl.ds(b - 1, 24), :]), ext[pl.ds(b + 1, 24), :]),
                (roll_lanes(e, 1), roll_lanes(e, 127)),
            )

        ys = sub24 + (at[1] * BY - 4)

        def main_block(i, _):
            fives = roll_rows(jnp.where(sub8 < 4, r5[pl.ds(pl.multiple_of(i * 8, 8) + 8, 8), :], r5[pl.ds(pl.multiple_of(i * 8, 8), 8), :]), 4)
            for j in range(8):
                b = pl.multiple_of(i * 192, 8) + main_row(j)
                e, nbrs = neighbours(b, jnp.broadcast_to(fives[j:j + 1, :], (24, 128)))
                coefficients(b, e, nbrs, (
                    jnp.broadcast_to(at[0] * BX + (i * 8 + j - 4), (24, 128)), ys, lane24 + at[2] * BZ,
                ))
            return 0
        lax.fori_loop(0, 5, main_block, 0, unroll=5)
        zs = jnp.where(slot24 < 13, slot24 + 119, slot24 - 18) + at[2] * BZ

        for l in range(10):
            b = slab_row(l)
            e, nbrs = neighbours(b, jnp.broadcast_to(f5[l:l + 1, :], (24, 128)))
            coefficients(b, e, nbrs, (group24 * 10 + (at[0] * BX - 4 + l), ys, zs))


    SLAB = [slab_row(l) for l in (9, 0, 1, 2, 3, 4, 5, 6, 7, 8)]

    def gradient(planes):
        for b in planes:
            p = ext[pl.ds(b, 24), :]
            nbrs = (ext[pl.ds(b + 24, 24), :], ext[pl.ds(b + 1, 24), :], roll_lanes(p, 127))
            for c in range(3):
                source[c, pl.ds(b, 24), :] = weights[c, pl.ds(b, 24), :] * (nbrs[c] - p)

    def scaled_force(c, first, count):
        def block(i, _):
            for u in range(10):
                b = pl.multiple_of(i * 240, 8) + (first + 24 * u)
                source[c, pl.ds(b, 24), :] = weights[c, pl.ds(b, 24), :] * ext[pl.ds(b, 24), :]
            return 0
        lax.fori_loop(0, count // 10, block, 0)

    def ends(ref):
        def each(c, _):
            refresh(ref.at[c])
            return 0
        lax.fori_loop(0, 3, each, 0, unroll=3)

    def sweep(src, dst, planes):
        for b in planes:
            k = [faces[f, pl.ds(b, 24), :] for f in range(6)]
            for c in range(3):
                v = src[c, pl.ds(b, 24), :]
                total = k[0] * src[c, pl.ds(b - 24, 24), :] + k[1] * src[c, pl.ds(b + 24, 24), :]
                total = total + (k[2] * src[c, pl.ds(b - 1, 24), :] + k[3] * src[c, pl.ds(b + 1, 24), :])
                total = total + (k[4] * roll_lanes(v, 1) + k[5] * roll_lanes(v, 127))
                dst[c, pl.ds(b, 24), :] = (
                    (1.0 - OMEGA) * v + source[c, pl.ds(b, 24), :] + weights[c, pl.ds(b, 24), :] * total
                )

    def minus_divergence(src, b, rows):
        x, y, z = (src[c, pl.ds(b, rows), :] for c in range(3))
        return (src[0, pl.ds(b - 24, rows), :] - x) + (src[1, pl.ds(b - 1, rows), :] - y) + (roll_lanes(z, 1) - z)

    def divergence(src, out):
        def slab_part(i, _):
            for u in range(5):
                b = pl.multiple_of(i * 120, 8) + slab_row(u)
                dslab[pl.ds(pl.multiple_of(i * 120, 8) + u * 24, 24), :] = minus_divergence(src, b, 24)
            return 0
        lax.fori_loop(0, 2, slab_part, 0, unroll=2)

        def together(i, _):
            for u in range(5):
                b = pl.ds(pl.multiple_of(i * 120, 8) + u * 24, 24)
                v = dslab[b, :]
                dslab[b, :] = jnp.where(slot24 < 9, v, roll_lanes(v, -9))
            return 0
        lax.fori_loop(0, 2, together, 0, unroll=2)
        lane16 = iota((16, 128), 1)
        for x in range(4, 36):
            h, l = divmod(x, 10)
            total = minus_divergence(src, main_row(x) + 4, 16)
            edge = roll_lanes(dslab[pl.ds(l * 24 + 4, 16), :], -(9 + 32 * h))
            out[pl.ds((x - 4) * 16, 16), :] = jnp.where((lane16 < 8) | (lane16 >= 124), edge, total)

    def main_rows(first, last):
        return [main_row(x) for x in range(first, last + 1)]

    def apply(out):
        ends(source)
        sweep(source, va, SLAB)
        ends(va)
        sweep(va, vb, SLAB + main_rows(2, 36))
        ends(vb)
        sweep(vb, va, SLAB + main_rows(3, 35))
        ends(va)
        divergence(va, out)


    me_z = at[2]
    me_xy = at[0] * ny + at[1]
    nxy = nx * ny

    def z_copy(k, off):
        return pltpu.make_async_remote_copy(
            src_ref=red.at[k], dst_ref=red1.at[k, me_z], send_sem=rs1.at[k], recv_sem=rr1.at[k],
            device_id=(at[0], at[1], lax.rem(me_z + off, nz)), device_id_type=MESH,
        )

    def xy_copy(k, ox, oy):
        return pltpu.make_async_remote_copy(
            src_ref=total1.at[k], dst_ref=red2.at[k, me_xy], send_sem=rs2.at[k], recv_sem=rr2.at[k],
            device_id=(lax.rem(at[0] + ox, nx), lax.rem(at[1] + oy, ny), at[2]), device_id_type=MESH,
        )

    def all_of(k, ref, count, sent, arrived):
        part = ref.at[k, pl.ds(0, count)]
        return pltpu.make_async_remote_copy(
            src_ref=part, dst_ref=part, send_sem=sent.at[k], recv_sem=arrived.at[k],
            device_id=at, device_id_type=MESH,
        )

    offsets_xy = [(ox, oy) for ox in range(nx) for oy in range(ny) if (ox, oy) != (0, 0)]

    def reduce_start(k):
        red1[k, me_z] = red[k]
        for off in range(1, nz):
            z_copy(k, off).start()

    def reduce_middle(k):
        all_of(k, red1, nz - 1, rs1, rr1).wait_recv()
        value = red1[k, 0]
        for i in range(1, nz):
            value = value + red1[k, i]
        total1[k] = value
        red2[k, me_xy] = value
        for ox, oy in offsets_xy:
            xy_copy(k, ox, oy).start()

    cells = float(totals[0] * totals[1] * totals[2])

    def reduce_end(k):
        all_of(k, red2, nxy - 1, rs2, rr2).wait_recv()
        value = red2[k, 0]
        for i in range(1, nxy):
            value = value + red2[k, i]
        gamma, delta, squares = (
            jnp.broadcast_to(jnp.sum(value[i], axis=1, keepdims=True), (8, 128)) for i in range(3)
        )
        norm[k] = squares / cells
        gamma_old, alpha_old = scal[0], scal[1]
        if isinstance(k, int):
            beta = gamma / gamma_old
            alpha = gamma / (delta - beta * gamma / alpha_old)
        else:
            beta = jnp.where(k == 0, F32(0.0), gamma / gamma_old)
            alpha = gamma / (delta - jnp.where(k == 0, F32(0.0), beta * gamma / alpha_old))
        scal[0] = gamma
        scal[1] = alpha
        return alpha, beta


    load_phase = pltpu.make_async_copy(phase_hbm, phase, in_sem.at[0])
    load_force = pltpu.make_async_copy(force_hbm, field.at[pl.ds(1, 3)], in_sem.at[1])
    load_phase.start()
    load_force.start()

    for t in range(0, 56, 8):
        r5[pl.ds(t, 8), :] = jnp.zeros((8, 128), F32)

    barrier = pltpu.get_barrier_semaphore()
    count = jnp.int32(0)
    for d in DIRS:
        ok, device = neighbour(d)

        @pl.when(ok)
        def _():
            pl.semaphore_signal(barrier, inc=1, device_id=device, device_id_type=MESH)
        count = count + ok.astype(jnp.int32)
    for off in range(1, nz):
        pl.semaphore_signal(barrier, inc=1, device_id=(at[0], at[1], lax.rem(me_z + off, nz)), device_id_type=MESH)
    for ox, oy in offsets_xy:
        pl.semaphore_signal(
            barrier, inc=1, device_id=(lax.rem(at[0] + ox, nx), lax.rem(at[1] + oy, ny), at[2]), device_id_type=MESH
        )
    count = count + (nz - 1 + nxy - 1)

    for d in DIRS:
        ok, _ = neighbour(d)

        @pl.when(jnp.logical_not(ok))
        def _():
            def clear_recv(k, _):
                for row in range(0, piece_rows(d), 8):
                    recv[k, pl.ds(OFFSETS[d] + row, 8), :] = jnp.zeros((8, 128), F32)
                return 0
            lax.fori_loop(0, NSETS, clear_recv, 0)

    zero24 = jnp.zeros((24, 128), F32)
    ext[pl.ds(0, 24), :] = zero24
    for ref in (source, va, vb):
        for c in range(3):
            for plane in (0, 1, 2, 3, 38, 39, 40, 41, 52):
                ref[c, pl.ds(plane * 24, 24), :] = zero24
    for f in range(6):
        faces[f, pl.ds(41 * 24, 24), :] = zero24
    for c in range(3):
        weights[c, pl.ds(41 * 24, 24), :] = zero24
        weights[c, pl.ds(52 * 24, 24), :] = zero24
    zero8 = jnp.zeros((8, 128), F32)
    scal[0] = zero8 + 1.0
    scal[1] = zero8 + 1.0
    for ref in (sch, sim, tim, pre):
        def clear(i, _):
            ref[pl.ds(pl.multiple_of(i * 64, 64), 64), :] = jnp.zeros((64, 128), F32)
            return 0
        lax.fori_loop(0, ROWS // 64, clear, 0)

    load_phase.wait()

    def lookup(i, _):
        for u in range(4):
            r = pl.multiple_of(i * 32, 32) + 8 * u
            ids = phase[pl.ds(r, 8), :]
            eta = jnp.zeros((8, 128), F32)
            for level in range(8):
                eta = eta + jnp.where(ids == level, table[level], F32(0.0))
            field[0, pl.ds(r, 8), :] = eta
        return 0
    lax.fori_loop(0, ROWS // 32, lookup, 0)
    for x in range(BX):
        y5[pl.ds(x, 1), :] = field[0, pl.ds(x * 16 + 11, 1), :]
    lax.fori_loop(0, 4, pack_first, 0)
    pl.semaphore_wait(barrier, count)
    has_y_up, _ = neighbour((0, 1, 0))
    has_y_down, _ = neighbour((0, -1, 0))
    copy5_out = pltpu.make_async_remote_copy(
        src_ref=y5, dst_ref=r5.at[pl.ds(8, 32)], send_sem=send5_sem, recv_sem=recv5_sem,
        device_id=(at[0], at[1] + 1, at[2]), device_id_type=MESH,
    )

    @pl.when(has_y_up)
    def _():
        copy5_out.start()

    def send_first(k, _):
        send(k, flat)
        send(k, deep)
        return 0
    lax.fori_loop(0, 4, send_first, 0)

    def rows_loop(body, init, step=16):
        def block(i, carry):
            for u in range(step):
                carry = body(pl.ds(pl.multiple_of(i * (8 * step), 8 * step) + 8 * u, 8), carry)
            return carry
        return lax.fori_loop(0, ROWS // (8 * step), block, init)

    def keep_partials(k, sums):
        for i in range(3):
            red[k, i] = jnp.sum(sums[i], axis=0, keepdims=True)

    def advance(alpha, beta, last):
        def step(at_r, carry):
            e, rr, w, n = field[0, at_r, :], res[at_r, :], wap[at_r, :], nap[at_r, :]
            p = e * rr + beta * sch[at_r, :]
            s = w + beta * sim[at_r, :]
            t = n + beta * tim[at_r, :]
            sch[at_r, :] = p
            sim[at_r, :] = s
            tim[at_r, :] = t
            pre[at_r, :] = pre[at_r, :] + alpha * p
            rr = rr - alpha * s
            w = w - alpha * t
            res[at_r, :] = rr
            wap[at_r, :] = w
            field[last, at_r, :] = e * w
            return carry[0] + rr * (e * rr), carry[1] + w * (e * rr), carry[2] + rr * rr
        return rows_loop(step, (zero8, zero8, zero8))

    def stage(k, _):
        unpack_flat(k)

        @pl.when(k >= 5)
        def _():
            reduce_middle(k - 5)

        @pl.when((k >= 1) & (k < 4))
        def _():
            scaled_force(k - 1, main_row(0), 40)

        @pl.when(k >= 4)
        def _():
            gradient(main_rows(0, 38))

        @pl.when(k >= 3)
        def _():
            sweep(source, va, main_rows(1, 37))
        unpack_deep(k)

        @pl.when(k == 0)
        def _():
            @pl.when(has_y_down)
            def _():
                copy5_out.wait_recv()
            refresh(ext)
            setup()

        @pl.when((k >= 1) & (k < 4))
        def _():
            scaled_force(k - 1, slab_row(0), 10)

        @pl.when(k >= 4)
        def _():
            refresh(ext)
            gradient(SLAB)

        @pl.when(k >= 3)
        def _():
            apply(nap)

        @pl.when(k == 3)
        def _():
            def step(at_r, _):
                r = nap[at_r, :]
                res[at_r, :] = r
                field[4, at_r, :] = field[0, at_r, :] * r
                return 0
            rows_loop(step, 0)

        @pl.when(k == 4)
        def _():
            def step(at_r, carry):
                e, rr, w = field[0, at_r, :], res[at_r, :], nap[at_r, :]
                z = e * rr
                wap[at_r, :] = w
                field[5, at_r, :] = e * w
                return carry[0] + rr * z, carry[1] + w * z, carry[2] + rr * rr
            keep_partials(0, rows_loop(step, (zero8, zero8, zero8)))

        @pl.when(k >= 5)
        def _():
            alpha, beta = reduce_end(k - 5)
            keep_partials(k - 4, advance(alpha, beta, k + 1))

        @pl.when((k >= 3) & (k < 6))
        def _():
            exchange_start(k + 1)

        @pl.when(k >= 4)
        def _():
            reduce_start(k - 4)
        return 0
    lax.fori_loop(0, NSETS, stage, 0)

    reduce_middle(2)
    finish_sends()

    @pl.when(has_y_up)
    def _():
        copy5_out.wait_send()
    for k in range(ITERS):
        all_of(k, red1, nz - 1, rs1, rr1).wait_send()
        all_of(k, red2, nxy - 1, rs2, rr2).wait_send()
    alpha, beta = reduce_end(2)

    def step2(at_r, _):
        rr = res[at_r, :]
        p = field[0, at_r, :] * rr + beta * sch[at_r, :]
        s = wap[at_r, :] + beta * sim[at_r, :]
        press_out[at_r, :] = pre[at_r, :] + alpha * p
        resid_out[at_r, :] = rr - alpha * s
        return 0
    rows_loop(step2, 0)
    norms_out[...] = jnp.where(lane8 == 0, norm[0], jnp.where(lane8 == 1, norm[1], norm[2]))


def solution(mesh):
    sizes = (mesh.shape["gx"], mesh.shape["gy"], mesh.shape["gz"])
    nx, ny, nz = sizes

    def per_device(force, phase, table, flags):
        v = functools.partial(pltpu.VMEM)
        dma = pltpu.SemaphoreType.DMA
        scratch = [
            v((ROWS, 128), jnp.int32),
            v((NSETS + 1, ROWS, 128), F32),
            v((NSETS, 2, 128, 128), F32),
            v((NSETS, 64, 128), F32),
            v((NSETS, 2, 16, 128), F32),
            v((32, 128), F32),
            v((NSETS, RECV_ROWS, 128), F32),
            v((56, 128), F32), v((16, 128), F32),
            v((EROWS, 128), F32),
            v((6, EROWS, 128), F32), v((3, EROWS, 128), F32), v((3, EROWS, 128), F32),
            v((3, EROWS, 128), F32), v((3, EROWS, 128), F32),
            v((120, 128), F32), v((240, 128), F32),
            *[v((ROWS, 128), F32) for _ in range(7)],
            v((ITERS, 3, 1, 128), F32), v((ITERS, 3, 1, 128), F32),
            v((ITERS, nz, 3, 1, 128), F32), v((ITERS, nx * ny, 3, 1, 128), F32),
            v((2, 8, 128), F32), v((ITERS, 8, 128), F32),
            dma((2,)), dma((26,)), dma((5, 26)), dma, dma,
            dma((ITERS,)), dma((ITERS,)), dma((ITERS,)), dma((ITERS,)),
        ]
        hbm = pl.BlockSpec(memory_space=pl.ANY)
        smem = pl.BlockSpec(memory_space=pltpu.SMEM)
        press, resid, norms = pl.pallas_call(
            functools.partial(kernel, sizes),
            out_shape=(
                pltpu.VMEM((ROWS, 128), F32),
                pltpu.VMEM((ROWS, 128), F32),
                pltpu.VMEM((8, 128), F32),
            ),
            in_specs=[hbm, hbm, smem, smem],
            out_specs=(pl.BlockSpec(memory_space=pltpu.VMEM), pl.BlockSpec(memory_space=pltpu.VMEM), pl.BlockSpec(memory_space=pltpu.VMEM)),
            scratch_shapes=scratch,
            compiler_params=pltpu.CompilerParams(
                collective_id=0, has_side_effects=True, vmem_limit_bytes=60 * 1024 * 1024
            ),
        )(force.reshape(3, ROWS, BZ), phase.reshape(ROWS, BZ), table, flags)
        return press.reshape(BX, BY, BZ), resid.reshape(BX, BY, BZ), norms[0, :ITERS]

    return jax.shard_map(
        per_device,
        mesh=mesh,
        in_specs=(P(None, "gx", "gy", "gz"), P("gx", "gy", "gz"), P(), P()),
        out_specs=(P("gx", "gy", "gz"), P("gx", "gy", "gz"), P()),
        check_vma=False,
    )
```
